256 devices in a mesh: gx: 4 (over x_lo, core), gy: 16 (over z, x_hi), gz: 4 (over y).
Axes of the slice: x: 4 (x_hi: 2, x_lo: 2; x = x_hi * 2 + x_lo), y: 4, z: 8, core: 2. Of those that a mesh axis runs over, the one named last changes fastest.
Arguments:
- fields: float32 [5, 64, 128, 512], P(None, 'gz', 'gy', 'gx'), may hold values from -4 to 4
- radius: float32 [8, 64, 128, 512], P(None, 'gz', 'gy', 'gx'), may hold values from 0.4 to 1.5
- weight: float32 [8, 64, 128, 512], P(None, 'gz', 'gy', 'gx'), may hold values from 0.05 to 0.5
- column: int32 [8, 64, 128, 512], P(None, 'gz', 'gy', 'gx'), may hold values from 0 to 127
- counts: int32 [64, 128, 512], P('gz', 'gy', 'gx'), may hold values from 1 to 8
- fall_depth: int32 [8, 64, 128, 4], P(None, 'gz', 'gy', 'gx'), may hold values from 0 to 8, as said below
Outputs:
- new_fields: float32 [5, 64, 128, 512], P(None, 'gz', 'gy', 'gx')
- moments: float32 [3, 64, 128, 512], P(None, 'gz', 'gy', 'gx')
The draws below stay inside these ranges and needn't reach their ends.
Inputs may be any that keep to these rules, and one draw needn't show every extreme that they name: The droplet in slot s of cell (k, j, i) sits in x cell (i // 128) * 128 + column[s, k, j, i]. Slots s < counts[k, j, i] hold live droplets. The droplets of slot s in cells (k, j, b * 128) to (k, j, (b + 1) * 128 - 1) fall together by fall_depth[s, k, j, b] levels, never below the lowest level: fall_depth[s, k, j, b] <= k; 8 is reached in every draw.
All inputs are finite; a program needn't handle non-finite values. Where the reference program divides by a largest or mean magnitude, that divisor is 1e-20 or more.
Results may differ from the reference program's by a relative error of at most 0.00021.
Values sent between devices are 32-bit elements; how exact they have to be, the bound alone decides.
A program may use at most 64 MiB of HBM per device.

```python
import math
import jax
import jax.numpy as jnp
from jax import lax

CX = 128
SLOTS = 8
NS = 4
FMAX = 8
NX = 512
NY = 128
NZ = 64
XBLOCKS = 4


def draw_fall_depth(key, part):
    drawn = jax.random.randint(key, (SLOTS, NZ, NY, XBLOCKS), 0, FMAX + 1, dtype=jnp.int32)
    drawn = drawn.at[0, NZ - 1, 0, 0].set(FMAX)
    levels = jnp.arange(NZ, dtype=jnp.int32)[None, :, None, None]
    return jnp.minimum(drawn, levels).astype(jnp.int32)


def set_ends(values, own_key, least, largest):
    shape = values.shape
    index_at = [jax.random.randint(jax.random.fold_in(own_key, axis), (), 0, shape[axis]) for axis in range(len(shape))]
    values = values.at[tuple(index_at)].set(least)
    longest = shape.index(max(shape))
    index_at[longest] = (index_at[longest] + 1) % shape[longest]
    return values.at[tuple(index_at)].set(largest)


def shard_levels(key, shape, cuts, smallest, high):
    loudness = 1.0
    for position, shards_of in cuts:
        steps = jax.random.uniform(jax.random.fold_in(jax.random.fold_in(key, 6), position), (shards_of,), jnp.float32, smallest / len(cuts), high / len(cuts))
        loudness = loudness * jnp.repeat(jnp.exp(steps), shape[position] // shards_of).reshape((-1,) + (1,) * (len(shape) - 1 - position))
    return loudness


def centred(rng, dims, spread, reach, cuts=(), held_as=jnp.bfloat16):
    entries = spread * jax.random.normal(rng, dims, jnp.float32)
    if cuts:
        entries = entries * shard_levels(rng, dims, cuts, -0.22, 0.18)
    return jnp.clip(entries, -reach, reach).astype(held_as)


def setup_inputs(seed: int = 0) -> dict:
    splits = jax.random.split(jax.random.key(seed), 7)
    fields = centred(splits[0], (5, NZ, NY, NX), 0.5, 4.0, ((1, 4), (2, 16), (3, 4)), jnp.float32)
    radius = jnp.clip(jnp.exp(math.log(1.5) - 1.3217558 * jax.random.uniform(splits[1], (SLOTS, NZ, NY, NX), jnp.float32) ** shard_levels(splits[1], (SLOTS, NZ, NY, NX), ((1, 4), (2, 16), (3, 4)), -0.2, 0.2)), 0.4, 1.5)
    weight = jnp.clip(jnp.exp(math.log(0.5) - 2.3025851 * jax.random.uniform(splits[2], (SLOTS, NZ, NY, NX), jnp.float32) ** shard_levels(splits[2], (SLOTS, NZ, NY, NX), ((1, 4), (2, 16), (3, 4)), -0.2, 0.2)), 0.05, 0.5)
    column = set_ends(jax.random.randint(splits[3], (SLOTS, NZ, NY, NX), 0, CX), jax.random.fold_in(splits[3], 1), 0, CX - 1).astype(jnp.int32)
    counts = set_ends(jax.random.randint(splits[4], (NZ, NY, NX), 1, SLOTS + 1), jax.random.fold_in(splits[4], 1), 1, SLOTS).astype(jnp.int32)
    fall_depth = draw_fall_depth(jax.random.fold_in(splits[6], 71), 0)
    return dict(fields=fields, radius=radius, weight=weight, column=column, counts=counts, fall_depth=fall_depth)


sound_speed = 10.0
buoyancy = 0.5
courant_goal = 0.6
growth = 0.3

def window(padded, margin, direction, offset, length):
    cut = []
    for dimension in range(3):
        if dimension == direction:
            cut.append(slice(margin + offset, margin + offset + length))
        else:
            cut.append(slice(margin, padded.shape[dimension] - margin))
    return padded[tuple(cut)]

def advect(quantity, margin, wind_pad, wind_margin):
    tendency = jnp.zeros(tuple((quantity.shape[dimension] - 2 * margin for dimension in range(3))), jnp.float32)
    for direction in range(3):
        cells_along = quantity.shape[direction] - 2 * margin
        stencil = [window(quantity, margin, direction, offset - 1, cells_along + 1) for offset in range(-2, 4)]
        face_wind = window(wind_pad[2 - direction], wind_margin, direction, -1, cells_along + 1)
        central = 37.0 * (stencil[2] + stencil[3]) - 8.0 * (stencil[1] + stencil[4]) + (stencil[0] + stencil[5])
        upwind = 10.0 * (stencil[3] - stencil[2]) - 5.0 * (stencil[4] - stencil[1]) + (stencil[5] - stencil[0])
        face_flux = (face_wind * central - jnp.abs(face_wind) * upwind) / 60.0
        upper_flux = lax.slice_in_dim(face_flux, 1, cells_along + 1, axis=direction)
        lower_flux = lax.slice_in_dim(face_flux, 0, cells_along, axis=direction)
        tendency = tendency - (upper_flux - lower_flux)
    return tendency

def extend(fields, margin):
    fields = jnp.pad(fields, ((0, 0), (margin, margin), (0, 0), (0, 0)))
    return jnp.pad(fields, ((0, 0), (0, 0), (margin, margin), (margin, margin)), mode='wrap')

def acoustic(fast_fields, lift_term, pressure_rate, sub_step, lid_mask):
    grid_levels, grid_rows, grid_cols = (fast_fields.shape[1], fast_fields.shape[2], fast_fields.shape[3])
    pressure_pad = extend(fast_fields[0:1], 1)[0]
    pressure = fast_fields[0]
    east_wind = fast_fields[1] - sub_step * sound_speed * (window(pressure_pad, 1, 2, 1, grid_cols) - pressure)
    north_wind = fast_fields[2] - sub_step * sound_speed * (window(pressure_pad, 1, 1, 1, grid_rows) - pressure)
    vertical_wind = (fast_fields[3] + sub_step * (lift_term - sound_speed * (window(pressure_pad, 1, 0, 1, grid_levels) - pressure))) * lid_mask
    wind_halo = extend(jnp.stack([east_wind, north_wind, vertical_wind]), 1)
    divergence = east_wind - window(wind_halo[0], 1, 2, -1, grid_cols) + (north_wind - window(wind_halo[1], 1, 1, -1, grid_rows)) + (vertical_wind - window(wind_halo[2], 1, 0, -1, grid_levels))
    pressure = pressure + sub_step * (pressure_rate - sound_speed * divergence)
    return jnp.stack([pressure, east_wind, north_wind, vertical_wind])

def reference(fields, radius, weight, column, counts, fall_depth):
    grid_levels, grid_rows, grid_cols = (fields.shape[1], fields.shape[2], fields.shape[3])
    lid_mask = (jnp.arange(grid_levels, dtype=jnp.int32) < grid_levels - 1).astype(jnp.float32)[:, None, None]
    initial = jnp.concatenate([fields[0:4], (fields[4] * lid_mask)[None]])
    top_speed = jnp.max(jnp.abs(initial[2]) + jnp.abs(initial[3]) + jnp.abs(initial[4]))
    time_step = courant_goal / (1.0 + top_speed)
    current = initial
    for fraction, substeps in ((1.0 / 3.0, 1), (0.5, NS // 2), (1.0, NS)):
        padded = extend(current, 3)
        tracer_rate = advect(padded[0], 3, padded[2:5], 3)
        pressure_rate = advect(padded[1], 3, padded[2:5], 3)
        lift_term = buoyancy * 0.5 * (window(padded[0], 3, 0, 0, grid_levels) + window(padded[0], 3, 0, 1, grid_levels)) * lid_mask
        sub_step = fraction * time_step / substeps
        fast_fields = initial[1:5]
        for repeat in range(substeps):
            fast_fields = acoustic(fast_fields, lift_term, pressure_rate, sub_step, lid_mask)
        tracer = initial[0] + fraction * time_step * tracer_rate
        current = jnp.concatenate([tracer[None], fast_fields])
    tracer = current[0]
    block_start = jnp.arange(grid_cols, dtype=jnp.int32) // CX * CX
    levels = jnp.arange(grid_levels, dtype=jnp.int32)[:, None, None]
    row_index = jnp.arange(grid_rows, dtype=jnp.int32)[None, :, None]
    moments = jnp.zeros((3, grid_levels * grid_rows * grid_cols), jnp.float32)
    for slot_index in range(SLOTS):
        cell_column = (block_start[None, None, :] + column[slot_index]).astype(jnp.int32)
        near_tracer = jnp.take_along_axis(tracer, cell_column, axis=2)
        squared = radius[slot_index] * radius[slot_index] * jnp.exp(growth * near_tracer)
        number = weight[slot_index] * (slot_index < counts).astype(jnp.float32)
        area_term = number * squared
        mass_term = area_term * jnp.sqrt(squared)
        fall_cells = jnp.repeat(fall_depth[slot_index], CX, axis=2).astype(jnp.int32)
        flat_index = (((levels - fall_cells) * grid_rows + row_index) * grid_cols + cell_column).astype(jnp.int32)
        moments = moments.at[:, flat_index.reshape(-1)].add(jnp.stack([number, area_term, mass_term]).reshape(3, -1))
    return (current, moments.reshape(3, grid_levels, grid_rows, grid_cols))
```

```python
import functools

import jax
import jax.numpy as jnp
from jax import lax
from jax.experimental import pallas as pl
from jax.experimental.pallas import tpu as pltpu
from jax.sharding import PartitionSpec as P

MESH = pl.DeviceIdType.MESH
F32 = jnp.float32
L = 16
DEPTHS = 9
PITCH = 136
WIDE = {0: 0, 1: 1, 3: 2}
NARROW = {2: 0, 4: 1, 5: 2, 6: 3}
SPLITS = (0, 40, 90, 110, 128)


def kernel(
    sizes,
    fields, counts, depth_in, rad_h, wgt_h, col_h,
    out, mom,
    rad, wgt, col, dep, dmat, gmat, ext, fall,
    c0, p0, w0, cq, pq, wq, uq, vq, umq, vmq,
    ta, aa, ba, uinc, vinc, winc, um0, vm0, uminc, vminc,
    tr, pr, lift, pf, uf, vf, wf, pg, ug, vg, wg,
    hx, hy,
    sx, rx, syw, ryw, sya, rya, szw, rzw, sza, rza,
    m1s, m1r, m2s, m2r,
    send_sem, recv_sem, m1_send, m1_recv, m2_send, m2_recv, fall_sem, load_sem,
):
    nx, ny, nz = sizes
    ix, iy, iz = lax.axis_index("gx"), lax.axis_index("gy"), lax.axis_index("gz")

    def near(axis, step):
        i, n = {"gx": (ix, nx), "gy": (iy, ny), "gz": (iz, nz)}[axis]
        return lax.rem(i + (step + n), n)

    lane = lax.broadcasted_iota(jnp.int32, (8, 128), 1)
    row = lax.broadcasted_iota(jnp.int32, (8, 128), 0)
    klo = (iz > 0).astype(F32)
    khi = (iz < nz - 1).astype(F32)

    loads = []
    for a, (src, dst) in enumerate(((rad_h, rad), (wgt_h, wgt), (col_h, col))):
        for s in range(8):
            loads.append(
                pltpu.make_async_copy(
                    src.at[pl.ds(s * 128, 128)], dst.at[pl.ds(s * PITCH, 128)], load_sem.at[a, s]
                )
            )
    for c in loads:
        c.start()

    group1 = [(a, b) for a in range(nx) for b in range(nz) if (a, b) != (0, 0)]
    group2 = list(range(1, ny))
    barrier = pltpu.get_barrier_semaphore()
    for a, b in group1:
        pl.semaphore_signal(
            barrier, inc=1, device_id={"gx": near("gx", a), "gz": near("gz", b)}, device_id_type=MESH
        )
    for a in group2:
        pl.semaphore_signal(barrier, inc=1, device_id={"gy": near("gy", a)}, device_id_type=MESH)

    def roll_l(x, s):
        s = s % 128
        return pltpu.roll(x, s, 1) if s else x

    def roll_s(x, s):
        s = s % 8
        return pltpu.roll(x, s, 0) if s else x

    def xp(q, h, n):
        return roll_l(jnp.where(lane < n, h, q), -n)

    def xm(q, h, n):
        return roll_l(jnp.where(lane >= 128 - n, h, q), n)

    def yp(q, h, n):
        return roll_s(jnp.where(row < n, h, q), -n)

    def ym(q, h, n):
        return roll_s(jnp.where(row >= 8 - n, h, q), n)

    def put_l(message, value, at, width):
        return jnp.where((lane >= at) & (lane < at + width), value, message)

    def put_s(message, value, at, width):
        return jnp.where((row >= at) & (row < at + width), value, message)

    def by_level(fn):
        def group(g, carry):
            state = {}
            for kk in range(8):
                fn(g, kk, g * 8 + kk, state)
            return carry

        lax.fori_loop(0, 2, group, 0)

    def copies(r):
        if r in WIDE:
            w = WIDE[r]
            ysrc, ydst, zsrc, zdst = syw.at[w], ryw.at[w], szw.at[w], rzw.at[w]
            yn = 24 if r == 1 else 16
            zn = 9 if r == 1 else 7
        else:
            w = NARROW[r]
            ysrc, ydst, zsrc, zdst = sya.at[w], rya.at[w], sza.at[w], rza.at[w]
            yn, zn = 4, 2
        made = []
        for d, step in ((0, 1), (1, -1)):
            made.append(
                pltpu.make_async_remote_copy(
                    src_ref=ysrc.at[d, pl.ds(0, yn)], dst_ref=ydst.at[d, pl.ds(0, yn)],
                    send_sem=send_sem.at[r, d], recv_sem=recv_sem.at[r, d],
                    device_id={"gy": near("gy", step)}, device_id_type=MESH,
                )
            )
            made.append(
                pltpu.make_async_remote_copy(
                    src_ref=zsrc.at[d, pl.ds(0, zn)], dst_ref=zdst.at[d, pl.ds(0, zn)],
                    send_sem=send_sem.at[r, 2 + d], recv_sem=recv_sem.at[r, 2 + d],
                    device_id={"gz": near("gz", step)}, device_id_type=MESH,
                )
            )
            made.append(
                pltpu.make_async_remote_copy(
                    src_ref=sx.at[r, d], dst_ref=rx.at[r, d],
                    send_sem=send_sem.at[r, 4 + d], recv_sem=recv_sem.at[r, 4 + d],
                    device_id={"gx": near("gx", step)}, device_id_type=MESH,
                )
            )
        return made

    def send(r):
        made = copies(r)
        for c in made:
            c.start()
        return made

    def arrive(made):
        for c in made:
            c.wait_recv()

    def x_lo(message, kk, a=None, b=None, wind=None, third=None):
        base = 16 * kk
        if a is not None:
            message = put_l(message, roll_l(a, base + 3), base, 3)
        if b is not None:
            message = put_l(message, roll_l(b, base + 6), base + 3, 3)
        if wind is not None:
            message = put_l(message, roll_l(wind, base + 7), base + 6, 1)
        if third is not None:
            message = put_l(message, roll_l(third, base + 11), base + 8, 3)
        return message

    def x_hi(message, kk, a=None, b=None, third=None):
        base = 16 * kk
        if a is not None:
            message = put_l(message, roll_l(a, base), base, 3)
        if b is not None:
            message = put_l(message, roll_l(b, base + 3), base + 3, 3)
        if third is not None:
            message = put_l(message, roll_l(third, base + 8), base + 8, 3)
        return message

    zero = jnp.zeros((8, 128), F32)

    dep[...] = jnp.zeros_like(dep)
    dep[:, :, 0:16] = depth_in[...]

    def prepare(g, kk, k, state):
        c, p, u, v = fields[0, k], fields[1, k], fields[2, k], fields[3, k]
        w = fields[4, k]
        if kk == 7:
            w = w * jnp.where(g == 1, khi, F32(1.0))
        c0[3 + k] = c
        p0[3 + k] = p
        w0[1 + k] = w
        speed = jnp.abs(u) + jnp.abs(v) + jnp.abs(w)
        state["m"] = speed if kk == 0 else jnp.maximum(state["m"], speed)
        state["lo"] = x_lo(state.get("lo", zero), kk, c, p, u)
        state["hi"] = x_hi(state.get("hi", zero), kk, c, p)
        syw[0, 0, k] = put_s(put_s(roll_s(v, -6), roll_s(p, -3), 2, 3), c, 5, 3)
        syw[0, 1, k] = put_s(c, roll_s(p, 3), 3, 3)
        if kk == 7:
            sx[0, 0, g] = state["lo"]
            sx[0, 1, g] = state["hi"]
            pg[g] = state["m"]

    by_level(prepare)
    for n in range(3):
        szw[0, 0, n] = fields[0, 13 + n]
        szw[0, 0, 3 + n] = fields[1, 13 + n]
        szw[0, 1, n] = fields[0, n]
        szw[0, 1, 3 + n] = fields[1, n]
    szw[0, 0, 6] = w0[16]
    szw[0, 1, 6] = zero
    m1s[...] = jnp.max(jnp.maximum(pg[0], pg[1]), axis=0, keepdims=True)

    pl.semaphore_wait(barrier, len(group1) + len(group2))

    first = []
    for o, (a, b) in enumerate(group1):
        first.append(
            pltpu.make_async_remote_copy(
                src_ref=m1s, dst_ref=m1r.at[o], send_sem=m1_send.at[o], recv_sem=m1_recv.at[o],
                device_id={"gx": near("gx", a), "gz": near("gz", b)}, device_id_type=MESH,
            )
        )
    for c in first:
        c.start()
    round0 = send(0)

    for c in loads:
        c.wait()
    target = lax.broadcasted_iota(jnp.int32, (128, 128), 0).astype(F32).astype(jnp.bfloat16)
    row16 = lax.rem(lax.broadcasted_iota(jnp.int32, (16, 128), 0), 8)

    def deposit_row(kj):
        r = rad[pl.ds(kj, 8, stride=PITCH), :]
        w = wgt[pl.ds(kj, 8, stride=PITCH), :]
        c = col[pl.ds(kj, 8, stride=PITCH), :].astype(F32)
        live = row < counts[pl.ds(kj, 1), :]
        number = jnp.where(live, w, 0.0)
        area = number * (r * r)
        mass = area * r
        lhs = []
        for q in (number, area, mass):
            top = q.astype(jnp.bfloat16).astype(F32)
            pair = jnp.concatenate([top, q - top], axis=0)
            lhs.append(
                jnp.concatenate(
                    [jnp.where(row16 == s, pair, 0.0).astype(jnp.bfloat16) for s in range(8)], axis=1
                )
            )
        lhs = jnp.concatenate(lhs, axis=0)
        hot = jnp.concatenate(
            [
                jnp.where(
                    jnp.broadcast_to(c[s : s + 1, :], (128, 128)).astype(jnp.bfloat16) == target,
                    jnp.bfloat16(1.0), jnp.bfloat16(0.0),
                )
                for s in range(8)
            ],
            axis=1,
        )
        got = lax.dot_general(lhs, hot, (((1,), (1,)), ((), ())), preferred_element_type=F32)
        for m in range(3):
            dmat[pl.ds(pl.multiple_of(kj * 24 + 8 * m, 8), 8), :] = got[16 * m : 16 * m + 8] + got[16 * m + 8 : 16 * m + 16]

    def droplets(part):
        def step(i, carry):
            deposit_row(i * 2)
            deposit_row(i * 2 + 1)
            return carry

        lax.fori_loop(SPLITS[part] // 2, SPLITS[part + 1] // 2, step, 0)

    def by_depth():
        def step(k, carry):
            deep = []
            for s in range(8):
                moved = pltpu.roll(dep[s], lax.rem(128 - k, 128), 1)
                deep.append(jnp.broadcast_to(moved[:, 0:1], (8, 128)))
            for m in range(3):
                got = [dmat[pl.ds(k * 192 + 8 * m + s, 8, stride=24), :] for s in range(8)]
                for d in range(DEPTHS):
                    total = jnp.where(deep[0] == d, got[0], 0.0)
                    for s in range(1, 8):
                        total = total + jnp.where(deep[s] == d, got[s], 0.0)
                    gmat[m, d, k] = total
            return carry

        lax.fori_loop(0, L, step, 0)

    droplets(0)

    for c in first:
        c.wait_recv()
    top = m1s[...]
    for o in range(len(group1)):
        top = jnp.maximum(top, m1r[o])
    m2s[...] = top
    second = []
    for o, a in enumerate(group2):
        second.append(
            pltpu.make_async_remote_copy(
                src_ref=m2s, dst_ref=m2r.at[o], send_sem=m2_send.at[o], recv_sem=m2_recv.at[o],
                device_id={"gy": near("gy", a)}, device_id_type=MESH,
            )
        )
    for c in second:
        c.start()

    def flux(a, q):
        central = 37.0 * (q[2] + q[3]) - 8.0 * (q[1] + q[4]) + (q[0] + q[5])
        upwind = 10.0 * (q[3] - q[2]) - 5.0 * (q[4] - q[1]) + (q[5] - q[0])
        return a * central - jnp.abs(a) * upwind

    def advect(q, k, xh, yh, winds):
        own = q[3 + k]
        u, um, v, vm, w, wm = winds
        line = [xm(own, xh[0], 3), xm(own, xh[0], 2), xm(own, xh[0], 1), own,
                xp(own, xh[1], 1), xp(own, xh[1], 2), xp(own, xh[1], 3)]
        total = flux(u, line[1:]) - flux(um, line[:-1])
        line = [ym(own, yh[0], 3), ym(own, yh[0], 2), ym(own, yh[0], 1), own,
                yp(own, yh[1], 1), yp(own, yh[1], 2), yp(own, yh[1], 3)]
        total = total + (flux(v, line[1:]) - flux(vm, line[:-1]))
        line = [q[k + n] for n in range(7)]
        total = total + (flux(w, line[1:]) - flux(wm, line[:-1]))
        return total * F32(-1.0 / 60.0)

    def x_halos(mx, g, kk):
        lo, hi = mx[0, g], mx[1, g]
        base = 16 * kk
        return (roll_l(lo, 125 - base), roll_l(hi, -base)), (roll_l(lo, 122 - base), roll_l(hi, -base - 3)), roll_l(lo, 121 - base)

    def y_halos(my, k):
        lo, hi = my[0, k], my[1, k]
        return (lo, hi), (roll_s(lo, 3), roll_s(hi, -3)), roll_s(lo, 6)

    def lid_at(g, kk):
        return jnp.where(g == 1, khi, F32(1.0)) if kk == 7 else None

    def masked(value, mask):
        return value if mask is None else value * mask

    arrive(round0)
    for n in range(3):
        c0[n] = rzw[0, 0, n] * klo
        p0[n] = rzw[0, 0, 3 + n] * klo
        c0[19 + n] = rzw[0, 1, n] * khi
        p0[19 + n] = rzw[0, 1, 3 + n] * khi
    w0[0] = rzw[0, 0, 6] * klo
    winc[0] = -10.0 * (p0[3] - p0[2]) * klo
    lift[0] = 0.25 * (c0[2] + c0[3]) * klo

    def build(g, kk, k, state):
        lid = lid_at(g, kk)
        xc, xq, xu = x_halos(rx.at[0], g, kk)
        yc, yq, yv = y_halos(ryw.at[0], k)
        p, u, v = p0[3 + k], fields[2, k], fields[3, k]
        w, wm = w0[1 + k], w0[k]
        um, vm = xm(u, xu, 1), ym(v, yv, 1)
        winds = (u, um, v, vm, w, wm)
        t = advect(c0, k, xc, yc, winds)
        q = advect(p0, k, xq, yq, winds)
        du = -10.0 * (xp(p, xq[1], 1) - p)
        dum = -10.0 * (p - xm(p, xq[0], 1))
        dv = -10.0 * (yp(p, yq[1], 1) - p)
        dvm = -10.0 * (p - ym(p, yq[0], 1))
        dw = masked(-10.0 * (p0[4 + k] - p), lid)
        dwm = winc[k]
        up = masked(0.25 * (c0[3 + k] + c0[4 + k]), lid)
        upm = lift[k]
        a = q - 10.0 * ((u - um) + (v - vm) + (w - wm))
        b = -10.0 * ((du - dum) + (dv - dvm) + ((dw + up) - (dwm + upm)))
        ta[k], aa[k], ba[k] = t, a, b
        uinc[k], vinc[k], winc[1 + k], lift[1 + k] = du, dv, dw, up
        um0[k], vm0[k], uminc[k], vminc[k] = um, vm, dum, dvm
        state["lo"] = x_lo(state.get("lo", zero), kk, t, a, None, b)
        state["hi"] = x_hi(state.get("hi", zero), kk, t, a, b)
        syw[1, 0, k] = put_s(put_s(zero, roll_s(a, -3), 2, 3), t, 5, 3)
        syw[1, 1, k] = put_s(put_s(zero, t, 0, 3), roll_s(a, 3), 3, 3)
        at = 4 * (kk % 2)
        if kk % 2 == 0:
            state["ylo"], state["yhi"] = zero, zero
        state["ylo"] = put_s(state["ylo"], roll_s(b, at + 3), at, 3)
        state["yhi"] = put_s(state["yhi"], roll_s(b, at), at, 3)
        if kk % 2 == 1:
            syw[1, 0, 16 + g * 4 + kk // 2] = state["ylo"]
            syw[1, 1, 16 + g * 4 + kk // 2] = state["yhi"]
        if kk == 7:
            sx[1, 0, g] = state["lo"]
            sx[1, 1, g] = state["hi"]

    by_level(build)
    for i, a in enumerate((ta, aa, ba)):
        for n in range(3):
            szw[1, 0, 3 * i + n] = a[13 + n]
            szw[1, 1, 3 * i + n] = a[n]
    round1 = send(1)
    droplets(1)

    for c in second:
        c.wait_recv()
    top = m2s[...]
    for o in range(len(group2)):
        top = jnp.maximum(top, m2r[o])
    top = jnp.broadcast_to(jnp.max(top, axis=1, keepdims=True), (1, 128))
    time_step = jnp.broadcast_to(0.6 / (1.0 + top), (8, 128))

    arrive(round1)
    t1 = time_step * F32(1.0 / 3.0)
    for d in range(2):
        for g in range(2):
            first_part, rate_part = rx[0, d, g], rx[1, d, g]
            slot = lax.rem(lane, 16)
            third = jnp.where((slot >= 3) & (slot < 6), roll_l(rate_part, -5), 0.0)
            hx[d, g] = first_part + t1 * (rate_part + t1 * third)

    def y_section1(g, kk, k, state):
        for d, at in ((0, 2), (1, 3)):
            third = roll_s(ryw[1, d, 16 + g * 4 + kk // 2], at - 4 * (kk % 2))
            third = jnp.where((row >= at) & (row < at + 3), third, 0.0)
            hy[d, k] = ryw[0, d, k] + t1 * (ryw[1, d, k] + t1 * third)
        cq[3 + k] = c0[3 + k] + t1 * ta[k]
        pq[3 + k] = p0[3 + k] + t1 * (aa[k] + t1 * ba[k])
        uq[k] = fields[2, k] + t1 * uinc[k]
        vq[k] = fields[3, k] + t1 * vinc[k]
        umq[k] = um0[k] + t1 * uminc[k]
        vmq[k] = vm0[k] + t1 * vminc[k]
        wq[1 + k] = w0[1 + k] + t1 * (winc[1 + k] + lift[1 + k])

    by_level(y_section1)
    wq[0] = w0[0] + t1 * (winc[0] + lift[0])
    for n in range(3):
        for d, to, keep in ((0, n, klo), (1, 19 + n, khi)):
            cq[to] = c0[to] + (t1 * keep) * rzw[1, d, n]
            pq[to] = p0[to] + (t1 * keep) * (rzw[1, d, 3 + n] + t1 * rzw[1, d, 6 + n])

    def rates(mx, my):
        def step(g, kk, k, state):
            xc, xq, _ = x_halos(mx, g, kk)
            yc, yq, _ = y_halos(my, k)
            winds = (uq[k], umq[k], vq[k], vmq[k], wq[1 + k], wq[k])
            tr[k] = advect(cq, k, xc, yc, winds)
            pr[k] = advect(pq, k, xq, yq, winds)
            lift[1 + k] = masked(0.25 * (cq[3 + k] + cq[4 + k]), lid_at(g, kk))

        by_level(step)
        lift[0] = 0.25 * (cq[2] + cq[3]) * klo

    def narrow_messages(r, g, kk, k, state, p, u, v):
        w = NARROW[r]
        state["lo"] = x_lo(state.get("lo", zero), kk, None, p, u)
        state["hi"] = x_hi(state.get("hi", zero), kk, None, p)
        at = 2 * (kk % 4)
        if kk % 4 == 0:
            state["ylo"], state["yhi"] = zero, zero
        state["ylo"] = put_s(put_s(state["ylo"], roll_s(p, at + 1), at, 1), roll_s(v, at + 2), at + 1, 1)
        state["yhi"] = put_s(state["yhi"], roll_s(p, at), at, 1)
        if kk % 4 == 3:
            sya[w, 0, g * 2 + kk // 4] = state["ylo"]
            sya[w, 1, g * 2 + kk // 4] = state["yhi"]
        if kk == 7:
            sx[r, 0, g] = state["lo"]
            sx[r, 1, g] = state["hi"]

    def narrow_z(r, p, w):
        n = NARROW[r]
        sza[n, 0, 0] = p[16]
        sza[n, 0, 1] = w[16]
        sza[n, 1, 0] = p[1]
        sza[n, 1, 1] = zero

    def first_substep(r, s, to):
        po, uo, vo, wo = to

        def step(g, kk, k, state):
            u = fields[2, k] + s * uinc[k]
            um = um0[k] + s * uminc[k]
            v = fields[3, k] + s * vinc[k]
            vm = vm0[k] + s * vminc[k]
            w = w0[1 + k] + s * (winc[1 + k] + lift[1 + k])
            wm = w0[k] + s * (winc[k] + lift[k])
            p = p0[3 + k] + s * (pr[k] - 10.0 * ((u - um) + (v - vm) + (w - wm)))
            po[1 + k], uo[k], vo[k], wo[1 + k] = p, u, v, w
            narrow_messages(r, g, kk, k, state, p, u, v)

        by_level(step)
        narrow_z(r, po, wo)
        return send(r)

    def next_substep(r, made, s, source, finish):
        n = NARROW[r]
        ps, us, vs, ws = source
        arrive(made)
        ps[0] = rza[n, 0, 0] * klo
        ws[0] = rza[n, 0, 1] * klo
        ps[17] = rza[n, 1, 0] * khi
        s10 = s * 10.0

        def step(g, kk, k, state):
            lid = lid_at(g, kk)
            _, xq, xu = x_halos(rx.at[r], g, kk)
            ylo, yhi = rya[n, 0, g * 2 + kk // 4], rya[n, 1, g * 2 + kk // 4]
            at = 2 * (kk % 4)
            p, u, v = ps[1 + k], us[k], vs[k]
            un = u - s10 * (xp(p, xq[1], 1) - p)
            um = xm(u, xu, 1) - s10 * (p - xm(p, xq[0], 1))
            vn = v - s10 * (yp(p, roll_s(yhi, -at), 1) - p)
            vm = ym(v, roll_s(ylo, 6 - at), 1) - s10 * (p - ym(p, roll_s(ylo, 7 - at), 1))
            wn = ws[1 + k] + s * lift[1 + k] - masked(s10 * (ps[2 + k] - p), lid)
            below = s10 * (p - ps[k])
            if kk == 0:
                below = below * jnp.where(g == 0, klo, F32(1.0))
            wm = ws[k] + s * lift[k] - below
            pn = p + s * (pr[k] - 10.0 * ((un - um) + (vn - vm) + (wn - wm)))
            finish(g, kk, k, state, pn, un, vn, wn)

        by_level(step)

    rates(hx, hy)
    t2 = time_step * F32(0.25)
    round2 = first_substep(2, t2, (pf, uf, vf, wf))
    droplets(2)

    half = time_step * F32(0.5)

    def finish2(g, kk, k, state, p, u, v, w):
        c = c0[3 + k] + half * tr[k]
        cq[3 + k], pq[3 + k], uq[k], vq[k], wq[1 + k] = c, p, u, v, w
        state["lo"] = x_lo(state.get("lo", zero), kk, c, p, u)
        state["hi"] = x_hi(state.get("hi", zero), kk, c, p)
        syw[2, 0, k] = put_s(put_s(roll_s(v, -6), roll_s(p, -3), 2, 3), c, 5, 3)
        syw[2, 1, k] = put_s(c, roll_s(p, 3), 3, 3)
        if kk == 7:
            sx[3, 0, g] = state["lo"]
            sx[3, 1, g] = state["hi"]

    next_substep(2, round2, t2, (pf, uf, vf, wf), finish2)
    for n in range(3):
        szw[2, 0, n] = cq[16 + n]
        szw[2, 0, 3 + n] = pq[16 + n]
        szw[2, 1, n] = cq[3 + n]
        szw[2, 1, 3 + n] = pq[3 + n]
    szw[2, 0, 6] = wq[16]
    szw[2, 1, 6] = zero
    round3 = send(3)
    droplets(3)
    by_depth()

    arrive(round3)
    for n in range(3):
        cq[n] = rzw[2, 0, n] * klo
        pq[n] = rzw[2, 0, 3 + n] * klo
        cq[19 + n] = rzw[2, 1, n] * khi
        pq[19 + n] = rzw[2, 1, 3 + n] * khi
    wq[0] = rzw[2, 0, 6] * klo

    def face_winds(g, kk, k, state):
        _, _, xu = x_halos(rx.at[3], g, kk)
        _, _, yv = y_halos(ryw.at[2], k)
        umq[k] = xm(uq[k], xu, 1)
        vmq[k] = ym(vq[k], yv, 1)

    by_level(face_winds)
    rates(rx.at[3], ryw.at[2])
    t3 = time_step * F32(0.25)
    round4 = first_substep(4, t3, (pf, uf, vf, wf))

    for k in range(L):
        c = c0[3 + k] + time_step * tr[k]
        out[0, k] = c
        growth = jnp.minimum(jnp.exp(0.3 * c), F32(3.0e38))
        ta[k] = growth
        aa[k] = jnp.sqrt(growth)

    def landed(t):
        totals = [None, None, None]
        for k in range(max(t, 0), min(t + DEPTHS, L)):
            d = k - t
            grow, root = ta[k], aa[k]
            parts = (gmat[0, d, k], gmat[1, d, k] * grow, gmat[2, d, k] * grow * root)
            totals = [a if b is None else b + a for a, b in zip(parts, totals)]
        return totals

    for t in range(-8, 0):
        for m, value in enumerate(landed(t)):
            ext[m, t + 8] = value
    dropped = pltpu.make_async_remote_copy(
        src_ref=ext, dst_ref=fall, send_sem=fall_sem.at[0], recv_sem=fall_sem.at[1],
        device_id={"gz": near("gz", -1)}, device_id_type=MESH,
    )
    dropped.start()
    for t in range(0, L):
        for m, value in enumerate(landed(t)):
            mom[m, t] = value

    def passing(r, to):
        po, uo, vo, wo = to

        def finish(g, kk, k, state, p, u, v, w):
            po[1 + k], uo[k], vo[k], wo[1 + k] = p, u, v, w
            narrow_messages(r, g, kk, k, state, p, u, v)

        return finish

    next_substep(4, round4, t3, (pf, uf, vf, wf), passing(5, (pg, ug, vg, wg)))
    narrow_z(5, pg, wg)
    round5 = send(5)
    next_substep(5, round5, t3, (pg, ug, vg, wg), passing(6, (pf, uf, vf, wf)))
    narrow_z(6, pf, wf)
    round6 = send(6)
    dropped.wait_recv()
    for m in range(3):
        for n in range(8):
            mom[m, 8 + n] = mom[m, 8 + n] + fall[m, n] * khi

    def last(g, kk, k, state, p, u, v, w):
        out[1, k], out[2, k], out[3, k], out[4, k] = p, u, v, w

    next_substep(6, round6, t3, (pf, uf, vf, wf), last)

    dropped.wait_send()
    for made in (first, second, round0, round1, round2, round3, round4, round5, round6):
        for c in made:
            c.wait_send()


def solution(mesh):
    sizes = (mesh.shape["gx"], mesh.shape["gy"], mesh.shape["gz"])
    nx, ny, nz = sizes
    vm = lambda *shape: pltpu.VMEM(shape + (8, 128), F32)
    dma = pltpu.SemaphoreType.DMA
    scratch = [
        pltpu.VMEM((8 * PITCH, 128), F32), pltpu.VMEM((8 * PITCH, 128), F32), pltpu.VMEM((8 * PITCH, 128), jnp.int32),
        pltpu.VMEM((8, 8, 128), jnp.int32), pltpu.VMEM((128 * 24, 128), F32), vm(3, DEPTHS, L), vm(3, 8), vm(3, 8),
        vm(22), vm(22), vm(17), vm(22), vm(22), vm(17), vm(16), vm(16), vm(16), vm(16),
        vm(16), vm(16), vm(16), vm(16), vm(16), vm(17), vm(16), vm(16), vm(16), vm(16),
        vm(16), vm(16), vm(17), vm(18), vm(16), vm(16), vm(17), vm(18), vm(16), vm(16), vm(17),
        vm(2, 2), vm(2, 16),
        vm(7, 2, 2), vm(7, 2, 2), vm(3, 2, 24), vm(3, 2, 24), vm(4, 2, 4), vm(4, 2, 4),
        vm(3, 2, 9), vm(3, 2, 9), vm(4, 2, 2), vm(4, 2, 2),
        pltpu.VMEM((1, 128), F32), pltpu.VMEM((nx * nz - 1, 1, 128), F32),
        pltpu.VMEM((1, 128), F32), pltpu.VMEM((ny - 1, 1, 128), F32),
        dma((7, 6)), dma((7, 6)), dma((nx * nz - 1,)), dma((nx * nz - 1,)), dma((ny - 1,)), dma((ny - 1,)),
        dma((2,)), dma((3, 8)),
    ]
    vmem = pl.BlockSpec(memory_space=pltpu.VMEM)
    hbm = pl.BlockSpec(memory_space=pl.ANY)

    def per_device(fields, radius, weight, column, counts, fall_depth):
        return pl.pallas_call(
            functools.partial(kernel, sizes),
            out_shape=(
                jax.ShapeDtypeStruct((5, L, 8, 128), F32),
                jax.ShapeDtypeStruct((3, L, 8, 128), F32),
            ),
            in_specs=[vmem, vmem, vmem, hbm, hbm, hbm],
            out_specs=(vmem, vmem),
            scratch_shapes=scratch,
            compiler_params=pltpu.CompilerParams(collective_id=0, has_side_effects=True),
            name="slab_step",
        )(
            fields,
            counts.reshape(128, 128),
            jnp.transpose(fall_depth[:, :, :, 0], (0, 2, 1)),
            radius.reshape(1024, 128),
            weight.reshape(1024, 128),
            column.reshape(1024, 128),
        )

    cut = P(None, "gz", "gy", "gx")
    return jax.shard_map(
        per_device,
        mesh=mesh,
        in_specs=(cut, cut, cut, cut, P("gz", "gy", "gx"), cut),
        out_specs=(cut, cut),
        check_vma=False,
    )
```

```python
import functools

import jax
import jax.numpy as jnp
from jax import lax
from jax.experimental import pallas as pl
from jax.experimental.pallas import tpu as pltpu
from jax.sharding import PartitionSpec as P

MESH = pl.DeviceIdType.MESH
F32 = jnp.float32
L = 16
DEPTHS = 9
PITCH = 136
Y_TILES = {0: (14, 12), 1: (18, 18), 7: (6, 6), 3: (6, 6), 2: (2, 2), 4: (2, 2), 5: (2, 2), 6: (2, 2)}
Z_TILES = {0: (7, 6), 1: (9, 9), 7: (3, 3), 3: (3, 3), 2: (1, 1), 4: (1, 1), 5: (1, 1), 6: (1, 1)}
Y_AT = {0: 0, 1: 14, 7: 32, 3: 38, 2: 44, 4: 46, 5: 48, 6: 50}
Z_AT = {0: 0, 1: 7, 7: 16, 3: 19, 2: 22, 4: 23, 5: 24, 6: 25}
Y_ALL, Z_ALL = 52, 26
SPLITS = (0, 24, 58, 80, 100, 128)


def kernel(
    sizes,
    fields_h, counts_h, depth_h, rad_h, wgt_h, col_h,
    out, mom,
    fields, counts, depth_in, rad, wgt, col, dep, dmat, gmat, ext, fall,
    c0, p0, w0, cq, pq, peak,
    ta, aa, ba, uinc, vinc, winc, um0, vm0, uminc, vminc,
    tr, lift, pf, pg, uf, vf, umf, vmf, wf, ug, vg, umg, vmg, wg,
    hx, hy,
    sx, rx, sy, ry, sz, rz,
    m1s, m1r, m2s, m2r,
    send_sem, recv_sem, m1_send, m1_recv, m2_send, m2_recv, fall_sem, load_sem, field_sem,
):
    nx, ny, nz = sizes
    ix, iy, iz = lax.axis_index("gx"), lax.axis_index("gy"), lax.axis_index("gz")

    def near(axis, step):
        i, n = {"gx": (ix, nx), "gy": (iy, ny), "gz": (iz, nz)}[axis]
        return lax.rem(i + (step + n), n)

    group1 = [(a, b) for a in range(nx) for b in range(nz) if (a, b) != (0, 0)]
    group2 = list(range(1, ny))
    barrier = pltpu.get_barrier_semaphore()
    for a in group2:
        pl.semaphore_signal(barrier, inc=1, device_id={"gy": near("gy", a)}, device_id_type=MESH)
    for a, b in group1:
        pl.semaphore_signal(
            barrier, inc=1, device_id={"gx": near("gx", a), "gz": near("gz", b)}, device_id_type=MESH
        )

    early = [
        pltpu.make_async_copy(src, dst, field_sem.at[n])
        for n, (src, dst) in enumerate(((fields_h, fields), (counts_h, counts), (depth_h, depth_in)))
    ]
    loads = []
    for a, (src, dst) in enumerate(((rad_h, rad), (wgt_h, wgt), (col_h, col))):
        for s in range(8):
            loads.append(
                pltpu.make_async_copy(
                    src.at[pl.ds(s * 128, 128)], dst.at[pl.ds(s * PITCH, 128)], load_sem.at[a, s]
                )
            )
    for c in early:
        c.start()

    lane = lax.broadcasted_iota(jnp.int32, (8, 128), 1)
    row = lax.broadcasted_iota(jnp.int32, (8, 128), 0)
    klo = (iz > 0).astype(F32)
    khi = (iz < nz - 1).astype(F32)
    zero = jnp.zeros((8, 128), F32)

    def roll_l(x, s):
        s = s % 128
        return pltpu.roll(x, s, 1) if s else x

    def roll_s(x, s):
        s = s % 8
        return pltpu.roll(x, s, 0) if s else x

    def xp(q, h, n):
        return roll_l(jnp.where(lane < n, h, q), -n)

    def xm(q, h, n):
        return roll_l(jnp.where(lane >= 128 - n, h, q), n)

    def yp(q, h, n):
        return roll_s(jnp.where(row < n, h, q), -n)

    def ym(q, h, n):
        return roll_s(jnp.where(row >= 8 - n, h, q), n)

    def put_l(message, value, at, width):
        return jnp.where((lane >= at) & (lane < at + width), value, message)

    def by_level(fn):
        def group(g, carry):
            state = {}
            for kk in range(8):
                fn(g, kk, g * 8 + kk, state)
            return carry

        lax.fori_loop(0, 2, group, 0)

    def copies(r):
        made = []
        for d, step in ((0, 1), (1, -1)):
            y, z = pl.ds(Y_AT[r], Y_TILES[r][d]), pl.ds(Z_AT[r], Z_TILES[r][d])
            for i, (src, dst, axis) in enumerate(
                ((sy.at[d, y], ry.at[d, y], "gy"), (sz.at[d, z], rz.at[d, z], "gz"), (sx.at[r, d], rx.at[r, d], "gx"))
            ):
                made.append(
                    pltpu.make_async_remote_copy(
                        src_ref=src, dst_ref=dst,
                        send_sem=send_sem.at[r, 2 * i + d], recv_sem=recv_sem.at[r, 2 * i + d],
                        device_id={axis: near(axis, step)}, device_id_type=MESH,
                    )
                )
        return made

    def send(r):
        made = copies(r)
        for c in made:
            c.start()
        return made

    def arrive(made):
        for c in made:
            c.wait_recv()

    def x_pack(state, r, g, kk, a=None, b=None, wind=None, third=None):
        base = 16 * kk
        lo, hi = state.get("xlo", zero), state.get("xhi", zero)
        for value, at in ((a, 0), (b, 3), (third, 8)):
            if value is not None:
                lo = put_l(lo, roll_l(value, base + at + 3), base + at, 3)
                hi = put_l(hi, roll_l(value, base + at), base + at, 3)
        if wind is not None:
            lo = put_l(lo, roll_l(wind, base + 7), base + 6, 1)
        state["xlo"], state["xhi"] = lo, hi
        if kk == 7:
            sx[r, 0, g] = lo
            sx[r, 1, g] = hi

    def y_pack3(state, name, start, g, kk, q):
        t, o = divmod(3 * kk, 8)
        for d, moved in ((0, roll_s(q, o - 5)), (1, roll_s(q, o))):
            key = (name, d)
            tiles = state.setdefault(key, [None, None, None])
            if tiles[t] is None:
                tiles[t] = moved
            else:
                tiles[t] = jnp.where(row >= o, moved, tiles[t])
            if o > 5:
                tiles[t + 1] = moved
            if o >= 5:
                sy[d, start + g * 3 + t] = tiles[t]

    def y_halo3(ref, start, g, kk):
        t, o = divmod(3 * kk, 8)
        got = []
        for d in range(2):
            value = ref[d, start + g * 3 + t]
            if o > 5:
                value = jnp.where(row >= o, value, ref[d, start + g * 3 + t + 1])
            got.append(roll_s(value, 5 - o if d == 0 else -o))
        return got

    def y_pack1(state, name, start, g, kk, last=None, first=None):
        for d, value, by in ((0, last, kk - 7), (1, first, kk)):
            if value is not None:
                key = (name, d)
                moved = roll_s(value, by)
                state[key] = moved if kk == 0 else jnp.where(row >= kk, moved, state[key])
                if kk == 7:
                    sy[d, start + g] = state[key]

    def x_halos(mx, g, kk):
        lo, hi = mx[0, g], mx[1, g]
        base = 16 * kk
        return (roll_l(lo, 125 - base), roll_l(hi, -base)), (roll_l(lo, 122 - base), roll_l(hi, -base - 3)), roll_l(lo, 121 - base)

    def x_halo(ref, at, g, kk):
        base = 16 * kk + at
        return roll_l(ref[0, g], 125 - base), roll_l(ref[1, g], -base)

    def lid_at(g, kk):
        return jnp.where(g == 1, khi, F32(1.0)) if kk == 7 else None

    def masked(value, mask):
        return value if mask is None else value * mask

    early[0].wait()
    for c in loads:
        c.start()

    def prepare(g, kk, k, state):
        c, p, u, v = fields[0, k], fields[1, k], fields[2, k], fields[3, k]
        w = masked(fields[4, k], lid_at(g, kk))
        c0[3 + k] = c
        p0[3 + k] = p
        w0[1 + k] = w
        speed = jnp.abs(u) + jnp.abs(v) + jnp.abs(w)
        state["m"] = speed if kk == 0 else jnp.maximum(state["m"], speed)
        x_pack(state, 0, g, kk, c, p, u)
        y_pack3(state, "c", Y_AT[0], g, kk, c)
        y_pack3(state, "p", Y_AT[0] + 6, g, kk, p)
        y_pack1(state, "v", Y_AT[0] + 12, g, kk, last=v)
        if kk == 7:
            peak[g] = state["m"]

    by_level(prepare)
    for n in range(3):
        sz[0, Z_AT[0] + n] = fields[0, 13 + n]
        sz[0, Z_AT[0] + 3 + n] = fields[1, 13 + n]
        sz[1, Z_AT[0] + n] = fields[0, n]
        sz[1, Z_AT[0] + 3 + n] = fields[1, n]
    sz[0, Z_AT[0] + 6] = w0[16]
    m1s[...] = jnp.max(jnp.maximum(peak[0], peak[1]), axis=0, keepdims=True)

    target = lax.broadcasted_iota(jnp.int32, (128, 128), 0).astype(F32).astype(jnp.bfloat16)
    row16 = lax.rem(lax.broadcasted_iota(jnp.int32, (16, 128), 0), 8)

    def deposit_row(kj):
        r = rad[pl.ds(kj, 8, stride=PITCH), :]
        w = wgt[pl.ds(kj, 8, stride=PITCH), :]
        c = col[pl.ds(kj, 8, stride=PITCH), :].astype(F32)
        live = row < counts[pl.ds(kj, 1), :]
        number = jnp.where(live, w, 0.0)
        area = number * (r * r)
        mass = area * r
        lhs = []
        for q in (number, area, mass):
            top = q.astype(jnp.bfloat16).astype(F32)
            pair = jnp.concatenate([top, q - top], axis=0)
            lhs.append(
                jnp.concatenate(
                    [jnp.where(row16 == s, pair, 0.0).astype(jnp.bfloat16) for s in range(8)], axis=1
                )
            )
        lhs = jnp.concatenate(lhs, axis=0)
        hot = jnp.concatenate(
            [
                jnp.where(
                    jnp.broadcast_to(c[s : s + 1, :], (128, 128)).astype(jnp.bfloat16) == target,
                    jnp.bfloat16(1.0), jnp.bfloat16(0.0),
                )
                for s in range(8)
            ],
            axis=1,
        )
        got = lax.dot_general(lhs, hot, (((1,), (1,)), ((), ())), preferred_element_type=F32)
        for m in range(3):
            dmat[pl.ds(pl.multiple_of(kj * 24 + 8 * m, 8), 8), :] = got[16 * m : 16 * m + 8] + got[16 * m + 8 : 16 * m + 16]

    def droplets(part):
        def step(i, carry):
            deposit_row(i * 2)
            deposit_row(i * 2 + 1)
            return carry

        lax.fori_loop(SPLITS[part] // 2, SPLITS[part + 1] // 2, step, 0)

    def by_depth():
        def step(k, carry):
            deep = []
            for s in range(8):
                moved = pltpu.roll(dep[s], lax.rem(128 - k, 128), 1)
                deep.append(jnp.broadcast_to(moved[:, 0:1], (8, 128)))
            for m in range(3):
                got = [dmat[pl.ds(k * 192 + 8 * m + s, 8, stride=24), :] for s in range(8)]
                for d in range(DEPTHS):
                    total = jnp.where(deep[0] == d, got[0], 0.0)
                    for s in range(1, 8):
                        total = total + jnp.where(deep[s] == d, got[s], 0.0)
                    gmat[m, d, k] = total
            return carry

        lax.fori_loop(0, L, step, 0)

    pl.semaphore_wait(barrier, len(group1) + len(group2))

    first = []
    for o, (a, b) in enumerate(group1):
        first.append(
            pltpu.make_async_remote_copy(
                src_ref=m1s, dst_ref=m1r.at[o], send_sem=m1_send.at[o], recv_sem=m1_recv.at[o],
                device_id={"gx": near("gx", a), "gz": near("gz", b)}, device_id_type=MESH,
            )
        )
    for c in first:
        c.start()
    round0 = send(0)
    for c in early[1:] + loads:
        c.wait()
    dep[...] = jnp.zeros_like(dep)
    dep[:, :, 0:16] = depth_in[...]
    droplets(0)

    def flux(a, q):
        central = 37.0 * (q[2] + q[3]) - 8.0 * (q[1] + q[4]) + (q[0] + q[5])
        upwind = 10.0 * (q[3] - q[2]) - 5.0 * (q[4] - q[1]) + (q[5] - q[0])
        return a * central - jnp.abs(a) * upwind

    def advect(q, k, xh, yh, winds):
        own = q[3 + k]
        u, um, v, vm, w, wm = winds
        line = [xm(own, xh[0], 3), xm(own, xh[0], 2), xm(own, xh[0], 1), own,
                xp(own, xh[1], 1), xp(own, xh[1], 2), xp(own, xh[1], 3)]
        total = flux(u, line[1:]) - flux(um, line[:-1])
        line = [ym(own, yh[0], 3), ym(own, yh[0], 2), ym(own, yh[0], 1), own,
                yp(own, yh[1], 1), yp(own, yh[1], 2), yp(own, yh[1], 3)]
        total = total + (flux(v, line[1:]) - flux(vm, line[:-1]))
        line = [q[k + n] for n in range(7)]
        total = total + (flux(w, line[1:]) - flux(wm, line[:-1]))
        return total * F32(-1.0 / 60.0)

    arrive(round0)
    for n in range(3):
        for d, to, keep in ((0, n, klo), (1, 19 + n, khi)):
            c0[to] = rz[d, Z_AT[0] + n] * keep
            p0[to] = rz[d, Z_AT[0] + 3 + n] * keep
    w0[0] = rz[0, Z_AT[0] + 6] * klo
    winc[0] = -10.0 * (p0[3] - p0[2]) * klo
    lift[0] = 0.25 * (c0[2] + c0[3]) * klo

    def build(g, kk, k, state):
        lid = lid_at(g, kk)
        xc, xq, xu = x_halos(rx.at[0], g, kk)
        yc = y_halo3(ry, Y_AT[0], g, kk)
        yq = y_halo3(ry, Y_AT[0] + 6, g, kk)
        yv = roll_s(ry[0, Y_AT[0] + 12 + g], 7 - kk)
        p, u, v = p0[3 + k], fields[2, k], fields[3, k]
        w, wm = w0[1 + k], w0[k]
        um, vm = xm(u, xu, 1), ym(v, yv, 1)
        winds = (u, um, v, vm, w, wm)
        t = advect(c0, k, xc, yc, winds)
        q = advect(p0, k, xq, yq, winds)
        du = -10.0 * (xp(p, xq[1], 1) - p)
        dum = -10.0 * (p - xm(p, xq[0], 1))
        dv = -10.0 * (yp(p, yq[1], 1) - p)
        dvm = -10.0 * (p - ym(p, yq[0], 1))
        dw = masked(-10.0 * (p0[4 + k] - p), lid)
        dwm = winc[k]
        up = masked(0.25 * (c0[3 + k] + c0[4 + k]), lid)
        upm = lift[k]
        a = q - 10.0 * ((u - um) + (v - vm) + (w - wm))
        b = -10.0 * ((du - dum) + (dv - dvm) + ((dw + up) - (dwm + upm)))
        ta[k], aa[k], ba[k] = t, a, b
        uinc[k], vinc[k], winc[1 + k], lift[1 + k] = du, dv, dw, up
        um0[k], vm0[k], uminc[k], vminc[k] = um, vm, dum, dvm
        x_pack(state, 1, g, kk, t, a, None, b)
        for i, value in enumerate((t, a, b)):
            y_pack3(state, i, Y_AT[1] + 6 * i, g, kk, value)

    by_level(build)
    for i, a in enumerate((ta, aa, ba)):
        for n in range(3):
            sz[0, Z_AT[1] + 3 * i + n] = a[13 + n]
            sz[1, Z_AT[1] + 3 * i + n] = a[n]
    round1 = send(1)

    for c in first:
        c.wait_recv()
    top = m1s[...]
    for o in range(len(group1)):
        top = jnp.maximum(top, m1r[o])
    m2s[...] = top
    second = []
    for o, a in enumerate(group2):
        second.append(
            pltpu.make_async_remote_copy(
                src_ref=m2s, dst_ref=m2r.at[o], send_sem=m2_send.at[o], recv_sem=m2_recv.at[o],
                device_id={"gy": near("gy", a)}, device_id_type=MESH,
            )
        )
    for c in second:
        c.start()

    droplets(1)

    for c in second:
        c.wait_recv()
    top = m2s[...]
    for o in range(len(group2)):
        top = jnp.maximum(top, m2r[o])
    top = jnp.broadcast_to(jnp.max(top, axis=1, keepdims=True), (1, 128))
    time_step = jnp.broadcast_to(0.6 / (1.0 + top), (8, 128))

    arrive(round1)
    t1 = time_step * F32(1.0 / 3.0)
    slot = lax.rem(lane, 16)
    for d in range(2):
        for g in range(2):
            third = jnp.where((slot >= 3) & (slot < 6), roll_l(rx[1, d, g], -5), 0.0)
            hx[d, g] = rx[0, d, g] + t1 * (rx[1, d, g] + t1 * third)
        for n in range(6):
            hy[d, n] = ry[d, n] + t1 * ry[d, 14 + n]
            hy[d, 6 + n] = ry[d, 6 + n] + t1 * (ry[d, 20 + n] + t1 * ry[d, 26 + n])

    def section1(g, kk, k, state):
        cq[3 + k] = c0[3 + k] + t1 * ta[k]
        pq[3 + k] = p0[3 + k] + t1 * (aa[k] + t1 * ba[k])
        uf[k] = fields[2, k] + t1 * uinc[k]
        vf[k] = fields[3, k] + t1 * vinc[k]
        umf[k] = um0[k] + t1 * uminc[k]
        vmf[k] = vm0[k] + t1 * vminc[k]
        wf[1 + k] = w0[1 + k] + t1 * (winc[1 + k] + lift[1 + k])

    by_level(section1)
    wf[0] = w0[0] + t1 * (winc[0] + lift[0])
    for n in range(3):
        for d, to, keep in ((0, n, klo), (1, 19 + n, khi)):
            cq[to] = c0[to] + (t1 * keep) * rz[d, Z_AT[1] + n]
            pq[to] = p0[to] + (t1 * keep) * (rz[d, Z_AT[1] + 3 + n] + t1 * rz[d, Z_AT[1] + 6 + n])

    def tracer_rates(mx, my, start, old, finish):
        u, v, um, vm, w = old

        def step(g, kk, k, state):
            winds = (u[k], um[k], v[k], vm[k], w[1 + k], w[k])
            finish(g, kk, k, state, advect(cq, k, x_halo(mx, 0, g, kk), y_halo3(my, start, g, kk), winds))

        by_level(step)

    def lifts():
        lift[0] = 0.25 * (cq[2] + cq[3]) * klo

        def step(g, kk, k, state):
            lift[1 + k] = masked(0.25 * (cq[3 + k] + cq[4 + k]), lid_at(g, kk))

        by_level(step)

    def narrow(r, g, kk, k, state, p):
        x_pack(state, r, g, kk, None, p)
        y_pack1(state, "p", Y_AT[r], g, kk, last=p, first=p)

    def narrow_send(r, p):
        sz[0, Z_AT[r]] = p[16]
        sz[1, Z_AT[r]] = p[1]
        return send(r)

    def first_substep(r, s, mx, my, start, old, new, rate_ref):
        u_, v_, um_, vm_, w_ = old
        un_, vn_, umn_, vmn_, wn_ = new
        wn_[0] = w0[0] + s * (winc[0] + lift[0])

        def step(g, kk, k, state):
            winds = (u_[k], um_[k], v_[k], vm_[k], w_[1 + k], w_[k])
            rate = advect(pq, k, x_halo(mx, 3, g, kk), y_halo3(my, start, g, kk), winds)
            rate_ref[k] = rate
            u = fields[2, k] + s * uinc[k]
            um = um0[k] + s * uminc[k]
            v = fields[3, k] + s * vinc[k]
            vm = vm0[k] + s * vminc[k]
            w = w0[1 + k] + s * (winc[1 + k] + lift[1 + k])
            wm = w0[k] + s * (winc[k] + lift[k])
            p = p0[3 + k] + s * (rate - 10.0 * ((u - um) + (v - vm) + (w - wm)))
            pf[1 + k], un_[k], vn_[k], umn_[k], vmn_[k], wn_[1 + k] = p, u, v, um, vm, w
            narrow(r, g, kk, k, state, p)

        by_level(step)
        return narrow_send(r, pf)

    def next_substep(r, made, s, ps, winds, rate_ref, finish):
        u_, v_, um_, vm_, w_ = winds
        s10 = s * 10.0
        arrive(made)
        ps[0] = rz[0, Z_AT[r]] * klo
        ps[17] = rz[1, Z_AT[r]] * khi
        w_[0] = w_[0] + s * lift[0] - (s10 * klo) * (ps[1] - ps[0])

        def step(g, kk, k, state):
            lid = lid_at(g, kk)
            xq = x_halo(rx.at[r], 3, g, kk)
            p = ps[1 + k]
            ylo, yhi = roll_s(ry[0, Y_AT[r] + g], 7 - kk), roll_s(ry[1, Y_AT[r] + g], -kk)
            u = u_[k] - s10 * (xp(p, xq[1], 1) - p)
            um = um_[k] - s10 * (p - xm(p, xq[0], 1))
            v = v_[k] - s10 * (yp(p, yhi, 1) - p)
            vm = vm_[k] - s10 * (p - ym(p, ylo, 1))
            w = w_[1 + k] + s * lift[1 + k] - masked(s10 * (ps[2 + k] - p), lid)
            wm = state["w"] if kk else w_[k]
            state["w"] = w
            pn = p + s * (rate_ref[k] - 10.0 * ((u - um) + (v - vm) + (w - wm)))
            finish(g, kk, k, state, pn, u, v, um, vm, w)

        by_level(step)

    state_f = (uf, vf, umf, vmf, wf)
    state_g = (ug, vg, umg, vmg, wg)

    t2 = time_step * F32(0.25)
    half = time_step * F32(0.5)
    lifts()
    round2 = first_substep(2, t2, hx, hy, 6, state_f, state_g, aa)

    def tracer2(g, kk, k, state, rate):
        c = c0[3 + k] + half * rate
        tr[k] = c
        x_pack(state, 7, g, kk, c)
        y_pack3(state, "c", Y_AT[7], g, kk, c)

    tracer_rates(hx, hy, 0, state_f, tracer2)
    for n in range(3):
        sz[0, Z_AT[7] + n] = tr[13 + n]
        sz[1, Z_AT[7] + n] = tr[n]
    round7 = send(7)
    droplets(2)

    def finish2(g, kk, k, state, p, u, v, um, vm, w):
        pq[3 + k] = p
        ug[k], vg[k], umg[k], vmg[k], wg[1 + k] = u, v, um, vm, w
        cq[3 + k] = tr[k]
        x_pack(state, 3, g, kk, None, p)
        y_pack3(state, "p", Y_AT[3], g, kk, p)

    next_substep(2, round2, t2, pf, state_g, aa, finish2)
    for n in range(3):
        sz[0, Z_AT[3] + n] = pq[16 + n]
        sz[1, Z_AT[3] + n] = pq[3 + n]
    round3 = send(3)

    arrive(round7)
    for n in range(3):
        for d, to, keep in ((0, n, klo), (1, 19 + n, khi)):
            cq[to] = rz[d, Z_AT[7] + n] * keep
    lifts()

    def tracer3(g, kk, k, state, rate):
        c = c0[3 + k] + time_step * rate
        out[0, k] = c
        growth = jnp.minimum(jnp.exp(0.3 * c), F32(3.0e38))
        ta[k] = growth
        ba[k] = jnp.sqrt(growth)

    tracer_rates(rx.at[7], ry, Y_AT[7], state_g, tracer3)

    droplets(3)
    arrive(round3)
    for n in range(3):
        for d, to, keep in ((0, n, klo), (1, 19 + n, khi)):
            pq[to] = rz[d, Z_AT[3] + n] * keep
    t3 = time_step * F32(0.25)
    round4 = first_substep(4, t3, rx.at[3], ry, Y_AT[3], state_g, state_f, aa)
    droplets(4)

    def passing(r, to):
        def finish(g, kk, k, state, p, u, v, um, vm, w):
            to[1 + k] = p
            uf[k], vf[k], umf[k], vmf[k], wf[1 + k] = u, v, um, vm, w
            narrow(r, g, kk, k, state, p)

        return finish

    next_substep(4, round4, t3, pf, state_f, aa, passing(5, pg))
    round5 = narrow_send(5, pg)
    by_depth()

    def landed(t):
        totals = [None, None, None]
        for k in range(max(t, 0), min(t + DEPTHS, L)):
            d = k - t
            grow, root = ta[k], ba[k]
            parts = (gmat[0, d, k], gmat[1, d, k] * grow, gmat[2, d, k] * grow * root)
            totals = [a if b is None else b + a for a, b in zip(parts, totals)]
        return totals

    for t in range(-8, 0):
        for m, value in enumerate(landed(t)):
            ext[m, t + 8] = value
    dropped = pltpu.make_async_remote_copy(
        src_ref=ext, dst_ref=fall, send_sem=fall_sem.at[0], recv_sem=fall_sem.at[1],
        device_id={"gz": near("gz", -1)}, device_id_type=MESH,
    )
    dropped.start()
    for t in range(0, L):
        for m, value in enumerate(landed(t)):
            mom[m, t] = value

    next_substep(5, round5, t3, pg, state_f, aa, passing(6, pf))
    round6 = narrow_send(6, pf)
    dropped.wait_recv()
    for m in range(3):
        for n in range(8):
            mom[m, 8 + n] = mom[m, 8 + n] + fall[m, n] * khi

    def last(g, kk, k, state, p, u, v, um, vm, w):
        wf[1 + k] = w
        out[1, k], out[2, k], out[3, k], out[4, k] = p, u, v, w

    next_substep(6, round6, t3, pf, state_f, aa, last)

    dropped.wait_send()
    for made in (first, second, round0, round1, round2, round7, round3, round4, round5, round6):
        for c in made:
            c.wait_send()


def solution(mesh):
    sizes = (mesh.shape["gx"], mesh.shape["gy"], mesh.shape["gz"])
    nx, ny, nz = sizes
    vm = lambda *shape: pltpu.VMEM(shape + (8, 128), F32)
    dma = pltpu.SemaphoreType.DMA
    scratch = [
        vm(5, L), pltpu.VMEM((128, 128), jnp.int32), pltpu.VMEM((8, 8, 16), jnp.int32),
        pltpu.VMEM((8 * PITCH, 128), F32), pltpu.VMEM((8 * PITCH, 128), F32), pltpu.VMEM((8 * PITCH, 128), jnp.int32),
        pltpu.VMEM((8, 8, 128), jnp.int32), pltpu.VMEM((128 * 24, 128), F32), vm(3, DEPTHS, L), vm(3, 8), vm(3, 8),
        vm(22), vm(22), vm(17), vm(22), vm(22), vm(2),
        vm(16), vm(16), vm(16), vm(16), vm(16), vm(17), vm(16), vm(16), vm(16), vm(16),
        vm(16), vm(17), vm(18), vm(18), vm(16), vm(16), vm(16), vm(16), vm(17), vm(16), vm(16), vm(16), vm(16), vm(17),
        vm(2, 2), vm(2, 12),
        vm(8, 2, 2), vm(8, 2, 2), vm(2, Y_ALL), vm(2, Y_ALL), vm(2, Z_ALL), vm(2, Z_ALL),
        pltpu.VMEM((1, 128), F32), pltpu.VMEM((nx * nz - 1, 1, 128), F32),
        pltpu.VMEM((1, 128), F32), pltpu.VMEM((ny - 1, 1, 128), F32),
        dma((8, 6)), dma((8, 6)), dma((nx * nz - 1,)), dma((nx * nz - 1,)), dma((ny - 1,)), dma((ny - 1,)),
        dma((2,)), dma((3, 8)), dma((3,)),
    ]
    vmem = pl.BlockSpec(memory_space=pltpu.VMEM)
    hbm = pl.BlockSpec(memory_space=pl.ANY)

    def per_device(fields, radius, weight, column, counts, fall_depth):
        held = pl.pallas_call(
            functools.partial(kernel, sizes),
            out_shape=(pltpu.VMEM((5, L, 8, 128), F32), pltpu.VMEM((3, L, 8, 128), F32)),
            in_specs=[hbm] * 6,
            out_specs=(vmem, vmem),
            scratch_shapes=scratch,
            compiler_params=pltpu.CompilerParams(collective_id=0, has_side_effects=True),
            name="slab_step",
        )(
            fields,
            counts.reshape(128, 128),
            jnp.transpose(fall_depth[:, :, :, 0], (0, 2, 1)),
            radius.reshape(1024, 128),
            weight.reshape(1024, 128),
            column.reshape(1024, 128),
        )
        return held

    cut = P(None, "gz", "gy", "gx")
    return jax.shard_map(
        per_device,
        mesh=mesh,
        in_specs=(cut, cut, cut, cut, P("gz", "gy", "gx"), cut),
        out_specs=(cut, cut),
        check_vma=False,
    )
```

```python
import functools

import jax
import jax.numpy as jnp
from jax import lax
from jax.experimental import pallas as pl
from jax.experimental.pallas import tpu as pltpu
from jax.sharding import PartitionSpec as P

MESH = pl.DeviceIdType.MESH
F32 = jnp.float32
L = 16
DEPTHS = 9
PITCH = 136
Y_TILES = {0: (14, 12), 1: (18, 18), 7: (6, 6), 3: (6, 6), 2: (2, 2), 5: (2, 2), 4: (10, 10)}
Z_TILES = {0: (7, 6), 1: (9, 9), 7: (3, 3), 3: (3, 3), 2: (1, 1), 5: (1, 1), 4: (5, 5)}
Y_AT = {0: 0, 1: 14, 7: 32, 3: 38, 2: 44, 5: 46, 4: 48}
Z_AT = {0: 0, 1: 7, 7: 16, 3: 19, 2: 22, 5: 23, 4: 24}
Y_ALL, Z_ALL = 58, 29
SPLITS = (0, 56, 128)
ROWS = 4


def kernel(
    sizes,
    fields_h, counts_h, depth_h, rad_h, wgt_h, col_h,
    out, mom,
    fields, counts, depth_in, rad, wgt, col, dep, dmat, gmat, ext, fall,
    c0, p0, w0, cq, pq, peak,
    ta, aa, ba, uinc, vinc, winc, um0, vm0, uminc, vminc,
    tr, lift, pf, uf, vf, umf, vmf, wf, ug, vg, umg, vmg, wg,
    hx, hy, ep, eg, ek, en,
    sx, rx, sy, ry, sz, rz, syz, rxy, rxz, ryz, rcorner,
    m1s, m1r, m2s, m2r,
    send_sem, recv_sem, edge_send, edge_recv, m1_send, m1_recv, m2_send, m2_recv, fall_sem, load_sem, field_sem,
):
    nx, ny, nz = sizes
    ix, iy, iz = lax.axis_index("gx"), lax.axis_index("gy"), lax.axis_index("gz")

    def near(axis, step):
        i, n = {"gx": (ix, nx), "gy": (iy, ny), "gz": (iz, nz)}[axis]
        return lax.rem(i + (step + n), n)

    def device(a=0, b=0, c=0):
        return {"gx": near("gx", a), "gy": near("gy", b), "gz": near("gz", c)}

    flip = 1 - 2 * lax.rem(iy, 2)
    group1 = [(a, f, b) for a in range(nx) for f in range(2) for b in range(nz) if (a, f, b) != (0, 0, 0)]
    group2 = [2 * n for n in range(1, ny // 2)]
    both = (0, 1)
    edges = [(a, b, None) for a in both for b in both]
    edges += [(a, None, c) for a in both for c in both]
    edges += [(None, b, c) for b in both for c in both]
    edges += [(a, b, c) for a in both for b in both for c in both]

    def edge_device(edge):
        return device(*(0 if d is None else 1 - 2 * d for d in edge))

    partners = [device(a, f * flip, b) for a, f, b in group1] + [device(0, a) for a in group2]
    partners += [device(0, 1), device(0, -1)] + [edge_device(e) for e in edges if e[1] is not None]
    barrier = pltpu.get_barrier_semaphore()
    for partner in reversed(partners):
        pl.semaphore_signal(barrier, inc=1, device_id=partner, device_id_type=MESH)

    early = [
        pltpu.make_async_copy(src, dst, field_sem.at[n])
        for n, (src, dst) in enumerate(((fields_h, fields), (counts_h, counts), (depth_h, depth_in)))
    ]
    loads = []
    for a, (src, dst) in enumerate(((rad_h, rad), (wgt_h, wgt), (col_h, col))):
        for s in range(8):
            loads.append(
                pltpu.make_async_copy(
                    src.at[pl.ds(s * 128, 128)], dst.at[pl.ds(s * PITCH, 128)], load_sem.at[a, s]
                )
            )
    for c in early:
        c.start()

    lane = lax.broadcasted_iota(jnp.int32, (8, 128), 1)
    row = lax.broadcasted_iota(jnp.int32, (8, 128), 0)
    klo = (iz > 0).astype(F32)
    khi = (iz < nz - 1).astype(F32)
    zero = jnp.zeros((8, 128), F32)

    def roll_l(x, s):
        s = s % 128
        return pltpu.roll(x, s, 1) if s else x

    def roll_s(x, s):
        s = s % 8
        return pltpu.roll(x, s, 0) if s else x

    def xp(q, h, n):
        return roll_l(jnp.where(lane < n, h, q), -n)

    def xm(q, h, n):
        return roll_l(jnp.where(lane >= 128 - n, h, q), n)

    def yp(q, h, n):
        return roll_s(jnp.where(row < n, h, q), -n)

    def ym(q, h, n):
        return roll_s(jnp.where(row >= 8 - n, h, q), n)

    def put_l(message, value, at, width):
        return jnp.where((lane >= at) & (lane < at + width), value, message)

    def by_level(fn):
        def group(g, carry):
            state = {}
            for kk in range(8):
                fn(g, kk, g * 8 + kk, state)
            return carry

        lax.fori_loop(0, 2, group, 0)

    def copies(r):
        made = []
        for d, step in ((0, 1), (1, -1)):
            y, z = pl.ds(Y_AT[r], Y_TILES[r][d]), pl.ds(Z_AT[r], Z_TILES[r][d])
            for i, (src, dst, axis) in enumerate(
                ((sy.at[d, y], ry.at[d, y], "gy"), (sz.at[d, z], rz.at[d, z], "gz"), (sx.at[r, d], rx.at[r, d], "gx"))
            ):
                made.append(
                    pltpu.make_async_remote_copy(
                        src_ref=src, dst_ref=dst,
                        send_sem=send_sem.at[r, 2 * i + d], recv_sem=recv_sem.at[r, 2 * i + d],
                        device_id={axis: near(axis, step)}, device_id_type=MESH,
                    )
                )
        return made

    def send(r):
        made = copies(r)
        for c in made:
            c.start()
        return made

    def arrive(made):
        for c in made:
            c.wait_recv()

    def x_pack(state, r, g, kk, a=None, b=None, wind=None, third=None):
        base = 16 * kk
        lo, hi = state.get("xlo", zero), state.get("xhi", zero)
        for value, at in ((a, 0), (b, 3), (third, 8)):
            if value is not None:
                lo = put_l(lo, roll_l(value, base + at + 3), base + at, 3)
                hi = put_l(hi, roll_l(value, base + at), base + at, 3)
        if wind is not None:
            lo = put_l(lo, roll_l(wind, base + 7), base + 6, 1)
        state["xlo"], state["xhi"] = lo, hi
        if kk == 7:
            sx[r, 0, g] = lo
            sx[r, 1, g] = hi

    def y_pack3(state, name, start, g, kk, q):
        t, o = divmod(3 * kk, 8)
        for d, moved in ((0, roll_s(q, o - 5)), (1, roll_s(q, o))):
            key = (name, d)
            tiles = state.setdefault(key, [None, None, None])
            if tiles[t] is None:
                tiles[t] = moved
            else:
                tiles[t] = jnp.where(row >= o, moved, tiles[t])
            if o > 5:
                tiles[t + 1] = moved
            if o >= 5:
                sy[d, start + g * 3 + t] = tiles[t]

    def y_halo3(ref, start, g, kk):
        t, o = divmod(3 * kk, 8)
        got = []
        for d in range(2):
            value = ref[d, start + g * 3 + t]
            if o > 5:
                value = jnp.where(row >= o, value, ref[d, start + g * 3 + t + 1])
            got.append(roll_s(value, 5 - o if d == 0 else -o))
        return got

    def y_pack1(state, name, start, g, kk, last=None, first=None):
        for d, value, by in ((0, last, kk - 7), (1, first, kk)):
            if value is not None:
                key = (name, d)
                moved = roll_s(value, by)
                state[key] = moved if kk == 0 else jnp.where(row >= kk, moved, state[key])
                if kk == 7:
                    sy[d, start + g] = state[key]

    def y_pack2(state, name, start, g, kk, q):
        t, o = divmod(2 * kk, 8)
        for d, by in ((0, o - 6), (1, o)):
            key = (name, d)
            moved = roll_s(q, by)
            state[key] = moved if o == 0 else jnp.where(row >= o, moved, state[key])
            if o == 6:
                sy[d, start + g * 2 + t] = state[key]

    def y_halo2(ref, start, g, kk):
        t, o = divmod(2 * kk, 8)
        return [roll_s(ref[d, start + g * 2 + t], 6 - o if d == 0 else -o) for d in range(2)]

    def x_halos(mx, g, kk):
        lo, hi = mx[0, g], mx[1, g]
        base = 16 * kk
        return (roll_l(lo, 125 - base), roll_l(hi, -base)), (roll_l(lo, 122 - base), roll_l(hi, -base - 3)), roll_l(lo, 121 - base)

    def x_halo(ref, at, g, kk):
        base = 16 * kk + at
        return roll_l(ref[0, g], 125 - base), roll_l(ref[1, g], -base)

    def lid_at(g, kk):
        return jnp.where(g == 1, khi, F32(1.0)) if kk == 7 else None

    def masked(value, mask):
        return value if mask is None else value * mask

    early[0].wait()
    for c in loads:
        c.start()

    def prepare(g, kk, k, state):
        c, p, u, v = fields[0, k], fields[1, k], fields[2, k], fields[3, k]
        w = masked(fields[4, k], lid_at(g, kk))
        c0[3 + k] = c
        p0[3 + k] = p
        w0[1 + k] = w
        speed = jnp.abs(u) + jnp.abs(v) + jnp.abs(w)
        state["m"] = speed if kk == 0 else jnp.maximum(state["m"], speed)
        x_pack(state, 0, g, kk, c, p, u)
        y_pack3(state, "c", Y_AT[0], g, kk, c)
        y_pack3(state, "p", Y_AT[0] + 6, g, kk, p)
        y_pack1(state, "v", Y_AT[0] + 12, g, kk, last=v)
        if kk == 7:
            peak[g] = state["m"]

    by_level(prepare)
    for n in range(3):
        sz[0, Z_AT[0] + n] = fields[0, 13 + n]
        sz[0, Z_AT[0] + 3 + n] = fields[1, 13 + n]
        sz[1, Z_AT[0] + n] = fields[0, n]
        sz[1, Z_AT[0] + 3 + n] = fields[1, n]
    sz[0, Z_AT[0] + 6] = w0[16]
    m1s[...] = jnp.max(jnp.maximum(peak[0], peak[1]), axis=0, keepdims=True)

    target = lax.broadcasted_iota(jnp.int32, (128, 128), 0).astype(F32).astype(jnp.bfloat16)
    row16 = lax.rem(lax.broadcasted_iota(jnp.int32, (16, 128), 0), 8)

    def deposit_row(kj):
        r = rad[pl.ds(kj, 8, stride=PITCH), :]
        w = wgt[pl.ds(kj, 8, stride=PITCH), :]
        c = col[pl.ds(kj, 8, stride=PITCH), :].astype(F32)
        live = row < counts[pl.ds(kj, 1), :]
        number = jnp.where(live, w, 0.0)
        area = number * (r * r)
        mass = area * r
        lhs = []
        for q in (number, area, mass):
            top = q.astype(jnp.bfloat16).astype(F32)
            pair = jnp.concatenate([top, q - top], axis=0)
            lhs.append(
                jnp.concatenate(
                    [jnp.where(row16 == s, pair, 0.0).astype(jnp.bfloat16) for s in range(8)], axis=1
                )
            )
        lhs = jnp.concatenate(lhs, axis=0)
        hot = jnp.concatenate(
            [
                jnp.where(
                    jnp.broadcast_to(c[s : s + 1, :], (128, 128)).astype(jnp.bfloat16) == target,
                    jnp.bfloat16(1.0), jnp.bfloat16(0.0),
                ).astype(jnp.float8_e4m3fn)
                for s in range(8)
            ],
            axis=1,
        )
        got = lax.dot_general(lhs, hot, (((1,), (1,)), ((), ())), preferred_element_type=F32)
        for m in range(3):
            dmat[pl.ds(pl.multiple_of(kj * 24 + 8 * m, 8), 8), :] = got[16 * m : 16 * m + 8] + got[16 * m + 8 : 16 * m + 16]

    def droplets(part):
        def step(i, carry):
            for n in range(ROWS):
                deposit_row(i * ROWS + n)
            return carry

        lax.fori_loop(SPLITS[part] // ROWS, SPLITS[part + 1] // ROWS, step, 0)

    def by_depth():
        def level(k):
            deep = []
            for s in range(8):
                moved = pltpu.roll(dep[s], lax.rem(128 - k, 128), 1)
                deep.append(jnp.broadcast_to(moved[:, 0:1], (8, 128)))
            for m in range(3):
                got = [dmat[pl.ds(k * 192 + 8 * m + s, 8, stride=24), :] for s in range(8)]
                for d in range(DEPTHS):
                    total = jnp.where(deep[0] == d, got[0], 0.0)
                    for s in range(1, 8):
                        total = total + jnp.where(deep[s] == d, got[s], 0.0)
                    gmat[m, d, k] = total

        def step(i, carry):
            level(2 * i)
            level(2 * i + 1)
            return carry

        lax.fori_loop(0, L // 2, step, 0)

    pl.semaphore_wait(barrier, len(partners))

    first = []
    for o, (a, f, b) in enumerate(group1):
        first.append(
            pltpu.make_async_remote_copy(
                src_ref=m1s, dst_ref=m1r.at[o], send_sem=m1_send.at[o], recv_sem=m1_recv.at[o],
                device_id=device(a, f * flip, b), device_id_type=MESH,
            )
        )
    for c in first:
        c.start()
    round0 = send(0)
    for c in early[1:] + loads:
        c.wait()
    dep[...] = jnp.zeros_like(dep)
    dep[:, :, 0:16] = depth_in[...]
    droplets(0)

    def flux(a, q):
        central = 37.0 * (q[2] + q[3]) - 8.0 * (q[1] + q[4]) + (q[0] + q[5])
        upwind = 10.0 * (q[3] - q[2]) - 5.0 * (q[4] - q[1]) + (q[5] - q[0])
        return a * central - jnp.abs(a) * upwind

    def advect(q, k, xh, yh, winds):
        own = q[3 + k]
        u, um, v, vm, w, wm = winds
        line = [xm(own, xh[0], 3), xm(own, xh[0], 2), xm(own, xh[0], 1), own,
                xp(own, xh[1], 1), xp(own, xh[1], 2), xp(own, xh[1], 3)]
        total = flux(u, line[1:]) - flux(um, line[:-1])
        line = [ym(own, yh[0], 3), ym(own, yh[0], 2), ym(own, yh[0], 1), own,
                yp(own, yh[1], 1), yp(own, yh[1], 2), yp(own, yh[1], 3)]
        total = total + (flux(v, line[1:]) - flux(vm, line[:-1]))
        line = [q[k + n] for n in range(7)]
        total = total + (flux(w, line[1:]) - flux(wm, line[:-1]))
        return total * F32(-1.0 / 60.0)

    for c in first:
        c.wait_recv()
    top = m1s[...]
    for o in range(len(group1)):
        top = jnp.maximum(top, m1r[o])
    m2s[...] = top
    second = []
    for o, a in enumerate(group2):
        second.append(
            pltpu.make_async_remote_copy(
                src_ref=m2s, dst_ref=m2r.at[o], send_sem=m2_send.at[o], recv_sem=m2_recv.at[o],
                device_id=device(0, a), device_id_type=MESH,
            )
        )
    for c in second:
        c.start()

    arrive(round0)
    for n in range(3):
        for d, to, keep in ((0, n, klo), (1, 19 + n, khi)):
            c0[to] = rz[d, Z_AT[0] + n] * keep
            p0[to] = rz[d, Z_AT[0] + 3 + n] * keep
    w0[0] = rz[0, Z_AT[0] + 6] * klo
    winc[0] = -10.0 * (p0[3] - p0[2]) * klo
    lift[0] = 0.25 * (c0[2] + c0[3]) * klo

    def build(g, kk, k, state):
        lid = lid_at(g, kk)
        xc, xq, xu = x_halos(rx.at[0], g, kk)
        yc = y_halo3(ry, Y_AT[0], g, kk)
        yq = y_halo3(ry, Y_AT[0] + 6, g, kk)
        yv = roll_s(ry[0, Y_AT[0] + 12 + g], 7 - kk)
        p, u, v = p0[3 + k], fields[2, k], fields[3, k]
        w, wm = w0[1 + k], w0[k]
        um, vm = xm(u, xu, 1), ym(v, yv, 1)
        winds = (u, um, v, vm, w, wm)
        t = advect(c0, k, xc, yc, winds)
        q = advect(p0, k, xq, yq, winds)
        du = -10.0 * (xp(p, xq[1], 1) - p)
        dum = -10.0 * (p - xm(p, xq[0], 1))
        dv = -10.0 * (yp(p, yq[1], 1) - p)
        dvm = -10.0 * (p - ym(p, yq[0], 1))
        dw = masked(-10.0 * (p0[4 + k] - p), lid)
        dwm = winc[k]
        up = masked(0.25 * (c0[3 + k] + c0[4 + k]), lid)
        upm = lift[k]
        a = q - 10.0 * ((u - um) + (v - vm) + (w - wm))
        b = -10.0 * ((du - dum) + (dv - dvm) + ((dw + up) - (dwm + upm)))
        ta[k], aa[k], ba[k] = t, a, b
        uinc[k], vinc[k], winc[1 + k], lift[1 + k] = du, dv, dw, up
        um0[k], vm0[k], uminc[k], vminc[k] = um, vm, dum, dvm
        x_pack(state, 1, g, kk, t, a, None, b)
        for i, value in enumerate((t, a, b)):
            y_pack3(state, i, Y_AT[1] + 6 * i, g, kk, value)

    by_level(build)
    for i, a in enumerate((ta, aa, ba)):
        for n in range(3):
            sz[0, Z_AT[1] + 3 * i + n] = a[13 + n]
            sz[1, Z_AT[1] + 3 * i + n] = a[n]
    round1 = send(1)

    droplets(1)

    for c in second:
        c.wait_recv()
    top = m2s[...]
    for o in range(len(group2)):
        top = jnp.maximum(top, m2r[o])
    top = jnp.broadcast_to(jnp.max(top, axis=1, keepdims=True), (1, 128))
    time_step = jnp.broadcast_to(0.6 / (1.0 + top), (8, 128))

    arrive(round1)
    t1 = time_step * F32(1.0 / 3.0)
    slot = lax.rem(lane, 16)
    for d in range(2):
        for g in range(2):
            third = jnp.where((slot >= 3) & (slot < 6), roll_l(rx[1, d, g], -5), 0.0)
            hx[d, g] = rx[0, d, g] + t1 * (rx[1, d, g] + t1 * third)
        for n in range(6):
            hy[d, n] = ry[d, n] + t1 * ry[d, 14 + n]
            hy[d, 6 + n] = ry[d, 6 + n] + t1 * (ry[d, 20 + n] + t1 * ry[d, 26 + n])

    def section1(g, kk, k, state):
        cq[3 + k] = c0[3 + k] + t1 * ta[k]
        pq[3 + k] = p0[3 + k] + t1 * (aa[k] + t1 * ba[k])
        uf[k] = fields[2, k] + t1 * uinc[k]
        vf[k] = fields[3, k] + t1 * vinc[k]
        umf[k] = um0[k] + t1 * uminc[k]
        vmf[k] = vm0[k] + t1 * vminc[k]
        wf[1 + k] = w0[1 + k] + t1 * (winc[1 + k] + lift[1 + k])

    by_level(section1)
    wf[0] = w0[0] + t1 * (winc[0] + lift[0])
    for n in range(3):
        for d, to, keep in ((0, n, klo), (1, 19 + n, khi)):
            cq[to] = c0[to] + (t1 * keep) * rz[d, Z_AT[1] + n]
            pq[to] = p0[to] + (t1 * keep) * (rz[d, Z_AT[1] + 3 + n] + t1 * rz[d, Z_AT[1] + 6 + n])

    def tracer_rates(mx, my, start, old, finish):
        u, v, um, vm, w = old

        def step(g, kk, k, state):
            winds = (u[k], um[k], v[k], vm[k], w[1 + k], w[k])
            finish(g, kk, k, state, advect(cq, k, x_halo(mx, 0, g, kk), y_halo3(my, start, g, kk), winds))

        by_level(step)

    def lifts():
        lift[0] = 0.25 * (cq[2] + cq[3]) * klo

        def step(g, kk, k, state):
            lift[1 + k] = masked(0.25 * (cq[3 + k] + cq[4 + k]), lid_at(g, kk))

        by_level(step)

    def narrow(r, g, kk, k, state, p):
        x_pack(state, r, g, kk, None, p)
        y_pack1(state, "p", Y_AT[r], g, kk, last=p, first=p)

    def narrow_send(r, p):
        sz[0, Z_AT[r]] = p[16]
        sz[1, Z_AT[r]] = p[1]
        return send(r)

    def first_substep(r, s, mx, my, start, old, new, rate_ref):
        u_, v_, um_, vm_, w_ = old
        un_, vn_, umn_, vmn_, wn_ = new
        wn_[0] = w0[0] + s * (winc[0] + lift[0])

        def step(g, kk, k, state):
            winds = (u_[k], um_[k], v_[k], vm_[k], w_[1 + k], w_[k])
            rate = advect(pq, k, x_halo(mx, 3, g, kk), y_halo3(my, start, g, kk), winds)
            rate_ref[k] = rate
            u = fields[2, k] + s * uinc[k]
            um = um0[k] + s * uminc[k]
            v = fields[3, k] + s * vinc[k]
            vm = vm0[k] + s * vminc[k]
            w = w0[1 + k] + s * (winc[1 + k] + lift[1 + k])
            wm = w0[k] + s * (winc[k] + lift[k])
            p = p0[3 + k] + s * (rate - 10.0 * ((u - um) + (v - vm) + (w - wm)))
            pf[1 + k], un_[k], vn_[k], umn_[k], vmn_[k], wn_[1 + k] = p, u, v, um, vm, w
            narrow(r, g, kk, k, state, p)

        by_level(step)
        return narrow_send(r, pf)

    def next_substep(r, made, s, ps, winds, rate_ref, finish):
        u_, v_, um_, vm_, w_ = winds
        s10 = s * 10.0
        arrive(made)
        ps[0] = rz[0, Z_AT[r]] * klo
        ps[17] = rz[1, Z_AT[r]] * khi
        w_[0] = w_[0] + s * lift[0] - (s10 * klo) * (ps[1] - ps[0])

        def step(g, kk, k, state):
            lid = lid_at(g, kk)
            xq = x_halo(rx.at[r], 3, g, kk)
            p = ps[1 + k]
            ylo, yhi = roll_s(ry[0, Y_AT[r] + g], 7 - kk), roll_s(ry[1, Y_AT[r] + g], -kk)
            u = u_[k] - s10 * (xp(p, xq[1], 1) - p)
            um = um_[k] - s10 * (p - xm(p, xq[0], 1))
            v = v_[k] - s10 * (yp(p, yhi, 1) - p)
            vm = vm_[k] - s10 * (p - ym(p, ylo, 1))
            w = w_[1 + k] + s * lift[1 + k] - masked(s10 * (ps[2 + k] - p), lid)
            wm = state["w"] if kk else w_[k]
            state["w"] = w
            pn = p + s * (rate_ref[k] - 10.0 * ((u - um) + (v - vm) + (w - wm)))
            finish(g, kk, k, state, pn, u, v, um, vm, w)

        by_level(step)

    state_f = (uf, vf, umf, vmf, wf)
    state_g = (ug, vg, umg, vmg, wg)

    t2 = time_step * F32(0.25)
    half = time_step * F32(0.5)
    lifts()
    round2 = first_substep(2, t2, hx, hy, 6, state_f, state_g, aa)

    def tracer2(g, kk, k, state, rate):
        c = c0[3 + k] + half * rate
        tr[k] = c
        x_pack(state, 7, g, kk, c)
        y_pack3(state, "c", Y_AT[7], g, kk, c)

    tracer_rates(hx, hy, 0, state_f, tracer2)
    for n in range(3):
        sz[0, Z_AT[7] + n] = tr[13 + n]
        sz[1, Z_AT[7] + n] = tr[n]
    round7 = send(7)
    by_depth()

    def finish2(g, kk, k, state, p, u, v, um, vm, w):
        pq[3 + k] = p
        ug[k], vg[k], umg[k], vmg[k], wg[1 + k] = u, v, um, vm, w
        cq[3 + k] = tr[k]
        x_pack(state, 3, g, kk, None, p)
        y_pack3(state, "p", Y_AT[3], g, kk, p)

    next_substep(2, round2, t2, pf, state_g, aa, finish2)
    for n in range(3):
        sz[0, Z_AT[3] + n] = pq[16 + n]
        sz[1, Z_AT[3] + n] = pq[3 + n]
    round3 = send(3)

    arrive(round7)
    for n in range(3):
        for d, to, keep in ((0, n, klo), (1, 19 + n, khi)):
            cq[to] = rz[d, Z_AT[7] + n] * keep
    t3 = time_step * F32(0.25)
    s10 = t3 * 10.0
    alpha = s10 * s10
    lifts()

    def forcing(g, kk, k, state):
        value = (lift[1 + k] - lift[k]) * (-0.1 * alpha)
        ek[0, 3 + k] = value
        narrow(5, g, kk, k, state, value)

    by_level(forcing)
    sz[0, Z_AT[5]] = ek[0, 18]
    sz[1, Z_AT[5]] = ek[0, 3]
    round5 = send(5)

    def tracer3(g, kk, k, state, rate):
        c = c0[3 + k] + time_step * rate
        out[0, k] = c
        growth = jnp.minimum(jnp.exp(0.3 * c), F32(3.0e38))
        ta[k] = growth
        ba[k] = jnp.sqrt(growth)

    tracer_rates(rx.at[7], ry, Y_AT[7], state_g, tracer3)

    def landed(t):
        totals = [None, None, None]
        for k in range(max(t, 0), min(t + DEPTHS, L)):
            d = k - t
            grow, root = ta[k], ba[k]
            parts = (gmat[0, d, k], gmat[1, d, k] * grow, gmat[2, d, k] * grow * root)
            totals = [a if b is None else b + a for a, b in zip(parts, totals)]
        return totals

    for t in range(-8, 0):
        for m, value in enumerate(landed(t)):
            ext[m, t + 8] = value

    arrive(round3)
    for n in range(3):
        for d, to, keep in ((0, n, klo), (1, 19 + n, khi)):
            pq[to] = rz[d, Z_AT[3] + n] * keep

    wf[0] = w0[0] + t3 * (winc[0] + lift[0])

    def open3(g, kk, k, state):
        winds = (ug[k], umg[k], vg[k], vmg[k], wg[1 + k], wg[k])
        rate = advect(pq, k, x_halo(rx.at[3], 3, g, kk), y_halo3(ry, Y_AT[3], g, kk), winds)
        u = fields[2, k] + t3 * uinc[k]
        um = um0[k] + t3 * uminc[k]
        v = fields[3, k] + t3 * vinc[k]
        vm = vm0[k] + t3 * vminc[k]
        w = w0[1 + k] + t3 * (winc[1 + k] + lift[1 + k])
        wm = w0[k] + t3 * (winc[k] + lift[k])
        e = t3 * (rate - 10.0 * ((u - um) + (v - vm) + (w - wm)))
        p = p0[3 + k] + e
        e = e + ek[0, 3 + k]
        ep[0, 3 + k], eg[0, 3 + k] = p, e
        uf[k], vf[k], wf[1 + k] = u, v, w
        x_pack(state, 4, g, kk, p, e)
        y_pack3(state, "p", Y_AT[4], g, kk, p)
        y_pack2(state, "e", Y_AT[4] + 6, g, kk, e)

    by_level(open3)
    for n in range(3):
        sz[0, Z_AT[4] + n] = ep[0, 16 + n]
        sz[1, Z_AT[4] + n] = ep[0, 3 + n]
    for n in range(2):
        sz[0, Z_AT[4] + 3 + n] = eg[0, 17 + n]
        sz[1, Z_AT[4] + 3 + n] = eg[0, 3 + n]
    for d in range(2):
        syz[d, 0, 0] = sy[d, Y_AT[4] + 5]
        syz[d, 0, 1] = sy[d, Y_AT[4] + 9]
        syz[d, 1, 0] = sy[d, Y_AT[4]]
        syz[d, 1, 1] = sy[d, Y_AT[4] + 6]
    round4 = send(4)
    for i, (a, b, c) in enumerate(edges):
        if c is None:
            src, dst = sx.at[4, a], rxy.at[a, b]
        elif b is None:
            src, dst = sx.at[4, a, 1 - c], rxz.at[a, c]
        elif a is None:
            src, dst = syz.at[b, c], ryz.at[b, c]
        else:
            src, dst = sx.at[4, a, 1 - c], rcorner.at[a, b, c]
        round4.append(
            pltpu.make_async_remote_copy(
                src_ref=src, dst_ref=dst, send_sem=edge_send.at[i], recv_sem=edge_recv.at[i],
                device_id=edge_device((a, b, c)), device_id_type=MESH,
            )
        )
        round4[-1].start()
    dropped = pltpu.make_async_remote_copy(
        src_ref=ext, dst_ref=fall, send_sem=fall_sem.at[0], recv_sem=fall_sem.at[1],
        device_id={"gz": near("gz", -1)}, device_id_type=MESH,
    )
    dropped.start()
    for t in range(0, L):
        for m, value in enumerate(landed(t)):
            mom[m, t] = value

    def join_l(lo, hi):
        return jnp.where(lane < 64, hi, lo)

    def join_s(lo, hi):
        return jnp.where(row < 4, hi, lo)

    def x_one(tile, d, at, kk):
        return roll_l(tile, 125 - at - 16 * kk if d == 0 else -at - 16 * kk)

    arrive(round5)
    arrive(round4)

    def assemble(g, kk, k, state):
        at = 3 + k
        ep[1, at] = join_s(*y_halo3(ry, Y_AT[4], g, kk))
        eg[1, at] = join_s(*y_halo2(ry, Y_AT[4] + 6, g, kk))
        ek[1, at] = join_s(roll_s(ry[0, Y_AT[5] + g], 7 - kk), roll_s(ry[1, Y_AT[5] + g], -kk))
        for off, ref in ((0, ep), (3, eg)):
            ref[2, at] = join_l(*(x_one(rx[4, d, g], d, off, kk) for d in both))
            ref[3, at] = join_s(*(join_l(*(x_one(rxy[d, b, g], d, off, kk) for d in both)) for b in both))
        ek[2, at] = join_l(*x_halo(rx.at[5], 3, g, kk))

    by_level(assemble)
    for n in range(3):
        ep[0, n] = rz[0, Z_AT[4] + n]
        ep[0, 19 + n] = rz[1, Z_AT[4] + n]
    for n in range(2):
        eg[0, 1 + n] = rz[0, Z_AT[4] + 3 + n]
        eg[0, 19 + n] = rz[1, Z_AT[4] + 3 + n]
    ek[0, 2] = rz[0, Z_AT[5]]
    ek[0, 19] = rz[1, Z_AT[5]]
    for c, levels in ((0, ((1, 6), (2, 7))), (1, ((19, 0), (20, 1)))):
        for to, kk in levels:
            t, o = divmod(3 * kk, 8)
            ep[1, to] = join_s(roll_s(ryz[0, c, 0], 5 - o), roll_s(ryz[1, c, 0], -o))
            ep[2, to] = join_l(*(x_one(rxz[d, c], d, 0, kk) for d in both))
            if to in (2, 19):
                o = (2 * kk) % 8
                eg[1, to] = join_s(roll_s(ryz[0, c, 1], 6 - o), roll_s(ryz[1, c, 1], -o))
                eg[2, to] = join_l(*(x_one(rxz[d, c], d, 3, kk) for d in both))
                ep[3, to] = join_s(*(join_l(*(x_one(rcorner[d, b, c], d, 0, kk) for d in both)) for b in both))

    other_x, other_y = (2, 3, 0, 1), (1, 0, 3, 2)

    def neighbours(ref, part, at):
        q, hx_, hy_ = ref[part, at], ref[other_x[part], at], ref[other_y[part], at]
        return q, xp(q, hx_, 1), xm(q, hx_, 1), yp(q, hy_, 1), ym(q, hy_, 1)

    def laplacian(ref, part, at, low=None, high=None):
        q, a, b, c, d = neighbours(ref, part, at)
        up, down = masked(ref[part, at + 1] - q, high), masked(q - ref[part, at - 1], low)
        return q, (a - q, c - q, up), ((a - q) - (q - b)) + ((c - q) - (q - d)) + (up - down)

    def edge_masks(at, g, kk):
        low = jnp.where(g == 0, klo, F32(1.0)) if kk == 0 else None
        return low, lid_at(g, kk)

    def winds3(k, steps):
        uf[k] = uf[k] - s10 * steps[0]
        vf[k] = vf[k] - s10 * steps[1]
        wf[1 + k] = wf[1 + k] + t3 * lift[1 + k] - s10 * steps[2]

    def second3(part, at, low=None, high=None):
        q, steps, lap = laplacian(ep, part, at, low, high)
        e = eg[part, at] + alpha * lap
        eg[part, at] = e
        en[part, at] = q + e
        return steps

    def two(g, kk, k, state):
        low, high = edge_masks(3 + k, g, kk)
        winds3(k, second3(0, 3 + k, low, high))
        for part in (1, 2, 3):
            second3(part, 3 + k, low, high)

    by_level(two)
    second3(0, 1)
    second3(0, 20)
    for part in (0, 1, 2):
        second3(part, 2, None, klo)
        second3(part, 19, khi, None)

    def third3(part, at, low=None, high=None):
        q, steps, lap = laplacian(en, part, at, low, high)
        e = eg[part, at] + ek[part, at] + alpha * lap
        eg[part, at] = e
        ep[part, at] = q + e
        return steps

    def three(g, kk, k, state):
        low, high = edge_masks(3 + k, g, kk)
        winds3(k, third3(0, 3 + k, low, high))
        for part in (1, 2):
            third3(part, 3 + k, low, high)

    by_level(three)
    third3(0, 2, None, klo)
    third3(0, 19, khi, None)

    def four(g, kk, k, state):
        low, high = edge_masks(3 + k, g, kk)
        q, steps, lap = laplacian(ep, 0, 3 + k, low, high)
        out[1, k] = q + (eg[0, 3 + k] + ek[0, 3 + k] + alpha * lap)
        out[2, k] = uf[k] - s10 * steps[0]
        out[3, k] = vf[k] - s10 * steps[1]
        out[4, k] = wf[1 + k] + t3 * lift[1 + k] - s10 * steps[2]

    by_level(four)

    dropped.wait_recv()
    for m in range(3):
        for n in range(8):
            mom[m, 8 + n] = mom[m, 8 + n] + fall[m, n] * khi
    dropped.wait_send()
    for made in (first, second, round0, round1, round2, round7, round3, round4, round5):
        for c in made:
            c.wait_send()


def solution(mesh):
    sizes = (mesh.shape["gx"], mesh.shape["gy"], mesh.shape["gz"])
    nx, ny, nz = sizes
    vm = lambda *shape: pltpu.VMEM(shape + (8, 128), F32)
    dma = pltpu.SemaphoreType.DMA
    scratch = [
        vm(5, L), pltpu.VMEM((128, 128), jnp.int32), pltpu.VMEM((8, 8, 16), jnp.int32),
        pltpu.VMEM((8 * PITCH, 128), F32), pltpu.VMEM((8 * PITCH, 128), F32), pltpu.VMEM((8 * PITCH, 128), jnp.int32),
        pltpu.VMEM((8, 8, 128), jnp.int32), pltpu.VMEM((128 * 24, 128), F32), vm(3, DEPTHS, L), vm(3, 8), vm(3, 8),
        vm(22), vm(22), vm(17), vm(22), vm(22), vm(2),
        vm(16), vm(16), vm(16), vm(16), vm(16), vm(17), vm(16), vm(16), vm(16), vm(16),
        vm(16), vm(17), vm(18), vm(16), vm(16), vm(16), vm(16), vm(17), vm(16), vm(16), vm(16), vm(16), vm(17),
        vm(2, 2), vm(2, 12), vm(4, 22), vm(4, 22), vm(4, 22), vm(4, 22),
        vm(8, 2, 2), vm(8, 2, 2), vm(2, Y_ALL), vm(2, Y_ALL), vm(2, Z_ALL), vm(2, Z_ALL),
        vm(2, 2, 2), vm(2, 2, 2), vm(2, 2), vm(2, 2, 2), vm(2, 2, 2),
        pltpu.VMEM((1, 128), F32), pltpu.VMEM((2 * nx * nz - 1, 1, 128), F32),
        pltpu.VMEM((1, 128), F32), pltpu.VMEM((ny // 2 - 1, 1, 128), F32),
        dma((8, 6)), dma((8, 6)), dma((20,)), dma((20,)),
        dma((2 * nx * nz - 1,)), dma((2 * nx * nz - 1,)), dma((ny // 2 - 1,)), dma((ny // 2 - 1,)),
        dma((2,)), dma((3, 8)), dma((3,)),
    ]
    vmem = pl.BlockSpec(memory_space=pltpu.VMEM)
    hbm = pl.BlockSpec(memory_space=pl.ANY)

    def per_device(fields, radius, weight, column, counts, fall_depth):
        held = pl.pallas_call(
            functools.partial(kernel, sizes),
            out_shape=(pltpu.VMEM((5, L, 8, 128), F32), pltpu.VMEM((3, L, 8, 128), F32)),
            in_specs=[hbm] * 6,
            out_specs=(vmem, vmem),
            scratch_shapes=scratch,
            compiler_params=pltpu.CompilerParams(collective_id=0, has_side_effects=True),
            name="slab_step",
        )(
            fields,
            counts.reshape(128, 128),
            jnp.transpose(fall_depth[:, :, :, 0], (0, 2, 1)),
            radius.reshape(1024, 128),
            weight.reshape(1024, 128),
            column.reshape(1024, 128),
        )
        return held

    cut = P(None, "gz", "gy", "gx")
    return jax.shard_map(
        per_device,
        mesh=mesh,
        in_specs=(cut, cut, cut, cut, P("gz", "gy", "gx"), cut),
        out_specs=(cut, cut),
        check_vma=False,
    )
```

```python
import functools

import jax
import jax.numpy as jnp
from jax import lax
from jax.experimental import pallas as pl
from jax.experimental.pallas import tpu as pltpu
from jax.sharding import PartitionSpec as P

MESH = pl.DeviceIdType.MESH
F32 = jnp.float32
L = 16
DEPTHS = 9
PITCH = 136
Y_TILES = {0: (14, 12), 1: (12, 12), 6: (6, 6), 7: (6, 6), 3: (6, 6), 2: (2, 2), 5: (2, 2), 4: (10, 10)}
Z_TILES = {0: (7, 6), 1: (9, 9), 7: (3, 3), 3: (3, 3), 2: (1, 1), 5: (1, 1), 4: (5, 5)}
Y_AT = {0: 0, 1: 14, 6: 26, 7: 32, 3: 38, 2: 44, 5: 46, 4: 48}
Z_AT = {0: 0, 1: 7, 7: 16, 3: 19, 2: 22, 5: 23, 4: 24}
Y_ALL, Z_ALL = 58, 29
SPLITS = (0, 56, 128)
ROWS = 4


def kernel(
    sizes,
    fields_h, counts_h, depth_h, rad_h, wgt_h, col_h,
    out, mom,
    fields, counts, depth_in, rad, wgt, col, dep, dmat, gmat, ext, fall,
    c0, p0, w0, cq, pq, peak,
    ta, aa, ba, uinc, vinc, winc, um0, vm0, uminc, vminc,
    tr, lift, pf, uf, vf, umf, vmf, wf, ug, vg, umg, vmg, wg,
    hx, hy, ep, eg, ek, en,
    sx, rx, sy, ry, sz, rz, syz, sxy, scorner, rxy, rxz, ryz, rcorner, xy,
    m1s, m1r, m2s, m2r,
    send_sem, recv_sem, small_sem, fall_sem, load_sem, field_sem,
):
    nx, ny, nz = sizes
    ix, iy, iz = lax.axis_index("gx"), lax.axis_index("gy"), lax.axis_index("gz")

    def near(axis, step):
        i, n = {"gx": (ix, nx), "gy": (iy, ny), "gz": (iz, nz)}[axis]
        return lax.rem(i + (step + n), n)

    early = [
        pltpu.make_async_copy(src, dst, field_sem.at[n])
        for n, (src, dst) in enumerate(((fields_h, fields), (counts_h, counts), (depth_h, depth_in)))
    ]
    loads = []
    for a, (src, dst) in enumerate(((rad_h, rad), (wgt_h, wgt), (col_h, col))):
        for s in range(8):
            loads.append(
                pltpu.make_async_copy(
                    src.at[pl.ds(s * 128, 128)], dst.at[pl.ds(s * PITCH, 128)], load_sem.at[a]
                )
            )
    for c in early:
        c.start()

    def device(a=0, b=0, c=0):
        return {"gx": near("gx", a), "gy": near("gy", b), "gz": near("gz", c)}

    flip = 1 - 2 * lax.rem(iy, 2)
    group1 = [(a, f, b) for a in range(nx) for f in range(2) for b in range(nz) if (a, f, b) != (0, 0, 0)]
    group2 = [2 * n for n in range(1, ny // 2)]
    both = (0, 1)
    edges = [(a, b, None) for a in both for b in both]
    edges += [(a, None, c) for a in both for c in both]
    edges += [(None, b, c) for b in both for c in both]
    edges += [(a, b, c) for a in both for b in both for c in both]

    def edge_device(edge):
        return device(*(0 if d is None else 1 - 2 * d for d in edge))

    partners = [device(a, f * flip, b) for a, f, b in group1] + [device(0, a) for a in group2]
    partners += [device(0, 1), device(0, -1)] + [edge_device(e) for e in edges if e[1] is not None]
    barrier = pltpu.get_barrier_semaphore()
    for partner in reversed(partners):
        pl.semaphore_signal(barrier, inc=1, device_id=partner, device_id_type=MESH)

    lane = lax.broadcasted_iota(jnp.int32, (8, 128), 1)
    row = lax.broadcasted_iota(jnp.int32, (8, 128), 0)
    klo = (iz > 0).astype(F32)
    khi = (iz < nz - 1).astype(F32)
    zero = jnp.zeros((8, 128), F32)

    def roll_l(x, s):
        s = s % 128
        return pltpu.roll(x, s, 1) if s else x

    def roll_s(x, s):
        s = s % 8
        return pltpu.roll(x, s, 0) if s else x

    def xp(q, h, n):
        return roll_l(jnp.where(lane < n, h, q), -n)

    def xm(q, h, n):
        return roll_l(jnp.where(lane >= 128 - n, h, q), n)

    def yp(q, h, n):
        return roll_s(jnp.where(row < n, h, q), -n)

    def ym(q, h, n):
        return roll_s(jnp.where(row >= 8 - n, h, q), n)

    def put_l(message, value, at, width):
        return jnp.where((lane >= at) & (lane < at + width), value, message)

    def by_level(fn):
        def group(g, carry):
            state = {}
            for kk in range(8):
                fn(g, kk, g * 8 + kk, state)
            return carry

        lax.fori_loop(0, 2, group, 0)

    def copies(r):
        made = []
        for d, step in ((0, 1), (1, -1)):
            y = pl.ds(Y_AT[r], Y_TILES[r][d])
            parts = [(sy.at[d, y], ry.at[d, y], "gy")]
            if r in Z_TILES:
                z = pl.ds(Z_AT[r], Z_TILES[r][d])
                parts += [(sz.at[d, z], rz.at[d, z], "gz"), (sx.at[r, d], rx.at[r, d], "gx")]
            for i, (src, dst, axis) in enumerate(parts):
                made.append(
                    pltpu.make_async_remote_copy(
                        src_ref=src, dst_ref=dst,
                        send_sem=send_sem.at[0], recv_sem=recv_sem.at[r],
                        device_id={axis: near(axis, step)}, device_id_type=MESH,
                    )
                )
        return made

    def send(r):
        for c in copies(r):
            c.start()
        n = sum(Y_TILES[r]) + (sum(Z_TILES[r]) + 4 if r in Z_TILES else 0) + (12 if r == 4 else 0)
        sent.append(n)
        return r, n

    sent = []

    def tiles(n, send, recv):
        span = dmat.at[pl.ds(0, 8 * n)]
        return pltpu.make_async_remote_copy(
            src_ref=span, dst_ref=span, send_sem=send, recv_sem=recv, device_id=device(1), device_id_type=MESH
        )

    def arrive(made):
        r, n = made
        tiles(n, send_sem.at[0], recv_sem.at[r]).wait_recv()

    def x_pack(state, r, g, kk, a=None, b=None, wind=None, third=None):
        base = 16 * kk
        lo, hi = state.get("xlo", zero), state.get("xhi", zero)
        for value, at in ((a, 0), (b, 3), (third, 8)):
            if value is not None:
                lo = put_l(lo, roll_l(value, base + at + 3), base + at, 3)
                hi = put_l(hi, roll_l(value, base + at), base + at, 3)
        if wind is not None:
            lo = put_l(lo, roll_l(wind, base + 7), base + 6, 1)
        state["xlo"], state["xhi"] = lo, hi
        if kk == 7:
            sx[r, 0, g] = lo
            sx[r, 1, g] = hi

    def y_pack3(state, name, start, g, kk, q):
        t, o = divmod(3 * kk, 8)
        for d, moved in ((0, roll_s(q, o - 5)), (1, roll_s(q, o))):
            key = (name, d)
            tiles = state.setdefault(key, [None, None, None])
            if tiles[t] is None:
                tiles[t] = moved
            else:
                tiles[t] = jnp.where(row >= o, moved, tiles[t])
            if o > 5:
                tiles[t + 1] = moved
            if o >= 5:
                sy[d, start + g * 3 + t] = tiles[t]

    def y_halo3(ref, start, g, kk):
        t, o = divmod(3 * kk, 8)
        got = []
        for d in range(2):
            value = ref[d, start + g * 3 + t]
            if o > 5:
                value = jnp.where(row >= o, value, ref[d, start + g * 3 + t + 1])
            got.append(roll_s(value, 5 - o if d == 0 else -o))
        return got

    def y_pack1(state, name, start, g, kk, last=None, first=None):
        for d, value, by in ((0, last, kk - 7), (1, first, kk)):
            if value is not None:
                key = (name, d)
                moved = roll_s(value, by)
                state[key] = moved if kk == 0 else jnp.where(row >= kk, moved, state[key])
                if kk == 7:
                    sy[d, start + g] = state[key]

    def y_pack2(state, name, start, g, kk, q):
        t, o = divmod(2 * kk, 8)
        for d, by in ((0, o - 6), (1, o)):
            key = (name, d)
            moved = roll_s(q, by)
            state[key] = moved if o == 0 else jnp.where(row >= o, moved, state[key])
            if o == 6:
                sy[d, start + g * 2 + t] = state[key]

    def y_halo2(ref, start, g, kk):
        t, o = divmod(2 * kk, 8)
        return [roll_s(ref[d, start + g * 2 + t], 6 - o if d == 0 else -o) for d in range(2)]

    def x_halos(mx, g, kk):
        lo, hi = mx[0, g], mx[1, g]
        base = 16 * kk
        return (roll_l(lo, 125 - base), roll_l(hi, -base)), (roll_l(lo, 122 - base), roll_l(hi, -base - 3)), roll_l(lo, 121 - base)

    def x_halo(ref, at, g, kk):
        base = 16 * kk + at
        return roll_l(ref[0, g], 125 - base), roll_l(ref[1, g], -base)

    def lid_at(g, kk):
        return jnp.where(g == 1, khi, F32(1.0)) if kk == 7 else None

    def masked(value, mask):
        return value if mask is None else value * mask

    early[0].wait()
    for c in loads:
        c.start()

    def prepare(g, kk, k, state):
        c, p, u, v = fields[0, k], fields[1, k], fields[2, k], fields[3, k]
        w = masked(fields[4, k], lid_at(g, kk))
        c0[3 + k] = c
        p0[3 + k] = p
        w0[1 + k] = w
        speed = jnp.abs(u) + jnp.abs(v) + jnp.abs(w)
        state["m"] = speed if kk == 0 else jnp.maximum(state["m"], speed)
        x_pack(state, 0, g, kk, c, p, u)
        y_pack3(state, "c", Y_AT[0], g, kk, c)
        y_pack3(state, "p", Y_AT[0] + 6, g, kk, p)
        y_pack1(state, "v", Y_AT[0] + 12, g, kk, last=v)
        if kk == 7:
            peak[g] = state["m"]

    by_level(prepare)
    for n in range(3):
        sz[0, Z_AT[0] + n] = fields[0, 13 + n]
        sz[0, Z_AT[0] + 3 + n] = fields[1, 13 + n]
        sz[1, Z_AT[0] + n] = fields[0, n]
        sz[1, Z_AT[0] + 3 + n] = fields[1, n]
    sz[0, Z_AT[0] + 6] = w0[16]
    m1s[...] = jnp.max(jnp.maximum(peak[0], peak[1]), axis=0, keepdims=True)

    target = lax.broadcasted_iota(jnp.int32, (128, 128), 0).astype(F32).astype(jnp.bfloat16)
    row16 = lax.rem(lax.broadcasted_iota(jnp.int32, (16, 128), 0), 8)

    def deposit_row(kj):
        r = rad[pl.ds(kj, 8, stride=PITCH), :]
        w = wgt[pl.ds(kj, 8, stride=PITCH), :]
        c = col[pl.ds(kj, 8, stride=PITCH), :].astype(F32)
        live = row < counts[pl.ds(kj, 1), :]
        number = jnp.where(live, w, 0.0)
        area = number * (r * r)
        mass = area * r
        lhs = []
        for q in (number, area, mass):
            top = q.astype(jnp.bfloat16).astype(F32)
            pair = jnp.concatenate([top, q - top], axis=0)
            lhs.append(
                jnp.concatenate(
                    [jnp.where(row16 == s, pair, 0.0).astype(jnp.bfloat16) for s in range(8)], axis=1
                )
            )
        lhs = jnp.concatenate(lhs, axis=0)
        hot = jnp.concatenate(
            [
                jnp.where(
                    jnp.broadcast_to(c[s : s + 1, :], (128, 128)).astype(jnp.bfloat16) == target,
                    jnp.bfloat16(1.0), jnp.bfloat16(0.0),
                ).astype(jnp.float8_e4m3fn)
                for s in range(8)
            ],
            axis=1,
        )
        got = lax.dot_general(lhs, hot, (((1,), (1,)), ((), ())), preferred_element_type=F32)
        for m in range(3):
            dmat[pl.ds(pl.multiple_of(kj * 24 + 8 * m, 8), 8), :] = got[16 * m : 16 * m + 8] + got[16 * m + 8 : 16 * m + 16]

    def droplets(part):
        def step(i, carry):
            for n in range(ROWS):
                deposit_row(i * ROWS + n)
            return carry

        lax.fori_loop(SPLITS[part] // ROWS, SPLITS[part + 1] // ROWS, step, 0)

    def by_depth():
        def level(k):
            deep = []
            for s in range(8):
                moved = pltpu.roll(dep[s], lax.rem(128 - k, 128), 1)
                deep.append(jnp.broadcast_to(moved[:, 0:1], (8, 128)))
            for m in range(3):
                got = [dmat[pl.ds(k * 192 + 8 * m + s, 8, stride=24), :] for s in range(8)]
                for d in range(DEPTHS):
                    total = jnp.where(deep[0] == d, got[0], 0.0)
                    for s in range(1, 8):
                        total = total + jnp.where(deep[s] == d, got[s], 0.0)
                    gmat[m, d, k] = total

        def step(i, carry):
            level(2 * i)
            level(2 * i + 1)
            return carry

        lax.fori_loop(0, L // 2, step, 0)

    pl.semaphore_wait(barrier, len(partners))

    def whole(ref, i):
        return pltpu.make_async_remote_copy(
            src_ref=ref, dst_ref=ref, send_sem=small_sem.at[2 * i], recv_sem=small_sem.at[2 * i + 1],
            device_id=device(1), device_id_type=MESH,
        )

    first = []
    for o, (a, f, b) in enumerate(group1):
        first.append(
            pltpu.make_async_remote_copy(
                src_ref=m1s, dst_ref=m1r.at[o], send_sem=small_sem.at[0], recv_sem=small_sem.at[1],
                device_id=device(a, f * flip, b), device_id_type=MESH,
            )
        )
    for c in first:
        c.start()
    round0 = send(0)
    for c in early[1:]:
        c.wait()
    for a, (src, dst) in enumerate(((rad_h, rad), (wgt_h, wgt), (col_h, col))):
        pltpu.make_async_copy(src, dst.at[pl.ds(0, 1024)], load_sem.at[a]).wait()
    dep[...] = jnp.zeros_like(dep)
    dep[:, :, 0:16] = depth_in[...]
    droplets(0)

    def flux(a, q):
        central = 37.0 * (q[2] + q[3]) - 8.0 * (q[1] + q[4]) + (q[0] + q[5])
        upwind = 10.0 * (q[3] - q[2]) - 5.0 * (q[4] - q[1]) + (q[5] - q[0])
        return a * central - jnp.abs(a) * upwind

    def advect(q, k, xh, yh, winds):
        own = q[3 + k]
        u, um, v, vm, w, wm = winds
        line = [xm(own, xh[0], 3), xm(own, xh[0], 2), xm(own, xh[0], 1), own,
                xp(own, xh[1], 1), xp(own, xh[1], 2), xp(own, xh[1], 3)]
        total = flux(u, line[1:]) - flux(um, line[:-1])
        line = [ym(own, yh[0], 3), ym(own, yh[0], 2), ym(own, yh[0], 1), own,
                yp(own, yh[1], 1), yp(own, yh[1], 2), yp(own, yh[1], 3)]
        total = total + (flux(v, line[1:]) - flux(vm, line[:-1]))
        line = [q[k + n] for n in range(7)]
        total = total + (flux(w, line[1:]) - flux(wm, line[:-1]))
        return total * F32(-1.0 / 60.0)

    whole(m1r, 0).wait_recv()
    top = m1s[...]
    for o in range(len(group1)):
        top = jnp.maximum(top, m1r[o])
    m2s[...] = top
    second = []
    for o, a in enumerate(group2):
        second.append(
            pltpu.make_async_remote_copy(
                src_ref=m2s, dst_ref=m2r.at[o], send_sem=small_sem.at[2], recv_sem=small_sem.at[3],
                device_id=device(0, a), device_id_type=MESH,
            )
        )
    for c in second:
        c.start()

    arrive(round0)
    for n in range(3):
        for d, to, keep in ((0, n, klo), (1, 19 + n, khi)):
            c0[to] = rz[d, Z_AT[0] + n] * keep
            p0[to] = rz[d, Z_AT[0] + 3 + n] * keep
    w0[0] = rz[0, Z_AT[0] + 6] * klo
    winc[0] = -10.0 * (p0[3] - p0[2]) * klo
    lift[0] = 0.25 * (c0[2] + c0[3]) * klo

    def build(g, kk, k, state):
        lid = lid_at(g, kk)
        xc, xq, xu = x_halos(rx.at[0], g, kk)
        yc = y_halo3(ry, Y_AT[0], g, kk)
        yq = y_halo3(ry, Y_AT[0] + 6, g, kk)
        yv = roll_s(ry[0, Y_AT[0] + 12 + g], 7 - kk)
        p, u, v = p0[3 + k], fields[2, k], fields[3, k]
        w, wm = w0[1 + k], w0[k]
        um, vm = xm(u, xu, 1), ym(v, yv, 1)
        winds = (u, um, v, vm, w, wm)
        t = advect(c0, k, xc, yc, winds)
        q = advect(p0, k, xq, yq, winds)
        du = -10.0 * (xp(p, xq[1], 1) - p)
        dum = -10.0 * (p - xm(p, xq[0], 1))
        dv = -10.0 * (yp(p, yq[1], 1) - p)
        dvm = -10.0 * (p - ym(p, yq[0], 1))
        dw = masked(-10.0 * (p0[4 + k] - p), lid)
        dwm = winc[k]
        up = masked(0.25 * (c0[3 + k] + c0[4 + k]), lid)
        upm = lift[k]
        a = q - 10.0 * ((u - um) + (v - vm) + (w - wm))
        b = -10.0 * ((du - dum) + (dv - dvm) + ((dw + up) - (dwm + upm)))
        ta[k], aa[k], ba[k] = t, a, b
        uinc[k], vinc[k], winc[1 + k], lift[1 + k] = du, dv, dw, up
        um0[k], vm0[k], uminc[k], vminc[k] = um, vm, dum, dvm
        x_pack(state, 1, g, kk, t, a, None, b)
        for i, value in enumerate((a, b)):
            y_pack3(state, i, Y_AT[1] + 6 * i, g, kk, value)
        y_pack3(state, "t", Y_AT[6], g, kk, t)

    by_level(build)
    for i, a in enumerate((ta, aa, ba)):
        for n in range(3):
            sz[0, Z_AT[1] + 3 * i + n] = a[13 + n]
            sz[1, Z_AT[1] + 3 * i + n] = a[n]
    round1 = send(1)
    round6 = send(6)

    droplets(1)

    whole(m2r, 1).wait_recv()
    top = m2s[...]
    for o in range(len(group2)):
        top = jnp.maximum(top, m2r[o])
    top = jnp.broadcast_to(jnp.max(top, axis=1, keepdims=True), (1, 128))
    time_step = jnp.broadcast_to(0.6 / (1.0 + top), (8, 128))

    arrive(round1)
    t1 = time_step * F32(1.0 / 3.0)
    slot = lax.rem(lane, 16)
    for d in range(2):
        for g in range(2):
            third = jnp.where((slot >= 3) & (slot < 6), roll_l(rx[1, d, g], -5), 0.0)
            hx[d, g] = rx[0, d, g] + t1 * (rx[1, d, g] + t1 * third)
        for n in range(6):
            hy[d, 6 + n] = ry[d, 6 + n] + t1 * (ry[d, 14 + n] + t1 * ry[d, 20 + n])

    def section1(g, kk, k, state):
        cq[3 + k] = c0[3 + k] + t1 * ta[k]
        pq[3 + k] = p0[3 + k] + t1 * (aa[k] + t1 * ba[k])
        uf[k] = fields[2, k] + t1 * uinc[k]
        vf[k] = fields[3, k] + t1 * vinc[k]
        umf[k] = um0[k] + t1 * uminc[k]
        vmf[k] = vm0[k] + t1 * vminc[k]
        wf[1 + k] = w0[1 + k] + t1 * (winc[1 + k] + lift[1 + k])

    by_level(section1)
    wf[0] = w0[0] + t1 * (winc[0] + lift[0])
    for n in range(3):
        for d, to, keep in ((0, n, klo), (1, 19 + n, khi)):
            cq[to] = c0[to] + (t1 * keep) * rz[d, Z_AT[1] + n]
            pq[to] = p0[to] + (t1 * keep) * (rz[d, Z_AT[1] + 3 + n] + t1 * rz[d, Z_AT[1] + 6 + n])

    def tracer_rates(mx, my, start, old, finish):
        u, v, um, vm, w = old

        def step(g, kk, k, state):
            winds = (u[k], um[k], v[k], vm[k], w[1 + k], w[k])
            finish(g, kk, k, state, advect(cq, k, x_halo(mx, 0, g, kk), y_halo3(my, start, g, kk), winds))

        by_level(step)

    def lifts():
        lift[0] = 0.25 * (cq[2] + cq[3]) * klo

        def step(g, kk, k, state):
            lift[1 + k] = masked(0.25 * (cq[3 + k] + cq[4 + k]), lid_at(g, kk))

        by_level(step)

    def narrow(r, g, kk, k, state, p):
        x_pack(state, r, g, kk, None, p)
        y_pack1(state, "p", Y_AT[r], g, kk, last=p, first=p)

    def narrow_send(r, p):
        sz[0, Z_AT[r]] = p[16]
        sz[1, Z_AT[r]] = p[1]
        return send(r)

    def first_substep(r, s, mx, my, start, old, new, rate_ref):
        u_, v_, um_, vm_, w_ = old
        un_, vn_, umn_, vmn_, wn_ = new
        wn_[0] = w0[0] + s * (winc[0] + lift[0])

        def step(g, kk, k, state):
            winds = (u_[k], um_[k], v_[k], vm_[k], w_[1 + k], w_[k])
            rate = advect(pq, k, x_halo(mx, 3, g, kk), y_halo3(my, start, g, kk), winds)
            rate_ref[k] = rate
            u = fields[2, k] + s * uinc[k]
            um = um0[k] + s * uminc[k]
            v = fields[3, k] + s * vinc[k]
            vm = vm0[k] + s * vminc[k]
            w = w0[1 + k] + s * (winc[1 + k] + lift[1 + k])
            wm = w0[k] + s * (winc[k] + lift[k])
            p = p0[3 + k] + s * (rate - 10.0 * ((u - um) + (v - vm) + (w - wm)))
            pf[1 + k], un_[k], vn_[k], umn_[k], vmn_[k], wn_[1 + k] = p, u, v, um, vm, w
            narrow(r, g, kk, k, state, p)

        by_level(step)
        return narrow_send(r, pf)

    def next_substep(r, made, s, ps, winds, rate_ref, finish):
        u_, v_, um_, vm_, w_ = winds
        s10 = s * 10.0
        arrive(made)
        ps[0] = rz[0, Z_AT[r]] * klo
        ps[17] = rz[1, Z_AT[r]] * khi
        w_[0] = w_[0] + s * lift[0] - (s10 * klo) * (ps[1] - ps[0])

        def step(g, kk, k, state):
            lid = lid_at(g, kk)
            xq = x_halo(rx.at[r], 3, g, kk)
            p = ps[1 + k]
            ylo, yhi = roll_s(ry[0, Y_AT[r] + g], 7 - kk), roll_s(ry[1, Y_AT[r] + g], -kk)
            u = u_[k] - s10 * (xp(p, xq[1], 1) - p)
            um = um_[k] - s10 * (p - xm(p, xq[0], 1))
            v = v_[k] - s10 * (yp(p, yhi, 1) - p)
            vm = vm_[k] - s10 * (p - ym(p, ylo, 1))
            w = w_[1 + k] + s * lift[1 + k] - masked(s10 * (ps[2 + k] - p), lid)
            wm = state["w"] if kk else w_[k]
            state["w"] = w
            pn = p + s * (rate_ref[k] - 10.0 * ((u - um) + (v - vm) + (w - wm)))
            finish(g, kk, k, state, pn, u, v, um, vm, w)

        by_level(step)

    state_f = (uf, vf, umf, vmf, wf)
    state_g = (ug, vg, umg, vmg, wg)

    t2 = time_step * F32(0.25)
    half = time_step * F32(0.5)
    lifts()
    round2 = first_substep(2, t2, hx, hy, 6, state_f, state_g, aa)

    def tracer2(g, kk, k, state, rate):
        c = c0[3 + k] + half * rate
        tr[k] = c
        x_pack(state, 7, g, kk, c)
        y_pack3(state, "c", Y_AT[7], g, kk, c)

    arrive(round6)
    for d in range(2):
        for n in range(6):
            hy[d, n] = ry[d, n] + t1 * ry[d, Y_AT[6] + n]
    tracer_rates(hx, hy, 0, state_f, tracer2)
    for n in range(3):
        sz[0, Z_AT[7] + n] = tr[13 + n]
        sz[1, Z_AT[7] + n] = tr[n]
    round7 = send(7)
    by_depth()

    def finish2(g, kk, k, state, p, u, v, um, vm, w):
        pq[3 + k] = p
        ug[k], vg[k], umg[k], vmg[k], wg[1 + k] = u, v, um, vm, w
        cq[3 + k] = tr[k]
        x_pack(state, 3, g, kk, None, p)
        y_pack3(state, "p", Y_AT[3], g, kk, p)

    next_substep(2, round2, t2, pf, state_g, aa, finish2)
    for n in range(3):
        sz[0, Z_AT[3] + n] = pq[16 + n]
        sz[1, Z_AT[3] + n] = pq[3 + n]
    round3 = send(3)

    arrive(round7)
    for n in range(3):
        for d, to, keep in ((0, n, klo), (1, 19 + n, khi)):
            cq[to] = rz[d, Z_AT[7] + n] * keep
    t3 = time_step * F32(0.25)
    s10 = t3 * 10.0
    alpha = s10 * s10
    lifts()

    def forcing(g, kk, k, state):
        value = (lift[1 + k] - lift[k]) * (-0.1 * alpha)
        ek[0, 3 + k] = value
        narrow(5, g, kk, k, state, value)

    by_level(forcing)
    sz[0, Z_AT[5]] = ek[0, 18]
    sz[1, Z_AT[5]] = ek[0, 3]
    round5 = send(5)

    def tracer3(g, kk, k, state, rate):
        c = c0[3 + k] + time_step * rate
        out[0, k] = c
        growth = jnp.minimum(jnp.exp(0.3 * c), F32(3.0e38))
        ta[k] = growth
        ba[k] = jnp.sqrt(growth)

    tracer_rates(rx.at[7], ry, Y_AT[7], state_g, tracer3)

    def landed(t):
        totals = [None, None, None]
        for k in range(max(t, 0), min(t + DEPTHS, L)):
            d = k - t
            grow, root = ta[k], ba[k]
            parts = (gmat[0, d, k], gmat[1, d, k] * grow, gmat[2, d, k] * grow * root)
            totals = [a if b is None else b + a for a, b in zip(parts, totals)]
        return totals

    for t in range(-8, 0):
        for m, value in enumerate(landed(t)):
            ext[m, t + 8] = value
    dropped = pltpu.make_async_remote_copy(
        src_ref=ext, dst_ref=fall, send_sem=fall_sem.at[0], recv_sem=fall_sem.at[1],
        device_id={"gz": near("gz", -1)}, device_id_type=MESH,
    )
    dropped.start()

    arrive(round3)
    for n in range(3):
        for d, to, keep in ((0, n, klo), (1, 19 + n, khi)):
            pq[to] = rz[d, Z_AT[3] + n] * keep

    wf[0] = w0[0] + t3 * (winc[0] + lift[0])

    def open3(g, kk, k, state):
        winds = (ug[k], umg[k], vg[k], vmg[k], wg[1 + k], wg[k])
        rate = advect(pq, k, x_halo(rx.at[3], 3, g, kk), y_halo3(ry, Y_AT[3], g, kk), winds)
        u = fields[2, k] + t3 * uinc[k]
        um = um0[k] + t3 * uminc[k]
        v = fields[3, k] + t3 * vinc[k]
        vm = vm0[k] + t3 * vminc[k]
        w = w0[1 + k] + t3 * (winc[1 + k] + lift[1 + k])
        wm = w0[k] + t3 * (winc[k] + lift[k])
        e = t3 * (rate - 10.0 * ((u - um) + (v - vm) + (w - wm)))
        p = p0[3 + k] + e
        e = e + ek[0, 3 + k]
        ep[0, 3 + k], eg[0, 3 + k] = p, e
        uf[k], vf[k], wf[1 + k] = u, v, w
        x_pack(state, 4, g, kk, p, e)
        y_pack3(state, "p", Y_AT[4], g, kk, p)
        y_pack2(state, "e", Y_AT[4] + 6, g, kk, e)

    by_level(open3)
    for n in range(3):
        sz[0, Z_AT[4] + n] = ep[0, 16 + n]
        sz[1, Z_AT[4] + n] = ep[0, 3 + n]
    for n in range(2):
        sz[0, Z_AT[4] + 3 + n] = eg[0, 17 + n]
        sz[1, Z_AT[4] + 3 + n] = eg[0, 3 + n]
    for d in range(2):
        syz[d, 0] = jnp.where(row < 2, roll_s(sy[d, Y_AT[4] + 9], 2), sy[d, Y_AT[4] + 5])
        syz[d, 1] = jnp.where(row < 6, sy[d, Y_AT[4]], roll_s(sy[d, Y_AT[4] + 6], 6))
        low, high = sx[4, d, 0], sx[4, d, 1]
        sxy[d, 0] = jnp.where(row < 4, roll_s(low, 3), roll_s(high, 7))
        sxy[d, 1] = jnp.where(row < 4, low, roll_s(high, 4))
        for c, tile in ((0, high), (1, low)):
            scorner[4 * d + c] = tile[7:8, :]
            scorner[4 * d + 2 + c] = tile[0:1, :]
    round4 = send(4)
    for i, (a, b, c) in enumerate(edges):
        if c is None:
            src, dst = sxy.at[a, b], rxy.at[a, b]
        elif b is None:
            src, dst = sx.at[4, a, 1 - c], rxz.at[a, c]
        elif a is None:
            src, dst = syz.at[b, c], ryz.at[b, c]
        else:
            src, dst = scorner.at[4 * a + 2 * b + c], rcorner.at[4 * a + 2 * b + c]
        corner = None not in (a, b, c)
        pltpu.make_async_remote_copy(
            src_ref=src, dst_ref=dst,
            send_sem=small_sem.at[4] if corner else send_sem.at[0],
            recv_sem=small_sem.at[5] if corner else recv_sem.at[4],
            device_id=edge_device((a, b, c)), device_id_type=MESH,
        ).start()
    for t in range(0, L):
        for m, value in enumerate(landed(t)):
            mom[m, t] = value

    def join_l(lo, hi):
        return jnp.where(lane < 64, hi, lo)

    def join_s(lo, hi):
        return jnp.where(row < 4, hi, lo)

    def x_one(tile, d, at, kk):
        return roll_l(tile, 125 - at - 16 * kk if d == 0 else -at - 16 * kk)

    arrive(round5)

    def assemble_forcing(g, kk, k, state):
        at = 3 + k
        ek[1, at] = join_s(roll_s(ry[0, Y_AT[5] + g], 7 - kk), roll_s(ry[1, Y_AT[5] + g], -kk))
        ek[2, at] = join_l(*x_halo(rx.at[5], 3, g, kk))

    by_level(assemble_forcing)
    ek[0, 2] = rz[0, Z_AT[5]]
    ek[0, 19] = rz[1, Z_AT[5]]
    dropped.wait_recv()
    for m in range(3):
        for n in range(8):
            mom[m, 8 + n] = mom[m, 8 + n] + fall[m, n] * khi

    arrive(round4)
    whole(rcorner, 2).wait_recv()

    for d in both:
        xy[d, 0, 0], xy[d, 0, 1] = roll_s(rxy[d, 0], 5), roll_s(rxy[d, 0], 1)
        xy[d, 1, 0], xy[d, 1, 1] = rxy[d, 1], roll_s(rxy[d, 1], 4)

    def assemble(g, kk, k, state):
        at = 3 + k
        ep[1, at] = join_s(*y_halo3(ry, Y_AT[4], g, kk))
        eg[1, at] = join_s(*y_halo2(ry, Y_AT[4] + 6, g, kk))
        for off, ref in ((0, ep), (3, eg)):
            ref[2, at] = join_l(*(x_one(rx[4, d, g], d, off, kk) for d in both))
            ref[3, at] = join_s(*(join_l(*(x_one(xy[d, b, g], d, off, kk) for d in both)) for b in both))

    by_level(assemble)
    for n in range(3):
        ep[0, n] = rz[0, Z_AT[4] + n]
        ep[0, 19 + n] = rz[1, Z_AT[4] + n]
    for n in range(2):
        eg[0, 1 + n] = rz[0, Z_AT[4] + 3 + n]
        eg[0, 19 + n] = rz[1, Z_AT[4] + 3 + n]
    for c, levels in ((0, ((1, 6), (2, 7))), (1, ((19, 0), (20, 1)))):
        for to, kk in levels:
            t, o = divmod(3 * kk, 8)
            ep[1, to] = join_s(roll_s(ryz[0, c], 5 - o), roll_s(ryz[1, c], -o))
            ep[2, to] = join_l(*(x_one(rxz[d, c], d, 0, kk) for d in both))
            if to in (2, 19):
                o = 0 if c == 0 else 6
                eg[1, to] = join_s(roll_s(ryz[0, c], 6 - o), roll_s(ryz[1, c], -o))
                eg[2, to] = join_l(*(x_one(rxz[d, c], d, 3, kk) for d in both))
                ends = [
                    join_l(*(x_one(jnp.broadcast_to(rcorner[4 * d + 2 * b + c], (8, 128)), d, 0, kk) for d in both))
                    for b in both
                ]
                ep[3, to] = join_s(*ends)

    other_x, other_y = (2, 3, 0, 1), (1, 0, 3, 2)

    def neighbours(ref, part, at):
        q, hx_, hy_ = ref[part, at], ref[other_x[part], at], ref[other_y[part], at]
        return q, xp(q, hx_, 1), xm(q, hx_, 1), yp(q, hy_, 1), ym(q, hy_, 1)

    def laplacian(ref, part, at, low=None, high=None):
        q, a, b, c, d = neighbours(ref, part, at)
        up, down = masked(ref[part, at + 1] - q, high), masked(q - ref[part, at - 1], low)
        return q, (a - q, c - q, up), ((a - q) - (q - b)) + ((c - q) - (q - d)) + (up - down)

    def edge_masks(at, g, kk):
        low = jnp.where(g == 0, klo, F32(1.0)) if kk == 0 else None
        return low, lid_at(g, kk)

    def winds3(k, steps):
        uf[k] = uf[k] - s10 * steps[0]
        vf[k] = vf[k] - s10 * steps[1]
        wf[1 + k] = wf[1 + k] + t3 * lift[1 + k] - s10 * steps[2]

    def second3(part, at, low=None, high=None):
        q, steps, lap = laplacian(ep, part, at, low, high)
        e = eg[part, at] + alpha * lap
        eg[part, at] = e
        en[part, at] = q + e
        return steps

    def two(g, kk, k, state):
        low, high = edge_masks(3 + k, g, kk)
        winds3(k, second3(0, 3 + k, low, high))
        for part in (1, 2, 3):
            second3(part, 3 + k, low, high)

    by_level(two)
    second3(0, 1)
    second3(0, 20)
    for part in (0, 1, 2):
        second3(part, 2, None, klo)
        second3(part, 19, khi, None)

    def third3(part, at, low=None, high=None):
        q, steps, lap = laplacian(en, part, at, low, high)
        e = eg[part, at] + ek[part, at] + alpha * lap
        eg[part, at] = e
        ep[part, at] = q + e
        return steps

    def three(g, kk, k, state):
        low, high = edge_masks(3 + k, g, kk)
        winds3(k, third3(0, 3 + k, low, high))
        for part in (1, 2):
            third3(part, 3 + k, low, high)

    by_level(three)
    third3(0, 2, None, klo)
    third3(0, 19, khi, None)

    def four(g, kk, k, state):
        low, high = edge_masks(3 + k, g, kk)
        q, steps, lap = laplacian(ep, 0, 3 + k, low, high)
        out[1, k] = q + (eg[0, 3 + k] + ek[0, 3 + k] + alpha * lap)
        out[2, k] = uf[k] - s10 * steps[0]
        out[3, k] = vf[k] - s10 * steps[1]
        out[4, k] = wf[1 + k] + t3 * lift[1 + k] - s10 * steps[2]

    by_level(four)

    dropped.wait_send()
    for i, ref in enumerate((m1r, m2r, rcorner)):
        whole(ref, i).wait_send()
    tiles(sum(sent), send_sem.at[0], recv_sem.at[0]).wait_send()


def solution(mesh):
    sizes = (mesh.shape["gx"], mesh.shape["gy"], mesh.shape["gz"])
    nx, ny, nz = sizes
    vm = lambda *shape: pltpu.VMEM(shape + (8, 128), F32)
    dma = pltpu.SemaphoreType.DMA
    scratch = [
        vm(5, L), pltpu.VMEM((128, 128), jnp.int32), pltpu.VMEM((8, 8, 16), jnp.int32),
        pltpu.VMEM((8 * PITCH, 128), F32), pltpu.VMEM((8 * PITCH, 128), F32), pltpu.VMEM((8 * PITCH, 128), jnp.int32),
        pltpu.VMEM((8, 8, 128), jnp.int32), pltpu.VMEM((128 * 24, 128), F32), vm(3, DEPTHS, L), vm(3, 8), vm(3, 8),
        vm(22), vm(22), vm(17), vm(22), vm(22), vm(2),
        vm(16), vm(16), vm(16), vm(16), vm(16), vm(17), vm(16), vm(16), vm(16), vm(16),
        vm(16), vm(17), vm(18), vm(16), vm(16), vm(16), vm(16), vm(17), vm(16), vm(16), vm(16), vm(16), vm(17),
        vm(2, 2), vm(2, 12), vm(4, 22), vm(4, 22), vm(4, 22), vm(4, 22),
        vm(8, 2, 2), vm(8, 2, 2), vm(2, Y_ALL), vm(2, Y_ALL), vm(2, Z_ALL), vm(2, Z_ALL),
        vm(2, 2), vm(2, 2), pltpu.VMEM((8, 1, 128), F32),
        vm(2, 2), vm(2, 2), vm(2, 2), pltpu.VMEM((8, 1, 128), F32), vm(2, 2, 2),
        pltpu.VMEM((1, 128), F32), pltpu.VMEM((2 * nx * nz - 1, 1, 128), F32),
        pltpu.VMEM((1, 128), F32), pltpu.VMEM((ny // 2 - 1, 1, 128), F32),
        dma((1,)), dma((8,)), dma((6,)), dma((2,)), dma((3,)), dma((3,)),
    ]
    vmem = pl.BlockSpec(memory_space=pltpu.VMEM)
    hbm = pl.BlockSpec(memory_space=pl.ANY)

    def per_device(fields, radius, weight, column, counts, fall_depth):
        held = pl.pallas_call(
            functools.partial(kernel, sizes),
            out_shape=(pltpu.VMEM((5, L, 8, 128), F32), pltpu.VMEM((3, L, 8, 128), F32)),
            in_specs=[hbm] * 6,
            out_specs=(vmem, vmem),
            scratch_shapes=scratch,
            compiler_params=pltpu.CompilerParams(collective_id=0, has_side_effects=True),
            name="slab_step",
        )(
            fields,
            counts.reshape(128, 128),
            jnp.transpose(fall_depth[:, :, :, 0], (0, 2, 1)),
            radius.reshape(1024, 128),
            weight.reshape(1024, 128),
            column.reshape(1024, 128),
        )
        return held

    cut = P(None, "gz", "gy", "gx")
    return jax.shard_map(
        per_device,
        mesh=mesh,
        in_specs=(cut, cut, cut, cut, P("gz", "gy", "gx"), cut),
        out_specs=(cut, cut),
        check_vma=False,
    )
```

```python
import functools

import jax
import jax.numpy as jnp
from jax import lax
from jax.experimental import pallas as pl
from jax.experimental.pallas import tpu as pltpu
from jax.sharding import PartitionSpec as P

MESH = pl.DeviceIdType.MESH
F32 = jnp.float32
L = 16
DEPTHS = 9
PITCH = 136
Y_TILES = {0: (14, 12), 1: (12, 12), 6: (6, 6), 7: (6, 6), 3: (6, 6), 2: (2, 2), 5: (2, 2), 4: (10, 10)}
Z_TILES = {0: (7, 6), 1: (9, 9), 7: (3, 3), 3: (3, 3), 2: (1, 1), 5: (1, 1), 4: (5, 5)}
Y_AT = {0: 0, 1: 14, 6: 26, 7: 32, 3: 38, 2: 44, 5: 46, 4: 48}
Z_AT = {0: 0, 1: 7, 7: 16, 3: 19, 2: 22, 5: 23, 4: 24}
Y_ALL, Z_ALL = 58, 29
SPLITS = (0, 72, 128)
ROWS = 4


def kernel(
    sizes,
    fields_h, counts_h, depth_h, rad_h, wgt_h, col_h,
    out, mom,
    fields, counts, depth_in, rad, wgt, col, dep, dmat, gmat, ext, fall,
    c0, p0, w0, cq, pq, peak,
    ta, aa, ba, uinc, vinc, winc, um0, vm0, uminc, vminc,
    tr, lift, pf, uf, vf, umf, vmf, wf, ug, vg, umg, vmg, wg,
    hx, hy, ep, eg, ek, en,
    sx, rx, sy, ry, sz, rz, syz, sxy, scorner, rxy, rxz, ryz, rcorner, xy,
    m1s, m1r, m2s, m2r,
    send_sem, recv_sem, small_sem, fall_sem, load_sem, field_sem,
):
    nx, ny, nz = sizes
    ix, iy, iz = lax.axis_index("gx"), lax.axis_index("gy"), lax.axis_index("gz")

    def near(axis, step):
        i, n = {"gx": (ix, nx), "gy": (iy, ny), "gz": (iz, nz)}[axis]
        return lax.rem(i + (step + n), n)

    early = [
        pltpu.make_async_copy(src, dst, field_sem.at[n])
        for n, (src, dst) in enumerate(((fields_h, fields), (counts_h, counts), (depth_h, depth_in)))
    ]
    loads = []
    for a, (src, dst) in enumerate(((rad_h, rad), (wgt_h, wgt), (col_h, col))):
        for s in range(8):
            loads.append(
                pltpu.make_async_copy(
                    src.at[pl.ds(s * 128, 128)], dst.at[pl.ds(s * PITCH, 128)], load_sem.at[a]
                )
            )
    for n in range(5):
        pltpu.make_async_copy(fields_h.at[n], fields.at[n], field_sem.at[0]).start()
    for c in early[1:]:
        c.start()

    def device(a=0, b=0, c=0):
        return {"gx": near("gx", a), "gy": near("gy", b), "gz": near("gz", c)}

    flip = 1 - 2 * lax.rem(iy, 2)
    group1 = [(a, f, b) for a in range(nx) for f in range(2) for b in range(nz) if (a, f, b) != (0, 0, 0)]
    group2 = [2 * n for n in range(1, ny // 2)]
    both = (0, 1)
    edges = [(a, b, None) for a in both for b in both]
    edges += [(a, None, c) for a in both for c in both]
    edges += [(None, b, c) for b in both for c in both]
    edges += [(a, b, c) for a in both for b in both for c in both]

    def edge_device(edge):
        return device(*(0 if d is None else 1 - 2 * d for d in edge))

    partners = [device(a, f * flip, b) for a, f, b in group1] + [device(0, a) for a in group2]
    partners += [device(0, 1), device(0, -1)] + [edge_device(e) for e in edges if e[1] is not None]
    barrier = pltpu.get_barrier_semaphore()
    for partner in reversed(partners):
        pl.semaphore_signal(barrier, inc=1, device_id=partner, device_id_type=MESH)

    lane = lax.broadcasted_iota(jnp.int32, (8, 128), 1)
    row = lax.broadcasted_iota(jnp.int32, (8, 128), 0)
    klo = (iz > 0).astype(F32)
    khi = (iz < nz - 1).astype(F32)
    zero = jnp.zeros((8, 128), F32)

    def roll_l(x, s):
        s = s % 128
        return pltpu.roll(x, s, 1) if s else x

    def roll_s(x, s):
        s = s % 8
        return pltpu.roll(x, s, 0) if s else x

    def xp(q, h, n):
        return roll_l(jnp.where(lane < n, h, q), -n)

    def xm(q, h, n):
        return roll_l(jnp.where(lane >= 128 - n, h, q), n)

    def yp(q, h, n):
        return roll_s(jnp.where(row < n, h, q), -n)

    def ym(q, h, n):
        return roll_s(jnp.where(row >= 8 - n, h, q), n)

    def put_l(message, value, at, width):
        return jnp.where((lane >= at) & (lane < at + width), value, message)

    def by_level(fn):
        def group(g, carry):
            state = {}
            for kk in range(8):
                fn(g, kk, g * 8 + kk, state)
            return carry

        lax.fori_loop(0, 2, group, 0)

    def copies(r):
        made = []
        for d, step in ((0, 1), (1, -1)):
            y = pl.ds(Y_AT[r], Y_TILES[r][d])
            parts = [(sy.at[d, y], ry.at[d, y], "gy")]
            if r in Z_TILES:
                z = pl.ds(Z_AT[r], Z_TILES[r][d])
                parts += [(sz.at[d, z], rz.at[d, z], "gz"), (sx.at[r, d], rx.at[r, d], "gx")]
            for i, (src, dst, axis) in enumerate(parts):
                made.append(
                    pltpu.make_async_remote_copy(
                        src_ref=src, dst_ref=dst,
                        send_sem=send_sem.at[0], recv_sem=recv_sem.at[r],
                        device_id={axis: near(axis, step)}, device_id_type=MESH,
                    )
                )
        return made

    def send(r):
        for c in copies(r):
            c.start()
        n = sum(Y_TILES[r]) + (sum(Z_TILES[r]) + 4 if r in Z_TILES else 0) + (12 if r == 4 else 0)
        sent.append(n)
        return r, n

    sent = []

    def tiles(n, send, recv):
        span = dmat.at[pl.ds(0, 8 * n)]
        return pltpu.make_async_remote_copy(
            src_ref=span, dst_ref=span, send_sem=send, recv_sem=recv, device_id=device(1), device_id_type=MESH
        )

    def arrive(made):
        r, n = made
        tiles(n, send_sem.at[0], recv_sem.at[r]).wait_recv()

    def x_pack(state, r, g, kk, a=None, b=None, wind=None, third=None):
        base = 16 * kk
        lo, hi = state.get("xlo", zero), state.get("xhi", zero)
        for value, at in ((a, 0), (b, 3), (third, 8)):
            if value is not None:
                lo = put_l(lo, roll_l(value, base + at + 3), base + at, 3)
                hi = put_l(hi, roll_l(value, base + at), base + at, 3)
        if wind is not None:
            lo = put_l(lo, roll_l(wind, base + 7), base + 6, 1)
        state["xlo"], state["xhi"] = lo, hi
        if kk == 7:
            sx[r, 0, g] = lo
            sx[r, 1, g] = hi

    def y_pack3(state, name, start, g, kk, q):
        t, o = divmod(3 * kk, 8)
        for d, moved in ((0, roll_s(q, o - 5)), (1, roll_s(q, o))):
            key = (name, d)
            tiles = state.setdefault(key, [None, None, None])
            if tiles[t] is None:
                tiles[t] = moved
            else:
                tiles[t] = jnp.where(row >= o, moved, tiles[t])
            if o > 5:
                tiles[t + 1] = moved
            if o >= 5:
                sy[d, start + g * 3 + t] = tiles[t]

    def y_halo3(ref, start, g, kk):
        t, o = divmod(3 * kk, 8)
        got = []
        for d in range(2):
            value = ref[d, start + g * 3 + t]
            if o > 5:
                value = jnp.where(row >= o, value, ref[d, start + g * 3 + t + 1])
            got.append(roll_s(value, 5 - o if d == 0 else -o))
        return got

    def y_pack1(state, name, start, g, kk, last=None, first=None):
        for d, value, by in ((0, last, kk - 7), (1, first, kk)):
            if value is not None:
                key = (name, d)
                moved = roll_s(value, by)
                state[key] = moved if kk == 0 else jnp.where(row >= kk, moved, state[key])
                if kk == 7:
                    sy[d, start + g] = state[key]

    def y_pack2(state, name, start, g, kk, q):
        t, o = divmod(2 * kk, 8)
        for d, by in ((0, o - 6), (1, o)):
            key = (name, d)
            moved = roll_s(q, by)
            state[key] = moved if o == 0 else jnp.where(row >= o, moved, state[key])
            if o == 6:
                sy[d, start + g * 2 + t] = state[key]

    def y_halo2(ref, start, g, kk):
        t, o = divmod(2 * kk, 8)
        return [roll_s(ref[d, start + g * 2 + t], 6 - o if d == 0 else -o) for d in range(2)]

    def x_halos(mx, g, kk):
        lo, hi = mx[0, g], mx[1, g]
        base = 16 * kk
        return (roll_l(lo, 125 - base), roll_l(hi, -base)), (roll_l(lo, 122 - base), roll_l(hi, -base - 3)), roll_l(lo, 121 - base)

    def x_halo(ref, at, g, kk):
        base = 16 * kk + at
        return roll_l(ref[0, g], 125 - base), roll_l(ref[1, g], -base)

    def lid_at(g, kk):
        return jnp.where(g == 1, khi, F32(1.0)) if kk == 7 else None

    def masked(value, mask):
        return value if mask is None else value * mask

    early[0].wait()
    for c in loads:
        c.start()

    def prepare(g, kk, k, state):
        c, p, u, v = fields[0, k], fields[1, k], fields[2, k], fields[3, k]
        w = masked(fields[4, k], lid_at(g, kk))
        c0[3 + k] = c
        p0[3 + k] = p
        w0[1 + k] = w
        speed = jnp.abs(u) + jnp.abs(v) + jnp.abs(w)
        state["m"] = speed if kk == 0 else jnp.maximum(state["m"], speed)
        x_pack(state, 0, g, kk, c, p, u)
        y_pack3(state, "c", Y_AT[0], g, kk, c)
        y_pack3(state, "p", Y_AT[0] + 6, g, kk, p)
        y_pack1(state, "v", Y_AT[0] + 12, g, kk, last=v)
        if kk == 7:
            peak[g] = state["m"]

    by_level(prepare)
    for n in range(3):
        sz[0, Z_AT[0] + n] = fields[0, 13 + n]
        sz[0, Z_AT[0] + 3 + n] = fields[1, 13 + n]
        sz[1, Z_AT[0] + n] = fields[0, n]
        sz[1, Z_AT[0] + 3 + n] = fields[1, n]
    sz[0, Z_AT[0] + 6] = w0[16]
    m1s[...] = jnp.max(jnp.maximum(peak[0], peak[1]), axis=0, keepdims=True)

    target = lax.broadcasted_iota(jnp.int32, (128, 128), 0).astype(F32).astype(jnp.bfloat16)
    row16 = lax.rem(lax.broadcasted_iota(jnp.int32, (16, 128), 0), 8)

    def deposit_row(kj):
        r = rad[pl.ds(kj, 8, stride=PITCH), :]
        w = wgt[pl.ds(kj, 8, stride=PITCH), :]
        c = col[pl.ds(kj, 8, stride=PITCH), :].astype(F32)
        live = row < counts[pl.ds(kj, 1), :]
        number = jnp.where(live, w, 0.0)
        area = number * (r * r)
        mass = area * r
        lhs = []
        for q in (number, area, mass):
            top = q.astype(jnp.bfloat16).astype(F32)
            pair = jnp.concatenate([top, q - top], axis=0)
            lhs.append(
                jnp.concatenate(
                    [jnp.where(row16 == s, pair, 0.0).astype(jnp.bfloat16) for s in range(8)], axis=1
                )
            )
        lhs = jnp.concatenate(lhs, axis=0)
        hot = jnp.concatenate(
            [
                jnp.where(
                    jnp.broadcast_to(c[s : s + 1, :], (128, 128)).astype(jnp.bfloat16) == target,
                    jnp.bfloat16(1.0), jnp.bfloat16(0.0),
                ).astype(jnp.float8_e4m3fn)
                for s in range(8)
            ],
            axis=1,
        )
        got = lax.dot_general(lhs, hot, (((1,), (1,)), ((), ())), preferred_element_type=F32)
        for m in range(3):
            dmat[pl.ds(pl.multiple_of(kj * 24 + 8 * m, 8), 8), :] = got[16 * m : 16 * m + 8] + got[16 * m + 8 : 16 * m + 16]

    def droplets(part):
        def step(i, carry):
            for n in range(ROWS):
                deposit_row(i * ROWS + n)
            return carry

        lax.fori_loop(SPLITS[part] // ROWS, SPLITS[part + 1] // ROWS, step, 0)

    def by_depth():
        def level(k):
            deep = []
            for s in range(8):
                moved = pltpu.roll(dep[s], lax.rem(128 - k, 128), 1)
                deep.append(jnp.broadcast_to(moved[:, 0:1], (8, 128)))
            for m in range(3):
                got = [dmat[pl.ds(k * 192 + 8 * m + s, 8, stride=24), :] for s in range(8)]
                for d in range(DEPTHS):
                    total = jnp.where(deep[0] == d, got[0], 0.0)
                    for s in range(1, 8):
                        total = total + jnp.where(deep[s] == d, got[s], 0.0)
                    gmat[m, d, k] = total

        def step(i, carry):
            level(2 * i)
            level(2 * i + 1)
            return carry

        lax.fori_loop(0, L // 2, step, 0)

    pl.semaphore_wait(barrier, len(partners))

    def whole(ref, i):
        return pltpu.make_async_remote_copy(
            src_ref=ref, dst_ref=ref, send_sem=small_sem.at[2 * i], recv_sem=small_sem.at[2 * i + 1],
            device_id=device(1), device_id_type=MESH,
        )

    first = []
    for o, (a, f, b) in enumerate(group1):
        first.append(
            pltpu.make_async_remote_copy(
                src_ref=m1s, dst_ref=m1r.at[o], send_sem=small_sem.at[0], recv_sem=small_sem.at[1],
                device_id=device(a, f * flip, b), device_id_type=MESH,
            )
        )
    for c in first:
        c.start()
    round0 = send(0)
    for c in early[1:]:
        c.wait()
    for a, (src, dst) in enumerate(((rad_h, rad), (wgt_h, wgt), (col_h, col))):
        pltpu.make_async_copy(src, dst.at[pl.ds(0, 1024)], load_sem.at[a]).wait()
    dep[...] = jnp.zeros_like(dep)
    dep[:, :, 0:16] = depth_in[...]
    droplets(0)

    def flux(a, q):
        central = 37.0 * (q[2] + q[3]) - 8.0 * (q[1] + q[4]) + (q[0] + q[5])
        upwind = 10.0 * (q[3] - q[2]) - 5.0 * (q[4] - q[1]) + (q[5] - q[0])
        return a * central - jnp.abs(a) * upwind

    def advect(q, k, xh, yh, winds):
        own = q[3 + k]
        u, um, v, vm, w, wm = winds
        line = [xm(own, xh[0], 3), xm(own, xh[0], 2), xm(own, xh[0], 1), own,
                xp(own, xh[1], 1), xp(own, xh[1], 2), xp(own, xh[1], 3)]
        total = flux(u, line[1:]) - flux(um, line[:-1])
        line = [ym(own, yh[0], 3), ym(own, yh[0], 2), ym(own, yh[0], 1), own,
                yp(own, yh[1], 1), yp(own, yh[1], 2), yp(own, yh[1], 3)]
        total = total + (flux(v, line[1:]) - flux(vm, line[:-1]))
        line = [q[k + n] for n in range(7)]
        total = total + (flux(w, line[1:]) - flux(wm, line[:-1]))
        return total * F32(-1.0 / 60.0)

    whole(m1r, 0).wait_recv()
    top = m1s[...]
    for o in range(len(group1)):
        top = jnp.maximum(top, m1r[o])
    m2s[...] = top
    second = []
    for o, a in enumerate(group2):
        second.append(
            pltpu.make_async_remote_copy(
                src_ref=m2s, dst_ref=m2r.at[o], send_sem=small_sem.at[2], recv_sem=small_sem.at[3],
                device_id=device(0, a), device_id_type=MESH,
            )
        )
    for c in second:
        c.start()

    arrive(round0)
    for n in range(3):
        for d, to, keep in ((0, n, klo), (1, 19 + n, khi)):
            c0[to] = rz[d, Z_AT[0] + n] * keep
            p0[to] = rz[d, Z_AT[0] + 3 + n] * keep
    w0[0] = rz[0, Z_AT[0] + 6] * klo
    winc[0] = -10.0 * (p0[3] - p0[2]) * klo
    lift[0] = 0.25 * (c0[2] + c0[3]) * klo

    def build(g, kk, k, state):
        lid = lid_at(g, kk)
        xc, xq, xu = x_halos(rx.at[0], g, kk)
        yc = y_halo3(ry, Y_AT[0], g, kk)
        yq = y_halo3(ry, Y_AT[0] + 6, g, kk)
        yv = roll_s(ry[0, Y_AT[0] + 12 + g], 7 - kk)
        p, u, v = p0[3 + k], fields[2, k], fields[3, k]
        w, wm = w0[1 + k], w0[k]
        um, vm = xm(u, xu, 1), ym(v, yv, 1)
        winds = (u, um, v, vm, w, wm)
        t = advect(c0, k, xc, yc, winds)
        q = advect(p0, k, xq, yq, winds)
        du = -10.0 * (xp(p, xq[1], 1) - p)
        dum = -10.0 * (p - xm(p, xq[0], 1))
        dv = -10.0 * (yp(p, yq[1], 1) - p)
        dvm = -10.0 * (p - ym(p, yq[0], 1))
        dw = masked(-10.0 * (p0[4 + k] - p), lid)
        dwm = winc[k]
        up = masked(0.25 * (c0[3 + k] + c0[4 + k]), lid)
        upm = lift[k]
        a = q - 10.0 * ((u - um) + (v - vm) + (w - wm))
        b = -10.0 * ((du - dum) + (dv - dvm) + ((dw + up) - (dwm + upm)))
        ta[k], aa[k], ba[k] = t, a, b
        uinc[k], vinc[k], winc[1 + k], lift[1 + k] = du, dv, dw, up
        um0[k], vm0[k], uminc[k], vminc[k] = um, vm, dum, dvm
        x_pack(state, 1, g, kk, t, a, None, b)
        for i, value in enumerate((a, b)):
            y_pack3(state, i, Y_AT[1] + 6 * i, g, kk, value)
        y_pack3(state, "t", Y_AT[6], g, kk, t)

    by_level(build)
    for i, a in enumerate((ta, aa, ba)):
        for n in range(3):
            sz[0, Z_AT[1] + 3 * i + n] = a[13 + n]
            sz[1, Z_AT[1] + 3 * i + n] = a[n]
    round1 = send(1)

    droplets(1)

    round6 = send(6)

    whole(m2r, 1).wait_recv()
    top = m2s[...]
    for o in range(len(group2)):
        top = jnp.maximum(top, m2r[o])
    top = jnp.broadcast_to(jnp.max(top, axis=1, keepdims=True), (1, 128))
    time_step = jnp.broadcast_to(0.6 / (1.0 + top), (8, 128))

    arrive(round1)
    t1 = time_step * F32(1.0 / 3.0)
    slot = lax.rem(lane, 16)
    for d in range(2):
        for g in range(2):
            third = jnp.where((slot >= 3) & (slot < 6), roll_l(rx[1, d, g], -5), 0.0)
            hx[d, g] = rx[0, d, g] + t1 * (rx[1, d, g] + t1 * third)
        for n in range(6):
            hy[d, 6 + n] = ry[d, 6 + n] + t1 * (ry[d, 14 + n] + t1 * ry[d, 20 + n])

    def section1(g, kk, k, state):
        cq[3 + k] = c0[3 + k] + t1 * ta[k]
        pq[3 + k] = p0[3 + k] + t1 * (aa[k] + t1 * ba[k])
        uf[k] = fields[2, k] + t1 * uinc[k]
        vf[k] = fields[3, k] + t1 * vinc[k]
        umf[k] = um0[k] + t1 * uminc[k]
        vmf[k] = vm0[k] + t1 * vminc[k]
        wf[1 + k] = w0[1 + k] + t1 * (winc[1 + k] + lift[1 + k])

    by_level(section1)
    wf[0] = w0[0] + t1 * (winc[0] + lift[0])
    for n in range(3):
        for d, to, keep in ((0, n, klo), (1, 19 + n, khi)):
            cq[to] = c0[to] + (t1 * keep) * rz[d, Z_AT[1] + n]
            pq[to] = p0[to] + (t1 * keep) * (rz[d, Z_AT[1] + 3 + n] + t1 * rz[d, Z_AT[1] + 6 + n])

    def tracer_rates(mx, my, start, old, finish):
        u, v, um, vm, w = old

        def step(g, kk, k, state):
            winds = (u[k], um[k], v[k], vm[k], w[1 + k], w[k])
            finish(g, kk, k, state, advect(cq, k, x_halo(mx, 0, g, kk), y_halo3(my, start, g, kk), winds))

        by_level(step)

    def lifts():
        lift[0] = 0.25 * (cq[2] + cq[3]) * klo

        def step(g, kk, k, state):
            lift[1 + k] = masked(0.25 * (cq[3 + k] + cq[4 + k]), lid_at(g, kk))

        by_level(step)

    def narrow(r, g, kk, k, state, p):
        x_pack(state, r, g, kk, None, p)
        y_pack1(state, "p", Y_AT[r], g, kk, last=p, first=p)

    def narrow_send(r, p):
        sz[0, Z_AT[r]] = p[16]
        sz[1, Z_AT[r]] = p[1]
        return send(r)

    def first_substep(r, s, mx, my, start, old, new, rate_ref):
        u_, v_, um_, vm_, w_ = old
        un_, vn_, umn_, vmn_, wn_ = new
        wn_[0] = w0[0] + s * (winc[0] + lift[0])

        def step(g, kk, k, state):
            winds = (u_[k], um_[k], v_[k], vm_[k], w_[1 + k], w_[k])
            rate = advect(pq, k, x_halo(mx, 3, g, kk), y_halo3(my, start, g, kk), winds)
            rate_ref[k] = rate
            u = fields[2, k] + s * uinc[k]
            um = um0[k] + s * uminc[k]
            v = fields[3, k] + s * vinc[k]
            vm = vm0[k] + s * vminc[k]
            w = w0[1 + k] + s * (winc[1 + k] + lift[1 + k])
            wm = w0[k] + s * (winc[k] + lift[k])
            p = p0[3 + k] + s * (rate - 10.0 * ((u - um) + (v - vm) + (w - wm)))
            pf[1 + k], un_[k], vn_[k], umn_[k], vmn_[k], wn_[1 + k] = p, u, v, um, vm, w
            narrow(r, g, kk, k, state, p)

        by_level(step)
        return narrow_send(r, pf)

    def next_substep(r, made, s, ps, winds, rate_ref, finish):
        u_, v_, um_, vm_, w_ = winds
        s10 = s * 10.0
        arrive(made)
        ps[0] = rz[0, Z_AT[r]] * klo
        ps[17] = rz[1, Z_AT[r]] * khi
        w_[0] = w_[0] + s * lift[0] - (s10 * klo) * (ps[1] - ps[0])

        def step(g, kk, k, state):
            lid = lid_at(g, kk)
            xq = x_halo(rx.at[r], 3, g, kk)
            p = ps[1 + k]
            ylo, yhi = roll_s(ry[0, Y_AT[r] + g], 7 - kk), roll_s(ry[1, Y_AT[r] + g], -kk)
            u = u_[k] - s10 * (xp(p, xq[1], 1) - p)
            um = um_[k] - s10 * (p - xm(p, xq[0], 1))
            v = v_[k] - s10 * (yp(p, yhi, 1) - p)
            vm = vm_[k] - s10 * (p - ym(p, ylo, 1))
            w = w_[1 + k] + s * lift[1 + k] - masked(s10 * (ps[2 + k] - p), lid)
            wm = state["w"] if kk else w_[k]
            state["w"] = w
            pn = p + s * (rate_ref[k] - 10.0 * ((u - um) + (v - vm) + (w - wm)))
            finish(g, kk, k, state, pn, u, v, um, vm, w)

        by_level(step)

    state_f = (uf, vf, umf, vmf, wf)
    state_g = (ug, vg, umg, vmg, wg)

    t2 = time_step * F32(0.25)
    half = time_step * F32(0.5)
    lifts()
    round2 = first_substep(2, t2, hx, hy, 6, state_f, state_g, aa)

    def tracer2(g, kk, k, state, rate):
        c = c0[3 + k] + half * rate
        tr[k] = c
        x_pack(state, 7, g, kk, c)
        y_pack3(state, "c", Y_AT[7], g, kk, c)

    by_depth()
    arrive(round6)
    for d in range(2):
        for n in range(6):
            hy[d, n] = ry[d, n] + t1 * ry[d, Y_AT[6] + n]
    tracer_rates(hx, hy, 0, state_f, tracer2)
    for n in range(3):
        sz[0, Z_AT[7] + n] = tr[13 + n]
        sz[1, Z_AT[7] + n] = tr[n]
    round7 = send(7)

    def finish2(g, kk, k, state, p, u, v, um, vm, w):
        pq[3 + k] = p
        ug[k], vg[k], umg[k], vmg[k], wg[1 + k] = u, v, um, vm, w
        cq[3 + k] = tr[k]
        x_pack(state, 3, g, kk, None, p)
        y_pack3(state, "p", Y_AT[3], g, kk, p)

    next_substep(2, round2, t2, pf, state_g, aa, finish2)
    for n in range(3):
        sz[0, Z_AT[3] + n] = pq[16 + n]
        sz[1, Z_AT[3] + n] = pq[3 + n]
    round3 = send(3)

    arrive(round7)
    for n in range(3):
        for d, to, keep in ((0, n, klo), (1, 19 + n, khi)):
            cq[to] = rz[d, Z_AT[7] + n] * keep
    t3 = time_step * F32(0.25)
    s10 = t3 * 10.0
    alpha = s10 * s10
    lifts()

    def forcing(g, kk, k, state):
        value = (lift[1 + k] - lift[k]) * (-0.1 * alpha)
        ek[0, 3 + k] = value
        narrow(5, g, kk, k, state, value)

    by_level(forcing)
    sz[0, Z_AT[5]] = ek[0, 18]
    sz[1, Z_AT[5]] = ek[0, 3]
    round5 = send(5)

    def tracer3(g, kk, k, state, rate):
        c = c0[3 + k] + time_step * rate
        out[0, k] = c
        growth = jnp.minimum(jnp.exp(0.3 * c), F32(3.0e38))
        ta[k] = growth
        ba[k] = jnp.sqrt(growth)

    tracer_rates(rx.at[7], ry, Y_AT[7], state_g, tracer3)

    def landed(t):
        totals = [None, None, None]
        for k in range(max(t, 0), min(t + DEPTHS, L)):
            d = k - t
            grow, root = ta[k], ba[k]
            parts = (gmat[0, d, k], gmat[1, d, k] * grow, gmat[2, d, k] * grow * root)
            totals = [a if b is None else b + a for a, b in zip(parts, totals)]
        return totals

    for t in range(-8, 0):
        for m, value in enumerate(landed(t)):
            ext[m, t + 8] = value
    dropped = pltpu.make_async_remote_copy(
        src_ref=ext, dst_ref=fall, send_sem=fall_sem.at[0], recv_sem=fall_sem.at[1],
        device_id={"gz": near("gz", -1)}, device_id_type=MESH,
    )
    dropped.start()

    arrive(round3)
    for n in range(3):
        for d, to, keep in ((0, n, klo), (1, 19 + n, khi)):
            pq[to] = rz[d, Z_AT[3] + n] * keep

    wf[0] = w0[0] + t3 * (winc[0] + lift[0])

    def open3(g, kk, k, state):
        winds = (ug[k], umg[k], vg[k], vmg[k], wg[1 + k], wg[k])
        rate = advect(pq, k, x_halo(rx.at[3], 3, g, kk), y_halo3(ry, Y_AT[3], g, kk), winds)
        u = fields[2, k] + t3 * uinc[k]
        um = um0[k] + t3 * uminc[k]
        v = fields[3, k] + t3 * vinc[k]
        vm = vm0[k] + t3 * vminc[k]
        w = w0[1 + k] + t3 * (winc[1 + k] + lift[1 + k])
        wm = w0[k] + t3 * (winc[k] + lift[k])
        e = t3 * (rate - 10.0 * ((u - um) + (v - vm) + (w - wm)))
        p = p0[3 + k] + e
        e = e + ek[0, 3 + k]
        ep[0, 3 + k], eg[0, 3 + k] = p, e
        uf[k], vf[k], wf[1 + k] = u, v, w
        x_pack(state, 4, g, kk, p, e)
        y_pack3(state, "p", Y_AT[4], g, kk, p)
        y_pack2(state, "e", Y_AT[4] + 6, g, kk, e)

    by_level(open3)
    for n in range(3):
        sz[0, Z_AT[4] + n] = ep[0, 16 + n]
        sz[1, Z_AT[4] + n] = ep[0, 3 + n]
    for n in range(2):
        sz[0, Z_AT[4] + 3 + n] = eg[0, 17 + n]
        sz[1, Z_AT[4] + 3 + n] = eg[0, 3 + n]
    for d in range(2):
        syz[d, 0] = jnp.where(row < 2, roll_s(sy[d, Y_AT[4] + 9], 2), sy[d, Y_AT[4] + 5])
        syz[d, 1] = jnp.where(row < 6, sy[d, Y_AT[4]], roll_s(sy[d, Y_AT[4] + 6], 6))
        low, high = sx[4, d, 0], sx[4, d, 1]
        sxy[d, 0] = jnp.where(row < 4, roll_s(low, 3), roll_s(high, 7))
        sxy[d, 1] = jnp.where(row < 4, low, roll_s(high, 4))
        for c, tile in ((0, high), (1, low)):
            scorner[4 * d + c] = tile[7:8, :]
            scorner[4 * d + 2 + c] = tile[0:1, :]
    round4 = send(4)
    for i, (a, b, c) in enumerate(edges):
        if c is None:
            src, dst = sxy.at[a, b], rxy.at[a, b]
        elif b is None:
            src, dst = sx.at[4, a, 1 - c], rxz.at[a, c]
        elif a is None:
            src, dst = syz.at[b, c], ryz.at[b, c]
        else:
            src, dst = scorner.at[4 * a + 2 * b + c], rcorner.at[4 * a + 2 * b + c]
        corner = None not in (a, b, c)
        pltpu.make_async_remote_copy(
            src_ref=src, dst_ref=dst,
            send_sem=small_sem.at[4] if corner else send_sem.at[0],
            recv_sem=small_sem.at[5] if corner else recv_sem.at[4],
            device_id=edge_device((a, b, c)), device_id_type=MESH,
        ).start()
    for t in range(0, L):
        for m, value in enumerate(landed(t)):
            mom[m, t] = value

    def join_l(lo, hi):
        return jnp.where(lane < 64, hi, lo)

    def join_s(lo, hi):
        return jnp.where(row < 4, hi, lo)

    def x_one(tile, d, at, kk):
        return roll_l(tile, 125 - at - 16 * kk if d == 0 else -at - 16 * kk)

    arrive(round5)

    def assemble_forcing(g, kk, k, state):
        at = 3 + k
        ek[1, at] = join_s(roll_s(ry[0, Y_AT[5] + g], 7 - kk), roll_s(ry[1, Y_AT[5] + g], -kk))
        ek[2, at] = join_l(*x_halo(rx.at[5], 3, g, kk))

    by_level(assemble_forcing)
    ek[0, 2] = rz[0, Z_AT[5]]
    ek[0, 19] = rz[1, Z_AT[5]]
    dropped.wait_recv()
    for m in range(3):
        for n in range(8):
            mom[m, 8 + n] = mom[m, 8 + n] + fall[m, n] * khi

    arrive(round4)
    whole(rcorner, 2).wait_recv()

    for d in both:
        xy[d, 0, 0], xy[d, 0, 1] = roll_s(rxy[d, 0], 5), roll_s(rxy[d, 0], 1)
        xy[d, 1, 0], xy[d, 1, 1] = rxy[d, 1], roll_s(rxy[d, 1], 4)

    def assemble(g, kk, k, state):
        at = 3 + k
        ep[1, at] = join_s(*y_halo3(ry, Y_AT[4], g, kk))
        eg[1, at] = join_s(*y_halo2(ry, Y_AT[4] + 6, g, kk))
        for off, ref in ((0, ep), (3, eg)):
            ref[2, at] = join_l(*(x_one(rx[4, d, g], d, off, kk) for d in both))
            ref[3, at] = join_s(*(join_l(*(x_one(xy[d, b, g], d, off, kk) for d in both)) for b in both))

    by_level(assemble)
    for n in range(3):
        ep[0, n] = rz[0, Z_AT[4] + n]
        ep[0, 19 + n] = rz[1, Z_AT[4] + n]
    for n in range(2):
        eg[0, 1 + n] = rz[0, Z_AT[4] + 3 + n]
        eg[0, 19 + n] = rz[1, Z_AT[4] + 3 + n]
    for c, levels in ((0, ((1, 6), (2, 7))), (1, ((19, 0), (20, 1)))):
        for to, kk in levels:
            t, o = divmod(3 * kk, 8)
            ep[1, to] = join_s(roll_s(ryz[0, c], 5 - o), roll_s(ryz[1, c], -o))
            ep[2, to] = join_l(*(x_one(rxz[d, c], d, 0, kk) for d in both))
            if to in (2, 19):
                o = 0 if c == 0 else 6
                eg[1, to] = join_s(roll_s(ryz[0, c], 6 - o), roll_s(ryz[1, c], -o))
                eg[2, to] = join_l(*(x_one(rxz[d, c], d, 3, kk) for d in both))
                ends = [
                    join_l(*(x_one(jnp.broadcast_to(rcorner[4 * d + 2 * b + c], (8, 128)), d, 0, kk) for d in both))
                    for b in both
                ]
                ep[3, to] = join_s(*ends)

    other_x, other_y = (2, 3, 0, 1), (1, 0, 3, 2)

    def neighbours(ref, part, at):
        q, hx_, hy_ = ref[part, at], ref[other_x[part], at], ref[other_y[part], at]
        return q, xp(q, hx_, 1), xm(q, hx_, 1), yp(q, hy_, 1), ym(q, hy_, 1)

    def laplacian(ref, part, at, low=None, high=None):
        q, a, b, c, d = neighbours(ref, part, at)
        up, down = masked(ref[part, at + 1] - q, high), masked(q - ref[part, at - 1], low)
        return q, (a - q, c - q, up), ((a - q) - (q - b)) + ((c - q) - (q - d)) + (up - down)

    def edge_masks(at, g, kk):
        low = jnp.where(g == 0, klo, F32(1.0)) if kk == 0 else None
        return low, lid_at(g, kk)

    def winds3(k, steps):
        uf[k] = uf[k] - s10 * steps[0]
        vf[k] = vf[k] - s10 * steps[1]
        wf[1 + k] = wf[1 + k] + t3 * lift[1 + k] - s10 * steps[2]

    def second3(part, at, low=None, high=None):
        q, steps, lap = laplacian(ep, part, at, low, high)
        e = eg[part, at] + alpha * lap
        eg[part, at] = e
        en[part, at] = q + e
        return steps

    def two(g, kk, k, state):
        low, high = edge_masks(3 + k, g, kk)
        winds3(k, second3(0, 3 + k, low, high))
        for part in (1, 2, 3):
            second3(part, 3 + k, low, high)

    by_level(two)
    second3(0, 1)
    second3(0, 20)
    for part in (0, 1, 2):
        second3(part, 2, None, klo)
        second3(part, 19, khi, None)

    def third3(part, at, low=None, high=None):
        q, steps, lap = laplacian(en, part, at, low, high)
        e = eg[part, at] + ek[part, at] + alpha * lap
        eg[part, at] = e
        ep[part, at] = q + e
        return steps

    def three(g, kk, k, state):
        low, high = edge_masks(3 + k, g, kk)
        winds3(k, third3(0, 3 + k, low, high))
        for part in (1, 2):
            third3(part, 3 + k, low, high)

    by_level(three)
    third3(0, 2, None, klo)
    third3(0, 19, khi, None)

    def four(g, kk, k, state):
        low, high = edge_masks(3 + k, g, kk)
        q, steps, lap = laplacian(ep, 0, 3 + k, low, high)
        out[1, k] = q + (eg[0, 3 + k] + ek[0, 3 + k] + alpha * lap)
        out[2, k] = uf[k] - s10 * steps[0]
        out[3, k] = vf[k] - s10 * steps[1]
        out[4, k] = wf[1 + k] + t3 * lift[1 + k] - s10 * steps[2]

    by_level(four)

    dropped.wait_send()
    for i, ref in enumerate((m1r, m2r, rcorner)):
        whole(ref, i).wait_send()
    tiles(sum(sent), send_sem.at[0], recv_sem.at[0]).wait_send()


def solution(mesh):
    sizes = (mesh.shape["gx"], mesh.shape["gy"], mesh.shape["gz"])
    nx, ny, nz = sizes
    vm = lambda *shape: pltpu.VMEM(shape + (8, 128), F32)
    dma = pltpu.SemaphoreType.DMA
    scratch = [
        vm(5, L), pltpu.VMEM((128, 128), jnp.int32), pltpu.VMEM((8, 8, 16), jnp.int32),
        pltpu.VMEM((8 * PITCH, 128), F32), pltpu.VMEM((8 * PITCH, 128), F32), pltpu.VMEM((8 * PITCH, 128), jnp.int32),
        pltpu.VMEM((8, 8, 128), jnp.int32), pltpu.VMEM((128 * 24, 128), F32), vm(3, DEPTHS, L), vm(3, 8), vm(3, 8),
        vm(22), vm(22), vm(17), vm(22), vm(22), vm(2),
        vm(16), vm(16), vm(16), vm(16), vm(16), vm(17), vm(16), vm(16), vm(16), vm(16),
        vm(16), vm(17), vm(18), vm(16), vm(16), vm(16), vm(16), vm(17), vm(16), vm(16), vm(16), vm(16), vm(17),
        vm(2, 2), vm(2, 12), vm(4, 22), vm(4, 22), vm(4, 22), vm(4, 22),
        vm(8, 2, 2), vm(8, 2, 2), vm(2, Y_ALL), vm(2, Y_ALL), vm(2, Z_ALL), vm(2, Z_ALL),
        vm(2, 2), vm(2, 2), pltpu.VMEM((8, 1, 128), F32),
        vm(2, 2), vm(2, 2), vm(2, 2), pltpu.VMEM((8, 1, 128), F32), vm(2, 2, 2),
        pltpu.VMEM((1, 128), F32), pltpu.VMEM((2 * nx * nz - 1, 1, 128), F32),
        pltpu.VMEM((1, 128), F32), pltpu.VMEM((ny // 2 - 1, 1, 128), F32),
        dma((1,)), dma((8,)), dma((6,)), dma((2,)), dma((3,)), dma((3,)),
    ]
    vmem = pl.BlockSpec(memory_space=pltpu.VMEM)
    hbm = pl.BlockSpec(memory_space=pl.ANY)

    def per_device(fields, radius, weight, column, counts, fall_depth):
        held = pl.pallas_call(
            functools.partial(kernel, sizes),
            out_shape=(pltpu.VMEM((5, L, 8, 128), F32), pltpu.VMEM((3, L, 8, 128), F32)),
            in_specs=[hbm] * 6,
            out_specs=(vmem, vmem),
            scratch_shapes=scratch,
            compiler_params=pltpu.CompilerParams(collective_id=0, has_side_effects=True),
            name="slab_step",
        )(
            fields,
            counts.reshape(128, 128),
            jnp.transpose(fall_depth[:, :, :, 0], (0, 2, 1)),
            radius.reshape(1024, 128),
            weight.reshape(1024, 128),
            column.reshape(1024, 128),
        )
        return held

    cut = P(None, "gz", "gy", "gx")
    return jax.shard_map(
        per_device,
        mesh=mesh,
        in_specs=(cut, cut, cut, cut, P("gz", "gy", "gx"), cut),
        out_specs=(cut, cut),
        check_vma=False,
    )
```

```python
import functools

import jax
import jax.numpy as jnp
from jax import lax
from jax.experimental import pallas as pl
from jax.experimental.pallas import tpu as pltpu
from jax.sharding import PartitionSpec as P

MESH = pl.DeviceIdType.MESH
F32 = jnp.float32
L = 16
DEPTHS = 9
PITCH = 136
Y_TILES = {0: (14, 12), 1: (12, 12), 6: (6, 6), 7: (6, 6), 3: (6, 6), 2: (2, 2), 5: (2, 2), 4: (10, 10)}
Z_TILES = {0: (7, 6), 1: (9, 9), 7: (3, 3), 3: (3, 3), 2: (1, 1), 5: (1, 1), 4: (5, 5)}
Y_AT = {0: 0, 1: 14, 6: 26, 7: 32, 3: 38, 2: 44, 5: 46, 4: 48}
Z_AT = {0: 0, 1: 7, 7: 16, 3: 19, 2: 22, 5: 23, 4: 24}
Y_ALL, Z_ALL = 58, 29
SPLITS = (0, 72, 128)
ROWS = 4


def kernel(
    sizes,
    fields_h, counts_h, depth_h, rad_h, wgt_h, col_h,
    out, mom,
    fields, counts, depth_in, rad, wgt, col, dep, dmat, gmat, ext, fall,
    c0, p0, w0, cq, pq, peak,
    ta, aa, ba, uinc, vinc, winc, um0, vm0, uminc, vminc,
    tr, lift, pf, uf, vf, umf, vmf, wf, ug, vg, umg, vmg, wg,
    hx, hy, ep, eg, ek, en,
    sx, rx, sy, ry, sz, rz, syz, sxy, scorner, rxy, rxz, ryz, rcorner, xy,
    m1s, m1r, m2s, m2r,
    send_sem, recv_sem, small_sem, fall_sem, load_sem, field_sem,
):
    nx, ny, nz = sizes
    ix, iy, iz = lax.axis_index("gx"), lax.axis_index("gy"), lax.axis_index("gz")

    def near(axis, step):
        i, n = {"gx": (ix, nx), "gy": (iy, ny), "gz": (iz, nz)}[axis]
        return lax.rem(i + (step + n), n)

    early = [
        pltpu.make_async_copy(src, dst, field_sem.at[n])
        for n, (src, dst) in enumerate(((fields_h, fields), (counts_h, counts), (depth_h, depth_in)))
    ]
    loads = []
    for a, (src, dst) in enumerate(((rad_h, rad), (wgt_h, wgt), (col_h, col))):
        for s in range(8):
            loads.append(
                pltpu.make_async_copy(
                    src.at[pl.ds(s * 128, 128)], dst.at[pl.ds(s * PITCH, 128)], load_sem.at[a]
                )
            )
    for n in range(5):
        pltpu.make_async_copy(fields_h.at[n], fields.at[n], field_sem.at[0]).start()
    for c in early[1:]:
        c.start()

    def device(a=0, b=0, c=0):
        return {"gx": near("gx", a), "gy": near("gy", b), "gz": near("gz", c)}

    flip = 1 - 2 * lax.rem(iy, 2)
    group1 = [(a, f, b) for a in range(nx) for f in range(2) for b in range(nz) if (a, f, b) != (0, 0, 0)]
    group2 = [2 * n for n in range(1, ny // 2)]
    both = (0, 1)
    edges = [(a, b, None) for a in both for b in both]
    edges += [(a, None, c) for a in both for c in both]
    edges += [(None, b, c) for b in both for c in both]
    edges += [(a, b, c) for a in both for b in both for c in both]

    def edge_device(edge):
        return device(*(0 if d is None else 1 - 2 * d for d in edge))

    partners = [device(a, f * flip, b) for a, f, b in group1] + [device(0, a) for a in group2]
    partners += [device(0, 1), device(0, -1)] + [edge_device(e) for e in edges if e[1] is not None]
    barrier = pltpu.get_barrier_semaphore()
    for partner in reversed(partners):
        pl.semaphore_signal(barrier, inc=1, device_id=partner, device_id_type=MESH)

    lane = lax.broadcasted_iota(jnp.int32, (8, 128), 1)
    row = lax.broadcasted_iota(jnp.int32, (8, 128), 0)
    klo = (iz > 0).astype(F32)
    khi = (iz < nz - 1).astype(F32)
    zero = jnp.zeros((8, 128), F32)

    def roll_l(x, s):
        s = s % 128
        return pltpu.roll(x, s, 1) if s else x

    def roll_s(x, s):
        s = s % 8
        return pltpu.roll(x, s, 0) if s else x

    def xp(q, h, n):
        return roll_l(jnp.where(lane < n, h, q), -n)

    def xm(q, h, n):
        return roll_l(jnp.where(lane >= 128 - n, h, q), n)

    def yp(q, h, n):
        return roll_s(jnp.where(row < n, h, q), -n)

    def ym(q, h, n):
        return roll_s(jnp.where(row >= 8 - n, h, q), n)

    def put_l(message, value, at, width):
        return jnp.where((lane >= at) & (lane < at + width), value, message)

    def by_level(fn):
        def group(g, carry):
            state = {}
            for kk in range(8):
                fn(g, kk, g * 8 + kk, state)
            return carry

        lax.fori_loop(0, 2, group, 0)

    def copies(r):
        made = []
        for d, step in ((0, 1), (1, -1)):
            y = pl.ds(Y_AT[r], Y_TILES[r][d])
            parts = [(sy.at[d, y], ry.at[d, y], "gy")]
            if r in Z_TILES:
                z = pl.ds(Z_AT[r], Z_TILES[r][d])
                parts += [(sz.at[d, z], rz.at[d, z], "gz"), (sx.at[r, d], rx.at[r, d], "gx")]
            for i, (src, dst, axis) in enumerate(parts):
                made.append(
                    pltpu.make_async_remote_copy(
                        src_ref=src, dst_ref=dst,
                        send_sem=send_sem.at[0], recv_sem=recv_sem.at[r],
                        device_id={axis: near(axis, step)}, device_id_type=MESH,
                    )
                )
        return made

    def send(r):
        for c in copies(r):
            c.start()
        n = sum(Y_TILES[r]) + (sum(Z_TILES[r]) + 4 if r in Z_TILES else 0) + (12 if r == 4 else 0)
        sent.append(n)
        return r, n

    sent = []

    def tiles(n, send, recv):
        span = dmat.at[pl.ds(0, 8 * n)]
        return pltpu.make_async_remote_copy(
            src_ref=span, dst_ref=span, send_sem=send, recv_sem=recv, device_id=device(1), device_id_type=MESH
        )

    def arrive(made):
        r, n = made
        tiles(n, send_sem.at[0], recv_sem.at[r]).wait_recv()

    def x_pack(state, r, g, kk, a=None, b=None, wind=None, third=None):
        base = 16 * kk
        lo, hi = state.get("xlo", zero), state.get("xhi", zero)
        for value, at in ((a, 0), (b, 3), (third, 8)):
            if value is not None:
                lo = put_l(lo, roll_l(value, base + at + 3), base + at, 3)
                hi = put_l(hi, roll_l(value, base + at), base + at, 3)
        if wind is not None:
            lo = put_l(lo, roll_l(wind, base + 7), base + 6, 1)
        state["xlo"], state["xhi"] = lo, hi
        if kk == 7:
            sx[r, 0, g] = lo
            sx[r, 1, g] = hi

    def y_pack3(state, name, start, g, kk, q):
        t, o = divmod(3 * kk, 8)
        for d, moved in ((0, roll_s(q, o - 5)), (1, roll_s(q, o))):
            key = (name, d)
            tiles = state.setdefault(key, [None, None, None])
            if tiles[t] is None:
                tiles[t] = moved
            else:
                tiles[t] = jnp.where(row >= o, moved, tiles[t])
            if o > 5:
                tiles[t + 1] = moved
            if o >= 5:
                sy[d, start + g * 3 + t] = tiles[t]

    def y_halo3(ref, start, g, kk):
        t, o = divmod(3 * kk, 8)
        got = []
        for d in range(2):
            value = ref[d, start + g * 3 + t]
            if o > 5:
                value = jnp.where(row >= o, value, ref[d, start + g * 3 + t + 1])
            got.append(roll_s(value, 5 - o if d == 0 else -o))
        return got

    def y_pack1(state, name, start, g, kk, last=None, first=None):
        for d, value, by in ((0, last, kk - 7), (1, first, kk)):
            if value is not None:
                key = (name, d)
                moved = roll_s(value, by)
                state[key] = moved if kk == 0 else jnp.where(row >= kk, moved, state[key])
                if kk == 7:
                    sy[d, start + g] = state[key]

    def y_pack2(state, name, start, g, kk, q):
        t, o = divmod(2 * kk, 8)
        for d, by in ((0, o - 6), (1, o)):
            key = (name, d)
            moved = roll_s(q, by)
            state[key] = moved if o == 0 else jnp.where(row >= o, moved, state[key])
            if o == 6:
                sy[d, start + g * 2 + t] = state[key]

    def y_halo2(ref, start, g, kk):
        t, o = divmod(2 * kk, 8)
        return [roll_s(ref[d, start + g * 2 + t], 6 - o if d == 0 else -o) for d in range(2)]

    def x_halos(mx, g, kk):
        lo, hi = mx[0, g], mx[1, g]
        base = 16 * kk
        return (roll_l(lo, 125 - base), roll_l(hi, -base)), (roll_l(lo, 122 - base), roll_l(hi, -base - 3)), roll_l(lo, 121 - base)

    def x_halo(ref, at, g, kk):
        base = 16 * kk + at
        return roll_l(ref[0, g], 125 - base), roll_l(ref[1, g], -base)

    def lid_at(g, kk):
        return jnp.where(g == 1, khi, F32(1.0)) if kk == 7 else None

    def masked(value, mask):
        return value if mask is None else value * mask

    early[0].wait()
    for c in loads:
        c.start()

    def prepare(g, kk, k, state):
        c, p, u, v = fields[0, k], fields[1, k], fields[2, k], fields[3, k]
        w = masked(fields[4, k], lid_at(g, kk))
        c0[3 + k] = c
        p0[3 + k] = p
        w0[1 + k] = w
        speed = jnp.abs(u) + jnp.abs(v) + jnp.abs(w)
        state["m"] = speed if kk == 0 else jnp.maximum(state["m"], speed)
        x_pack(state, 0, g, kk, c, p, u)
        y_pack3(state, "c", Y_AT[0], g, kk, c)
        y_pack3(state, "p", Y_AT[0] + 6, g, kk, p)
        y_pack1(state, "v", Y_AT[0] + 12, g, kk, last=v)
        if kk == 7:
            peak[g] = state["m"]

    by_level(prepare)
    for n in range(3):
        sz[0, Z_AT[0] + n] = fields[0, 13 + n]
        sz[0, Z_AT[0] + 3 + n] = fields[1, 13 + n]
        sz[1, Z_AT[0] + n] = fields[0, n]
        sz[1, Z_AT[0] + 3 + n] = fields[1, n]
    sz[0, Z_AT[0] + 6] = w0[16]
    m1s[...] = jnp.max(jnp.maximum(peak[0], peak[1]), axis=0, keepdims=True)

    target = lax.broadcasted_iota(jnp.int32, (128, 128), 0).astype(F32).astype(jnp.bfloat16)
    row16 = lax.rem(lax.broadcasted_iota(jnp.int32, (16, 128), 0), 8)

    def deposit_row(kj):
        r = rad[pl.ds(kj, 8, stride=PITCH), :]
        w = wgt[pl.ds(kj, 8, stride=PITCH), :]
        c = col[pl.ds(kj, 8, stride=PITCH), :].astype(F32)
        live = row < counts[pl.ds(kj, 1), :]
        number = jnp.where(live, w, 0.0)
        area = number * (r * r)
        mass = area * r
        lhs = []
        for q in (number, area, mass):
            top = q.astype(jnp.bfloat16).astype(F32)
            pair = jnp.concatenate([top, q - top], axis=0)
            lhs.append(
                jnp.concatenate(
                    [jnp.where(row16 == s, pair, 0.0).astype(jnp.bfloat16) for s in range(8)], axis=1
                )
            )
        lhs = jnp.concatenate(lhs, axis=0)
        hot = jnp.concatenate(
            [
                jnp.where(
                    jnp.broadcast_to(c[s : s + 1, :], (128, 128)).astype(jnp.bfloat16) == target,
                    jnp.bfloat16(1.0), jnp.bfloat16(0.0),
                ).astype(jnp.float8_e4m3fn)
                for s in range(8)
            ],
            axis=1,
        )
        got = lax.dot_general(lhs, hot, (((1,), (1,)), ((), ())), preferred_element_type=F32)
        for m in range(3):
            dmat[pl.ds(pl.multiple_of(kj * 24 + 8 * m, 8), 8), :] = got[16 * m : 16 * m + 8] + got[16 * m + 8 : 16 * m + 16]

    def droplets(part):
        def step(i, carry):
            for n in range(ROWS):
                deposit_row(i * ROWS + n)
            return carry

        lax.fori_loop(SPLITS[part] // ROWS, SPLITS[part + 1] // ROWS, step, 0)

    def by_depth():
        def level(k):
            deep = []
            for s in range(8):
                moved = pltpu.roll(dep[s], lax.rem(128 - k, 128), 1)
                deep.append(jnp.broadcast_to(moved[:, 0:1], (8, 128)))
            for m in range(3):
                got = [dmat[pl.ds(k * 192 + 8 * m + s, 8, stride=24), :] for s in range(8)]
                for d in range(DEPTHS):
                    total = jnp.where(deep[0] == d, got[0], 0.0)
                    for s in range(1, 8):
                        total = total + jnp.where(deep[s] == d, got[s], 0.0)
                    gmat[m, d, k] = total

        def step(i, carry):
            level(2 * i)
            level(2 * i + 1)
            return carry

        lax.fori_loop(0, L // 2, step, 0)

    pl.semaphore_wait(barrier, len(partners))

    def whole(ref, i):
        return pltpu.make_async_remote_copy(
            src_ref=ref, dst_ref=ref, send_sem=small_sem.at[2 * i], recv_sem=small_sem.at[2 * i + 1],
            device_id=device(1), device_id_type=MESH,
        )

    first = []
    for o, (a, f, b) in enumerate(group1):
        first.append(
            pltpu.make_async_remote_copy(
                src_ref=m1s, dst_ref=m1r.at[o], send_sem=small_sem.at[0], recv_sem=small_sem.at[1],
                device_id=device(a, f * flip, b), device_id_type=MESH,
            )
        )
    for c in first:
        c.start()
    round0 = send(0)
    for c in early[1:]:
        c.wait()
    for a, (src, dst) in enumerate(((rad_h, rad), (wgt_h, wgt), (col_h, col))):
        pltpu.make_async_copy(src, dst.at[pl.ds(0, 1024)], load_sem.at[a]).wait()
    dep[...] = jnp.zeros_like(dep)
    dep[:, :, 0:16] = depth_in[...]
    droplets(0)

    def flux(a, q):
        central = 37.0 * (q[2] + q[3]) - 8.0 * (q[1] + q[4]) + (q[0] + q[5])
        upwind = 10.0 * (q[3] - q[2]) - 5.0 * (q[4] - q[1]) + (q[5] - q[0])
        return a * central - jnp.abs(a) * upwind

    def advect(q, k, xh, yh, winds):
        own = q[3 + k]
        u, um, v, vm, w, wm = winds
        line = [xm(own, xh[0], 3), xm(own, xh[0], 2), xm(own, xh[0], 1), own,
                xp(own, xh[1], 1), xp(own, xh[1], 2), xp(own, xh[1], 3)]
        total = flux(u, line[1:]) - flux(um, line[:-1])
        line = [ym(own, yh[0], 3), ym(own, yh[0], 2), ym(own, yh[0], 1), own,
                yp(own, yh[1], 1), yp(own, yh[1], 2), yp(own, yh[1], 3)]
        total = total + (flux(v, line[1:]) - flux(vm, line[:-1]))
        line = [q[k + n] for n in range(7)]
        total = total + (flux(w, line[1:]) - flux(wm, line[:-1]))
        return total * F32(-1.0 / 60.0)

    whole(m1r, 0).wait_recv()
    top = m1s[...]
    for o in range(len(group1)):
        top = jnp.maximum(top, m1r[o])
    m2s[...] = top
    second = []
    for o, a in enumerate(group2):
        second.append(
            pltpu.make_async_remote_copy(
                src_ref=m2s, dst_ref=m2r.at[o], send_sem=small_sem.at[2], recv_sem=small_sem.at[3],
                device_id=device(0, a), device_id_type=MESH,
            )
        )
    for c in second:
        c.start()

    arrive(round0)
    for n in range(3):
        for d, to, keep in ((0, n, klo), (1, 19 + n, khi)):
            c0[to] = rz[d, Z_AT[0] + n] * keep
            p0[to] = rz[d, Z_AT[0] + 3 + n] * keep
    w0[0] = rz[0, Z_AT[0] + 6] * klo
    winc[0] = -10.0 * (p0[3] - p0[2]) * klo
    lift[0] = 0.25 * (c0[2] + c0[3]) * klo

    def build(g, kk, k, state):
        lid = lid_at(g, kk)
        xc, xq, xu = x_halos(rx.at[0], g, kk)
        yc = y_halo3(ry, Y_AT[0], g, kk)
        yq = y_halo3(ry, Y_AT[0] + 6, g, kk)
        yv = roll_s(ry[0, Y_AT[0] + 12 + g], 7 - kk)
        p, u, v = p0[3 + k], fields[2, k], fields[3, k]
        w, wm = w0[1 + k], w0[k]
        um, vm = xm(u, xu, 1), ym(v, yv, 1)
        winds = (u, um, v, vm, w, wm)
        t = advect(c0, k, xc, yc, winds)
        q = advect(p0, k, xq, yq, winds)
        du = -10.0 * (xp(p, xq[1], 1) - p)
        dum = -10.0 * (p - xm(p, xq[0], 1))
        dv = -10.0 * (yp(p, yq[1], 1) - p)
        dvm = -10.0 * (p - ym(p, yq[0], 1))
        dw = masked(-10.0 * (p0[4 + k] - p), lid)
        dwm = winc[k]
        up = masked(0.25 * (c0[3 + k] + c0[4 + k]), lid)
        upm = lift[k]
        a = q - 10.0 * ((u - um) + (v - vm) + (w - wm))
        b = -10.0 * ((du - dum) + (dv - dvm) + ((dw + up) - (dwm + upm)))
        ta[k], aa[k], ba[k] = t, a, b
        uinc[k], vinc[k], winc[1 + k], lift[1 + k] = du, dv, dw, up
        um0[k], vm0[k], uminc[k], vminc[k] = um, vm, dum, dvm
        x_pack(state, 1, g, kk, t, a, None, b)
        for i, value in enumerate((a, b)):
            y_pack3(state, i, Y_AT[1] + 6 * i, g, kk, value)
        y_pack3(state, "t", Y_AT[6], g, kk, t)

    by_level(build)
    for i, a in enumerate((ta, aa, ba)):
        for n in range(3):
            sz[0, Z_AT[1] + 3 * i + n] = a[13 + n]
            sz[1, Z_AT[1] + 3 * i + n] = a[n]
    round1 = send(1)

    droplets(1)

    round6 = send(6)

    whole(m2r, 1).wait_recv()
    top = m2s[...]
    for o in range(len(group2)):
        top = jnp.maximum(top, m2r[o])
    top = jnp.broadcast_to(jnp.max(top, axis=1, keepdims=True), (1, 128))
    time_step = jnp.broadcast_to(0.6 / (1.0 + top), (8, 128))

    arrive(round1)
    t1 = time_step * F32(1.0 / 3.0)
    slot = lax.rem(lane, 16)
    for d in range(2):
        for g in range(2):
            third = jnp.where((slot >= 3) & (slot < 6), roll_l(rx[1, d, g], -5), 0.0)
            hx[d, g] = rx[0, d, g] + t1 * (rx[1, d, g] + t1 * third)
        for n in range(6):
            hy[d, 6 + n] = ry[d, 6 + n] + t1 * (ry[d, 14 + n] + t1 * ry[d, 20 + n])

    def section1(g, kk, k, state):
        cq[3 + k] = c0[3 + k] + t1 * ta[k]
        pq[3 + k] = p0[3 + k] + t1 * (aa[k] + t1 * ba[k])
        uf[k] = fields[2, k] + t1 * uinc[k]
        vf[k] = fields[3, k] + t1 * vinc[k]
        umf[k] = um0[k] + t1 * uminc[k]
        vmf[k] = vm0[k] + t1 * vminc[k]
        wf[1 + k] = w0[1 + k] + t1 * (winc[1 + k] + lift[1 + k])

    by_level(section1)
    wf[0] = w0[0] + t1 * (winc[0] + lift[0])
    for n in range(3):
        for d, to, keep in ((0, n, klo), (1, 19 + n, khi)):
            cq[to] = c0[to] + (t1 * keep) * rz[d, Z_AT[1] + n]
            pq[to] = p0[to] + (t1 * keep) * (rz[d, Z_AT[1] + 3 + n] + t1 * rz[d, Z_AT[1] + 6 + n])

    def tracer_rates(mx, my, start, old, finish):
        u, v, um, vm, w = old

        def step(g, kk, k, state):
            winds = (u[k], um[k], v[k], vm[k], w[1 + k], w[k])
            finish(g, kk, k, state, advect(cq, k, x_halo(mx, 0, g, kk), y_halo3(my, start, g, kk), winds))

        by_level(step)

    def lifts():
        lift[0] = 0.25 * (cq[2] + cq[3]) * klo

        def step(g, kk, k, state):
            lift[1 + k] = masked(0.25 * (cq[3 + k] + cq[4 + k]), lid_at(g, kk))

        by_level(step)

    def narrow(r, g, kk, k, state, p):
        x_pack(state, r, g, kk, None, p)
        y_pack1(state, "p", Y_AT[r], g, kk, last=p, first=p)

    def narrow_send(r, p):
        sz[0, Z_AT[r]] = p[16]
        sz[1, Z_AT[r]] = p[1]
        return send(r)

    def first_substep(r, s, mx, my, start, old, new, rate_ref):
        u_, v_, um_, vm_, w_ = old
        un_, vn_, umn_, vmn_, wn_ = new
        wn_[0] = w0[0] + s * (winc[0] + lift[0])

        def step(g, kk, k, state):
            winds = (u_[k], um_[k], v_[k], vm_[k], w_[1 + k], w_[k])
            rate = advect(pq, k, x_halo(mx, 3, g, kk), y_halo3(my, start, g, kk), winds)
            rate_ref[k] = rate
            u = fields[2, k] + s * uinc[k]
            um = um0[k] + s * uminc[k]
            v = fields[3, k] + s * vinc[k]
            vm = vm0[k] + s * vminc[k]
            w = w0[1 + k] + s * (winc[1 + k] + lift[1 + k])
            wm = w0[k] + s * (winc[k] + lift[k])
            p = p0[3 + k] + s * (rate - 10.0 * ((u - um) + (v - vm) + (w - wm)))
            pf[1 + k], un_[k], vn_[k], umn_[k], vmn_[k], wn_[1 + k] = p, u, v, um, vm, w
            narrow(r, g, kk, k, state, p)

        by_level(step)
        return narrow_send(r, pf)

    def next_substep(r, made, s, ps, winds, rate_ref, finish):
        u_, v_, um_, vm_, w_ = winds
        s10 = s * 10.0
        arrive(made)
        ps[0] = rz[0, Z_AT[r]] * klo
        ps[17] = rz[1, Z_AT[r]] * khi
        w_[0] = w_[0] + s * lift[0] - (s10 * klo) * (ps[1] - ps[0])

        def step(g, kk, k, state):
            lid = lid_at(g, kk)
            xq = x_halo(rx.at[r], 3, g, kk)
            p = ps[1 + k]
            ylo, yhi = roll_s(ry[0, Y_AT[r] + g], 7 - kk), roll_s(ry[1, Y_AT[r] + g], -kk)
            u = u_[k] - s10 * (xp(p, xq[1], 1) - p)
            um = um_[k] - s10 * (p - xm(p, xq[0], 1))
            v = v_[k] - s10 * (yp(p, yhi, 1) - p)
            vm = vm_[k] - s10 * (p - ym(p, ylo, 1))
            w = w_[1 + k] + s * lift[1 + k] - masked(s10 * (ps[2 + k] - p), lid)
            wm = state["w"] if kk else w_[k]
            state["w"] = w
            pn = p + s * (rate_ref[k] - 10.0 * ((u - um) + (v - vm) + (w - wm)))
            finish(g, kk, k, state, pn, u, v, um, vm, w)

        by_level(step)

    state_f = (uf, vf, umf, vmf, wf)
    state_g = (ug, vg, umg, vmg, wg)

    t2 = time_step * F32(0.25)
    half = time_step * F32(0.5)
    lifts()
    round2 = first_substep(2, t2, hx, hy, 6, state_f, state_g, aa)

    def tracer2(g, kk, k, state, rate):
        c = c0[3 + k] + half * rate
        tr[k] = c
        x_pack(state, 7, g, kk, c)
        y_pack3(state, "c", Y_AT[7], g, kk, c)

    by_depth()
    arrive(round6)
    for d in range(2):
        for n in range(6):
            hy[d, n] = ry[d, n] + t1 * ry[d, Y_AT[6] + n]
    tracer_rates(hx, hy, 0, state_f, tracer2)
    for n in range(3):
        sz[0, Z_AT[7] + n] = tr[13 + n]
        sz[1, Z_AT[7] + n] = tr[n]
    round7 = send(7)

    def finish2(g, kk, k, state, p, u, v, um, vm, w):
        pq[3 + k] = p
        ug[k], vg[k], umg[k], vmg[k], wg[1 + k] = u, v, um, vm, w
        cq[3 + k] = tr[k]
        x_pack(state, 3, g, kk, None, p)
        y_pack3(state, "p", Y_AT[3], g, kk, p)

    next_substep(2, round2, t2, pf, state_g, aa, finish2)
    for n in range(3):
        sz[0, Z_AT[3] + n] = pq[16 + n]
        sz[1, Z_AT[3] + n] = pq[3 + n]
    round3 = send(3)

    arrive(round7)
    for n in range(3):
        for d, to, keep in ((0, n, klo), (1, 19 + n, khi)):
            cq[to] = rz[d, Z_AT[7] + n] * keep
    t3 = time_step * F32(0.25)
    s10 = t3 * 10.0
    alpha = s10 * s10
    lifts()

    def forcing(g, kk, k, state):
        value = (lift[1 + k] - lift[k]) * (-0.1 * alpha)
        ek[0, 3 + k] = value
        narrow(5, g, kk, k, state, value)

    by_level(forcing)
    sz[0, Z_AT[5]] = ek[0, 18]
    sz[1, Z_AT[5]] = ek[0, 3]
    round5 = send(5)

    def tracer3(g, kk, k, state, rate):
        c = c0[3 + k] + time_step * rate
        out[0, k] = c
        growth = jnp.minimum(jnp.exp(0.3 * c), F32(3.0e38))
        ta[k] = growth
        ba[k] = jnp.sqrt(growth)

    tracer_rates(rx.at[7], ry, Y_AT[7], state_g, tracer3)

    def landed(t):
        totals = [None, None, None]
        for k in range(max(t, 0), min(t + DEPTHS, L)):
            d = k - t
            grow, root = ta[k], ba[k]
            parts = (gmat[0, d, k], gmat[1, d, k] * grow, gmat[2, d, k] * grow * root)
            totals = [a if b is None else b + a for a, b in zip(parts, totals)]
        return totals

    for t in range(-8, 0):
        for m, value in enumerate(landed(t)):
            ext[m, t + 8] = value
    dropped = pltpu.make_async_remote_copy(
        src_ref=ext, dst_ref=fall, send_sem=fall_sem.at[0], recv_sem=fall_sem.at[1],
        device_id={"gz": near("gz", -1)}, device_id_type=MESH,
    )
    dropped.start()

    arrive(round3)
    for n in range(3):
        for d, to, keep in ((0, n, klo), (1, 19 + n, khi)):
            pq[to] = rz[d, Z_AT[3] + n] * keep

    wf[0] = w0[0] + t3 * (winc[0] + lift[0])

    def open3(g, kk, k, state):
        winds = (ug[k], umg[k], vg[k], vmg[k], wg[1 + k], wg[k])
        rate = advect(pq, k, x_halo(rx.at[3], 3, g, kk), y_halo3(ry, Y_AT[3], g, kk), winds)
        u = fields[2, k] + t3 * uinc[k]
        um = um0[k] + t3 * uminc[k]
        v = fields[3, k] + t3 * vinc[k]
        vm = vm0[k] + t3 * vminc[k]
        w = w0[1 + k] + t3 * (winc[1 + k] + lift[1 + k])
        wm = w0[k] + t3 * (winc[k] + lift[k])
        e = t3 * (rate - 10.0 * ((u - um) + (v - vm) + (w - wm)))
        p = p0[3 + k] + e
        e = e + ek[0, 3 + k]
        ep[0, 3 + k], eg[0, 3 + k] = p, e
        uf[k], vf[k], wf[1 + k] = u, v, w
        x_pack(state, 4, g, kk, p, e)
        y_pack3(state, "p", Y_AT[4], g, kk, p)
        y_pack2(state, "e", Y_AT[4] + 6, g, kk, e)

    by_level(open3)
    for n in range(3):
        sz[0, Z_AT[4] + n] = ep[0, 16 + n]
        sz[1, Z_AT[4] + n] = ep[0, 3 + n]
    for n in range(2):
        sz[0, Z_AT[4] + 3 + n] = eg[0, 17 + n]
        sz[1, Z_AT[4] + 3 + n] = eg[0, 3 + n]
    for d in range(2):
        syz[d, 0] = jnp.where(row < 2, roll_s(sy[d, Y_AT[4] + 9], 2), sy[d, Y_AT[4] + 5])
        syz[d, 1] = jnp.where(row < 6, sy[d, Y_AT[4]], roll_s(sy[d, Y_AT[4] + 6], 6))
        low, high = sx[4, d, 0], sx[4, d, 1]
        sxy[d, 0] = jnp.where(row < 4, roll_s(low, 3), roll_s(high, 7))
        sxy[d, 1] = jnp.where(row < 4, low, roll_s(high, 4))
        for c, tile in ((0, high), (1, low)):
            scorner[4 * d + c] = tile[7:8, :]
            scorner[4 * d + 2 + c] = tile[0:1, :]
    for i, (a, b, c) in enumerate(edges):
        if c is None:
            src, dst = sxy.at[a, b], rxy.at[a, b]
        elif b is None:
            src, dst = sx.at[4, a, 1 - c], rxz.at[a, c]
        elif a is None:
            src, dst = syz.at[b, c], ryz.at[b, c]
        else:
            src, dst = scorner.at[4 * a + 2 * b + c], rcorner.at[4 * a + 2 * b + c]
        corner = None not in (a, b, c)
        pltpu.make_async_remote_copy(
            src_ref=src, dst_ref=dst,
            send_sem=small_sem.at[4] if corner else send_sem.at[0],
            recv_sem=small_sem.at[5] if corner else recv_sem.at[4],
            device_id=edge_device((a, b, c)), device_id_type=MESH,
        ).start()
    round4 = send(4)
    for t in range(0, L):
        for m, value in enumerate(landed(t)):
            mom[m, t] = value

    def join_l(lo, hi):
        return jnp.where(lane < 64, hi, lo)

    def join_s(lo, hi):
        return jnp.where(row < 4, hi, lo)

    def x_one(tile, d, at, kk):
        return roll_l(tile, 125 - at - 16 * kk if d == 0 else -at - 16 * kk)

    arrive(round5)

    def assemble_forcing(g, kk, k, state):
        at = 3 + k
        ek[1, at] = join_s(roll_s(ry[0, Y_AT[5] + g], 7 - kk), roll_s(ry[1, Y_AT[5] + g], -kk))
        ek[2, at] = join_l(*x_halo(rx.at[5], 3, g, kk))

    by_level(assemble_forcing)
    ek[0, 2] = rz[0, Z_AT[5]]
    ek[0, 19] = rz[1, Z_AT[5]]
    dropped.wait_recv()
    for m in range(3):
        for n in range(8):
            mom[m, 8 + n] = mom[m, 8 + n] + fall[m, n] * khi

    arrive(round4)
    whole(rcorner, 2).wait_recv()

    for d in both:
        xy[d, 0, 0], xy[d, 0, 1] = roll_s(rxy[d, 0], 5), roll_s(rxy[d, 0], 1)
        xy[d, 1, 0], xy[d, 1, 1] = rxy[d, 1], roll_s(rxy[d, 1], 4)

    def assemble(g, kk, k, state):
        at = 3 + k
        ep[1, at] = join_s(*y_halo3(ry, Y_AT[4], g, kk))
        eg[1, at] = join_s(*y_halo2(ry, Y_AT[4] + 6, g, kk))
        for off, ref in ((0, ep), (3, eg)):
            ref[2, at] = join_l(*(x_one(rx[4, d, g], d, off, kk) for d in both))
            ref[3, at] = join_s(*(join_l(*(x_one(xy[d, b, g], d, off, kk) for d in both)) for b in both))

    by_level(assemble)
    for n in range(3):
        ep[0, n] = rz[0, Z_AT[4] + n]
        ep[0, 19 + n] = rz[1, Z_AT[4] + n]
    for n in range(2):
        eg[0, 1 + n] = rz[0, Z_AT[4] + 3 + n]
        eg[0, 19 + n] = rz[1, Z_AT[4] + 3 + n]
    for c, levels in ((0, ((1, 6), (2, 7))), (1, ((19, 0), (20, 1)))):
        for to, kk in levels:
            t, o = divmod(3 * kk, 8)
            ep[1, to] = join_s(roll_s(ryz[0, c], 5 - o), roll_s(ryz[1, c], -o))
            ep[2, to] = join_l(*(x_one(rxz[d, c], d, 0, kk) for d in both))
            if to in (2, 19):
                o = 0 if c == 0 else 6
                eg[1, to] = join_s(roll_s(ryz[0, c], 6 - o), roll_s(ryz[1, c], -o))
                eg[2, to] = join_l(*(x_one(rxz[d, c], d, 3, kk) for d in both))
                ends = [
                    join_l(*(x_one(jnp.broadcast_to(rcorner[4 * d + 2 * b + c], (8, 128)), d, 0, kk) for d in both))
                    for b in both
                ]
                ep[3, to] = join_s(*ends)

    other_x, other_y = (2, 3, 0, 1), (1, 0, 3, 2)

    def neighbours(ref, part, at):
        q, hx_, hy_ = ref[part, at], ref[other_x[part], at], ref[other_y[part], at]
        return q, xp(q, hx_, 1), xm(q, hx_, 1), yp(q, hy_, 1), ym(q, hy_, 1)

    def laplacian(ref, part, at, low=None, high=None):
        q, a, b, c, d = neighbours(ref, part, at)
        up, down = masked(ref[part, at + 1] - q, high), masked(q - ref[part, at - 1], low)
        return q, (a - q, c - q, up), ((a - q) - (q - b)) + ((c - q) - (q - d)) + (up - down)

    def edge_masks(at, g, kk):
        low = jnp.where(g == 0, klo, F32(1.0)) if kk == 0 else None
        return low, lid_at(g, kk)

    def winds3(k, steps):
        uf[k] = uf[k] - s10 * steps[0]
        vf[k] = vf[k] - s10 * steps[1]
        wf[1 + k] = wf[1 + k] + t3 * lift[1 + k] - s10 * steps[2]

    def second3(part, at, low=None, high=None):
        q, steps, lap = laplacian(ep, part, at, low, high)
        e = eg[part, at] + alpha * lap
        eg[part, at] = e
        en[part, at] = q + e
        return steps

    def two(g, kk, k, state):
        low, high = edge_masks(3 + k, g, kk)
        winds3(k, second3(0, 3 + k, low, high))
        for part in (1, 2, 3):
            second3(part, 3 + k, low, high)

    by_level(two)
    second3(0, 1)
    second3(0, 20)
    for part in (0, 1, 2):
        second3(part, 2, None, klo)
        second3(part, 19, khi, None)

    def third3(part, at, low=None, high=None):
        q, steps, lap = laplacian(en, part, at, low, high)
        e = eg[part, at] + ek[part, at] + alpha * lap
        eg[part, at] = e
        ep[part, at] = q + e
        return steps

    def three(g, kk, k, state):
        low, high = edge_masks(3 + k, g, kk)
        winds3(k, third3(0, 3 + k, low, high))
        for part in (1, 2):
            third3(part, 3 + k, low, high)

    by_level(three)
    third3(0, 2, None, klo)
    third3(0, 19, khi, None)

    def four(g, kk, k, state):
        low, high = edge_masks(3 + k, g, kk)
        q, steps, lap = laplacian(ep, 0, 3 + k, low, high)
        out[1, k] = q + (eg[0, 3 + k] + ek[0, 3 + k] + alpha * lap)
        out[2, k] = uf[k] - s10 * steps[0]
        out[3, k] = vf[k] - s10 * steps[1]
        out[4, k] = wf[1 + k] + t3 * lift[1 + k] - s10 * steps[2]

    by_level(four)

    dropped.wait_send()
    for i, ref in enumerate((m1r, m2r, rcorner)):
        whole(ref, i).wait_send()
    tiles(sum(sent), send_sem.at[0], recv_sem.at[0]).wait_send()


def solution(mesh):
    sizes = (mesh.shape["gx"], mesh.shape["gy"], mesh.shape["gz"])
    nx, ny, nz = sizes
    vm = lambda *shape: pltpu.VMEM(shape + (8, 128), F32)
    dma = pltpu.SemaphoreType.DMA
    scratch = [
        vm(5, L), pltpu.VMEM((128, 128), jnp.int32), pltpu.VMEM((8, 8, 16), jnp.int32),
        pltpu.VMEM((8 * PITCH, 128), F32), pltpu.VMEM((8 * PITCH, 128), F32), pltpu.VMEM((8 * PITCH, 128), jnp.int32),
        pltpu.VMEM((8, 8, 128), jnp.int32), pltpu.VMEM((128 * 24, 128), F32), vm(3, DEPTHS, L), vm(3, 8), vm(3, 8),
        vm(22), vm(22), vm(17), vm(22), vm(22), vm(2),
        vm(16), vm(16), vm(16), vm(16), vm(16), vm(17), vm(16), vm(16), vm(16), vm(16),
        vm(16), vm(17), vm(18), vm(16), vm(16), vm(16), vm(16), vm(17), vm(16), vm(16), vm(16), vm(16), vm(17),
        vm(2, 2), vm(2, 12), vm(4, 22), vm(4, 22), vm(4, 22), vm(4, 22),
        vm(8, 2, 2), vm(8, 2, 2), vm(2, Y_ALL), vm(2, Y_ALL), vm(2, Z_ALL), vm(2, Z_ALL),
        vm(2, 2), vm(2, 2), pltpu.VMEM((8, 1, 128), F32),
        vm(2, 2), vm(2, 2), vm(2, 2), pltpu.VMEM((8, 1, 128), F32), vm(2, 2, 2),
        pltpu.VMEM((1, 128), F32), pltpu.VMEM((2 * nx * nz - 1, 1, 128), F32),
        pltpu.VMEM((1, 128), F32), pltpu.VMEM((ny // 2 - 1, 1, 128), F32),
        dma((1,)), dma((8,)), dma((6,)), dma((2,)), dma((3,)), dma((3,)),
    ]
    vmem = pl.BlockSpec(memory_space=pltpu.VMEM)
    hbm = pl.BlockSpec(memory_space=pl.ANY)

    def per_device(fields, radius, weight, column, counts, fall_depth):
        held = pl.pallas_call(
            functools.partial(kernel, sizes),
            out_shape=(pltpu.VMEM((5, L, 8, 128), F32), pltpu.VMEM((3, L, 8, 128), F32)),
            in_specs=[hbm] * 6,
            out_specs=(vmem, vmem),
            scratch_shapes=scratch,
            compiler_params=pltpu.CompilerParams(collective_id=0, has_side_effects=True),
            name="slab_step",
        )(
            fields,
            counts.reshape(128, 128),
            jnp.transpose(fall_depth[:, :, :, 0], (0, 2, 1)),
            radius.reshape(1024, 128),
            weight.reshape(1024, 128),
            column.reshape(1024, 128),
        )
        return held

    cut = P(None, "gz", "gy", "gx")
    return jax.shard_map(
        per_device,
        mesh=mesh,
        in_specs=(cut, cut, cut, cut, P("gz", "gy", "gx"), cut),
        out_specs=(cut, cut),
        check_vma=False,
    )
```
